256 devices in a mesh: frame: 64 (over x, z, y_lo), row: 4 (over y_hi, core).
Axes of the slice: x: 4, y: 4 (y_hi: 2, y_lo: 2; y = y_hi * 2 + y_lo), z: 8, core: 2. Of those that a mesh axis runs over, the one named last changes fastest.
Arguments:
- clip: bfloat16 [128, 16, 256, 128], P('frame', 'row'), may hold values from -6 to 6
- first_kernel: bfloat16 [3, 3, 3, 128, 128], replicated, may hold values from -0.109375 to 0.109375
- second_kernel: bfloat16 [3, 3, 3, 128, 128], replicated, may hold values from -0.109375 to 0.109375
- cotangent: bfloat16 [128, 16, 256, 128], P('frame', 'row'), may hold values from -6 to 6
Outputs:
- critic_map: bfloat16 [128, 16, 256, 128], P('frame', 'row')
- clip_grad: bfloat16 [128, 16, 256, 128], P('frame', 'row')
- first_grad: float32 [3, 3, 3, 128, 128], replicated
- second_grad: float32 [3, 3, 3, 128, 128], replicated
The draws below stay inside these ranges and needn't reach their ends.
All inputs are finite; a program needn't handle non-finite values.
Results may differ from the reference program's by a relative error of at most 0.012.
Values may be sent and summed in bfloat16 or wider, within the bound.
A program may use at most 64 MiB of HBM per device.

```python
import jax
import jax.numpy as jnp
from jax import lax

CH = 128
WIDTH = 256
FRAMES = 128
ROWS = 16


def level_of(stream_key, extent, shards, low, high):
    loudness = 1.0
    for position, parts in shards:
        draws = jax.random.uniform(jax.random.fold_in(jax.random.fold_in(stream_key, 6), position), (parts,), jnp.float32, low / len(shards), high / len(shards))
        loudness = loudness * jnp.repeat(jnp.exp(draws), extent[position] // parts).reshape((-1,) + (1,) * (len(extent) - 1 - position))
    return loudness


def centred(rng, extent, scale, most, cuts=(), held_as=jnp.bfloat16):
    gain = level_of(rng, extent, cuts, -0.22, 0.18) if cuts else 1.0
    values = jax.random.normal(rng, extent, jnp.float32) * scale * gain
    return jnp.minimum(jnp.maximum(values, -most), most).astype(held_as)


def setup_inputs(seed: int = 0) -> dict:
    key_list = jax.random.split(jax.random.key(seed), 5)
    clip = centred(key_list[0], (FRAMES, ROWS, WIDTH, CH), 1.0, 6.0, ((0, 64), (1, 4)))
    first_kernel = centred(key_list[1], (3, 3, 3, CH, CH), (27 * CH) ** -0.5, 0.109375)
    second_kernel = centred(key_list[2], (3, 3, 3, CH, CH), (27 * CH) ** -0.5, 0.109375)
    cotangent = centred(key_list[3], (FRAMES, ROWS, WIDTH, CH), 1.0, 6.0, ((0, 64), (1, 4)))
    return dict(clip=clip, first_kernel=first_kernel, second_kernel=second_kernel, cotangent=cotangent)


def correlate(padded, kernel):
    result = lax.conv_general_dilated(padded[None], kernel, (1, 1, 1), ((0, 0), (0, 0), (1, 1)), dimension_numbers=('NDHWC', 'DHWIO', 'NDHWC'), preferred_element_type=jnp.float32)
    return result[0]

def silu_slope(value):
    sigma = jax.nn.sigmoid(value)
    return sigma * (1.0 + value * (1.0 - sigma))

def flipped_kernel(kernel):
    return jnp.transpose(kernel[::-1, ::-1, ::-1], (0, 1, 2, 4, 3))

def weight_grad(padded, delta):
    frame_count, row_count, columns, channels = delta.shape
    widened = jnp.pad(padded, ((0, 0), (0, 0), (1, 1), (0, 0)))
    flat_delta = delta.reshape(-1, channels)
    blocks = []
    for frame_off in range(3):
        for row_off in range(3):
            for col_off in range(3):
                window_slab = widened[frame_off:frame_off + frame_count, row_off:row_off + row_count, col_off:col_off + columns]
                blocks.append(lax.dot_general(window_slab.reshape(-1, channels), flat_delta, (((0,), (0,)), ((), ())), preferred_element_type=jnp.float32))
    return jnp.stack(blocks).reshape(3, 3, 3, channels, channels)

def reference(clip, first_kernel, second_kernel, cotangent):
    grad_scale = 1.0 / float(FRAMES * ROWS * WIDTH) ** 0.5
    clip_pad = jnp.pad(clip, ((2, 0), (1, 1), (0, 0), (0, 0)))
    first_pre = correlate(clip_pad, first_kernel)
    first_act = jax.nn.silu(first_pre).astype(jnp.bfloat16)
    act_pad = jnp.pad(first_act, ((2, 0), (1, 1), (0, 0), (0, 0)))
    second_pre = correlate(act_pad, second_kernel)
    critic_map = jax.nn.silu(second_pre).astype(jnp.bfloat16)
    second_delta = (cotangent.astype(jnp.float32) * silu_slope(second_pre)).astype(jnp.bfloat16)
    second_grad = weight_grad(act_pad, second_delta) * grad_scale
    first_back = correlate(jnp.pad(second_delta, ((0, 2), (1, 1), (0, 0), (0, 0))), flipped_kernel(second_kernel))
    first_delta = (first_back * silu_slope(first_pre)).astype(jnp.bfloat16)
    first_grad = weight_grad(clip_pad, first_delta) * grad_scale
    clip_grad = correlate(jnp.pad(first_delta, ((0, 2), (1, 1), (0, 0), (0, 0))), flipped_kernel(first_kernel)).astype(jnp.bfloat16)
    return (critic_map, clip_grad, first_grad, second_grad)
```

```python
import jax
import jax.numpy as jnp
from jax import lax
from jax.experimental import pallas as pl
from jax.experimental.pallas import tpu as pltpu
from jax.sharding import PartitionSpec as P


MESH = pl.DeviceIdType.MESH
NX, NY, NZ = 4, 4, 8
NXY = NX * NY
BLK = 112
HALF = NXY * BLK
ROWS = 2 * HALF
TILE = 16
ZT = BLK // TILE


class Place:
    def __init__(self):
        f, r = lax.axis_index("frame"), lax.axis_index("row")
        self.x, self.z = f // (2 * NZ), (f // 2) % NZ
        self.y, self.core = (r // 2) * 2 + f % 2, r % 2
        self.p = self.x * NY + self.y

    @staticmethod
    def at(x, y, z, core):
        return ((x * NZ + z) * 2 + y % 2, (y // 2) * 2 + core)


def remote(src, dst, send, recv, device):
    return pltpu.make_async_remote_copy(
        src_ref=src, dst_ref=dst, send_sem=send, recv_sem=recv, device_id=device, device_id_type=MESH)


def take(ref, rows, sem):
    view = ref.at[pl.ds(0, rows)]
    pltpu.make_async_copy(view, view, sem).wait()


def rows_of(start, size):
    return pl.ds(pl.multiple_of(start, TILE), size)


class AllReduce:
    def __init__(self, me, part, full, other, slots, piece, tiles, send, recv):
        self.me, self.part, self.full = me, part, full
        self.other, self.slots, self.piece, self.tiles = other, slots, piece, tiles
        self.send, self.recv = send, recv

    def xy_peer(self, o):
        p = (self.me.p + o) % NXY
        return p, Place.at(p // NY, p % NY, self.me.z, self.me.core)

    def z_peer(self, o):
        d = (self.me.z + o) % NZ
        return d, Place.at(self.me.x, self.me.y, d, self.me.core)

    def twin(self):
        return Place.at(self.me.x, self.me.y, self.me.z, 1 - self.me.core)

    def scatter_core(self):
        remote(self.part.at[rows_of((1 - self.me.core) * HALF, HALF)], self.other,
               self.send.at[0], self.recv.at[0], self.twin()).start()

    def scatter_xy(self):
        me = self.me
        take(self.other, HALF, self.recv.at[0])
        base = me.core * HALF

        @pl.loop(0, HALF // 128)
        def _(i):
            mine = rows_of(base + i * 128, 128)
            total = self.part[mine, :].astype(jnp.float32) + self.other[rows_of(i * 128, 128), :].astype(jnp.float32)
            self.part[mine, :] = total.astype(jnp.bfloat16)

        @pl.loop(1, NXY)
        def _(o):
            p, peer = self.xy_peer(o)
            remote(self.part.at[rows_of(base + p * BLK, BLK)], self.slots.at[rows_of(me.p * BLK, BLK)],
                   self.send.at[1], self.recv.at[1], peer).start()

    def scatter_z(self):
        me = self.me
        take(self.slots, (NXY - 1) * BLK, self.recv.at[1])
        total = self.part[rows_of(me.core * HALF + me.p * BLK, BLK), :].astype(jnp.float32)

        def add(o, total):
            p = (me.p + o) % NXY
            return total + self.slots[rows_of(p * BLK, BLK), :].astype(jnp.float32)

        self.piece[...] = lax.fori_loop(1, NXY, add, total).astype(jnp.bfloat16)

        @pl.loop(1, NZ)
        def _(o):
            d, peer = self.z_peer(o)

            @pl.when(d < ZT)
            def _():
                remote(self.piece.at[rows_of(d * TILE, TILE)], self.tiles.at[rows_of(me.z * TILE, TILE)],
                       self.send.at[2], self.recv.at[2], peer).start()

    def gather_z(self):
        me = self.me

        @pl.when(me.z < ZT)
        def _():
            take(self.tiles, (NZ - 1) * TILE, self.recv.at[2])
            total = self.piece[rows_of(me.z * TILE, TILE), :].astype(jnp.float32)
            for o in range(1, NZ):
                d = (me.z + o) % NZ
                total = total + self.tiles[rows_of(d * TILE, TILE), :].astype(jnp.float32)
            mine = rows_of(me.core * HALF + me.p * BLK + me.z * TILE, TILE)
            self.full[mine, :] = total.astype(jnp.bfloat16)

            @pl.loop(1, NZ)
            def _(o):
                d, peer = self.z_peer(o)
                remote(self.full.at[mine], self.full.at[mine], self.send.at[3], self.recv.at[3], peer).start()

    def gather_xy(self):
        me = self.me

        @pl.when(me.z < ZT)
        def _():
            take(self.full, (ZT - 1) * TILE, self.recv.at[3])

        @pl.when(me.z >= ZT)
        def _():
            take(self.full, ZT * TILE, self.recv.at[3])

        mine = rows_of(me.core * HALF + me.p * BLK, BLK)

        @pl.loop(1, NXY)
        def _(o):
            p, peer = self.xy_peer(o)
            remote(self.full.at[mine], self.full.at[mine], self.send.at[4], self.recv.at[4], peer).start()

    def gather_core(self):
        take(self.full, (NXY - 1) * BLK, self.recv.at[4])
        mine = rows_of(self.me.core * HALF, HALF)
        remote(self.full.at[mine], self.full.at[mine], self.send.at[5], self.recv.at[5], self.twin()).start()

    def finish(self):
        me = self.me
        take(self.full, HALF, self.recv.at[5])
        take(self.part, HALF, self.send.at[0])
        take(self.part, (NXY - 1) * BLK, self.send.at[1])

        @pl.when(me.z < ZT)
        def _():
            take(self.piece, (ZT - 1) * TILE, self.send.at[2])
            take(self.full, (NZ - 1) * TILE, self.send.at[3])

        @pl.when(me.z >= ZT)
        def _():
            take(self.piece, ZT * TILE, self.send.at[2])

        take(self.full, (NXY - 1) * BLK, self.send.at[4])
        take(self.full, HALF, self.send.at[5])


def greet_reduce_peers(me, barrier):
    pl.semaphore_signal(barrier, inc=1, device_id=Place.at(me.x, me.y, me.z, 1 - me.core), device_id_type=MESH)

    @pl.loop(1, NXY)
    def _(o):
        p = (me.p + o) % NXY
        pl.semaphore_signal(barrier, inc=1, device_id=Place.at(p // NY, p % NY, me.z, me.core), device_id_type=MESH)

    @pl.loop(1, NZ)
    def _(o):
        d = (me.z + o) % NZ
        pl.semaphore_signal(barrier, inc=1, device_id=Place.at(me.x, me.y, d, me.core), device_id_type=MESH)

    return 1 + NXY - 1 + NZ - 1


def reduce_kernel(first, second, full_first, full_second, part, other, slots, piece, tiles, send, recv):
    me = Place()
    barrier = pltpu.get_barrier_semaphore()
    pl.semaphore_wait(barrier, greet_reduce_peers(me, barrier))
    sums = [
        AllReduce(me, p, f, other.at[i], slots.at[i], piece.at[i], tiles.at[i], send.at[i], recv.at[i])
        for i, (p, f) in enumerate([(part.at[0], full_first), (part.at[1], full_second)])]
    for i, ref in enumerate((first, second)):
        @pl.loop(0, ROWS // 128)
        def _(k):
            part[i, rows_of(k * 128, 128), :] = ref[rows_of(k * 128, 128), :]
    for stage in ("scatter_core", "scatter_xy", "scatter_z", "gather_z", "gather_xy", "gather_core", "finish"):
        for s in sums:
            getattr(s, stage)()


def reduce_over_all(first, second):
    whole = pl.BlockSpec(memory_space=pltpu.VMEM)
    shape = jax.ShapeDtypeStruct((ROWS, 128), jnp.bfloat16)
    bf16 = jnp.bfloat16
    return pl.pallas_call(
        reduce_kernel,
        out_shape=(shape, shape),
        in_specs=[whole] * 2,
        out_specs=(whole, whole),
        scratch_shapes=[
            pltpu.VMEM((2, ROWS, 128), bf16),
            pltpu.VMEM((2, HALF, 128), bf16),
            pltpu.VMEM((2, NXY * BLK, 128), bf16),
            pltpu.VMEM((2, BLK, 128), bf16),
            pltpu.VMEM((2, NZ * TILE, 128), bf16),
            pltpu.SemaphoreType.DMA((2, 6)),
            pltpu.SemaphoreType.DMA((2, 6)),
        ],
        compiler_params=pltpu.CompilerParams(collective_id=0, has_side_effects=True),
    )(first, second)


def extended_2(value, sides, width):
    for axis, dim in sides:
        size, length = (lax.axis_size(axis), value.shape[dim])
        up = [(i, (i + 1) % size) for i in range(size - 1)]
        down = [(j, i) for i, j in up]
        last = lax.slice_in_dim(value, length - width, length, axis=dim)
        leading = lax.slice_in_dim(value, 0, width, axis=dim)
        before = lax.ppermute(last, axis, up)
        after = lax.ppermute(leading, axis, down)
        value = jnp.concatenate([before, value, after], axis=dim)
    return value


def passed_along(value, axis, by):
    length = lax.axis_size(axis)
    pairs = [(i, i + by) for i in range(length) if 0 <= i + by < length]
    return lax.ppermute(value, axis, pairs)


def correlate(padded, kernel):
    result = lax.conv_general_dilated(
        padded[None],
        kernel,
        (1, 1, 1),
        ((0, 0), (0, 0), (1, 1)),
        dimension_numbers=("NDHWC", "DHWIO", "NDHWC"),
        preferred_element_type=jnp.float32,
    )
    return result[0]


def silu_slope(value):
    sigma = jax.nn.sigmoid(value)
    return sigma * (1.0 + value * (1.0 - sigma))


def flipped_kernel(kernel):
    return jnp.transpose(kernel[::-1, ::-1, ::-1], (0, 1, 2, 4, 3))


def weight_grad(padded, delta):
    frame_count, row_count, columns, channels = delta.shape
    widened = jnp.pad(padded, ((0, 0), (0, 0), (1, 1), (0, 0)))
    flat_delta = delta.reshape(-1, channels)
    blocks = []
    for frame_off in range(3):
        for row_off in range(3):
            for col_off in range(3):
                window_slab = widened[
                    frame_off : frame_off + frame_count,
                    row_off : row_off + row_count,
                    col_off : col_off + columns,
                ]
                blocks.append(
                    lax.dot_general(
                        window_slab.reshape(-1, channels),
                        flat_delta,
                        (((0,), (0,)), ((), ())),
                        preferred_element_type=jnp.float32,
                    )
                )
    return jnp.stack(blocks).reshape(3, 3, 3, channels, channels)


def forward_pad(activation):
    rim_rows = extended_2(activation, (("row", 1),), 1)
    earlier = passed_along(rim_rows[-2:], "frame", 1)
    return jnp.concatenate([earlier, rim_rows], 0)


def input_grad(delta, kernel):
    reversed_kernel = flipped_kernel(kernel)
    rim_rows = extended_2(delta, (("row", 1),), 1)
    upcoming = passed_along(rim_rows[:2], "frame", -1)
    extended = jnp.concatenate([rim_rows, upcoming], 0)
    return correlate(extended, reversed_kernel)


def on_device(clip, first_kernel, second_kernel, cotangent):
    frame_count, row_count, columns, channels = clip.shape
    cell_total = frame_count * lax.axis_size("frame") * row_count * lax.axis_size("row") * columns
    grad_scale = 1.0 / float(cell_total) ** 0.5
    clip_pad = forward_pad(clip)
    first_pre = correlate(clip_pad, first_kernel)
    first_act = jax.nn.silu(first_pre).astype(jnp.bfloat16)
    act_pad = forward_pad(first_act)
    second_pre = correlate(act_pad, second_kernel)
    critic_map = jax.nn.silu(second_pre).astype(jnp.bfloat16)
    second_delta = (cotangent.astype(jnp.float32) * silu_slope(second_pre)).astype(jnp.bfloat16)
    second_grad = weight_grad(act_pad, second_delta) * grad_scale
    first_back = input_grad(second_delta, second_kernel)
    first_delta = (first_back * silu_slope(first_pre)).astype(jnp.bfloat16)
    first_grad = weight_grad(clip_pad, first_delta) * grad_scale
    clip_grad = input_grad(first_delta, first_kernel).astype(jnp.bfloat16)

    def flat(grad):
        return jnp.pad(grad.reshape(-1, channels).astype(jnp.bfloat16), ((0, ROWS - 27 * channels), (0, 0)))

    def whole(total):
        return total[: 27 * channels].reshape(3, 3, 3, channels, channels).astype(jnp.float32)

    sums = reduce_over_all(flat(first_grad), flat(second_grad))
    first_grad, second_grad = (whole(total) for total in sums)
    return (critic_map, clip_grad, first_grad, second_grad)


def solution(mesh):
    placed = (P("frame", "row", None, None), P(), P(), P("frame", "row", None, None))
    return jax.shard_map(
        on_device,
        mesh=mesh,
        in_specs=placed,
        out_specs=(P("frame", "row", None, None), P("frame", "row", None, None), P(), P()),
        check_vma=False,
    )
```

```python
import functools

import jax
import jax.numpy as jnp
from jax import lax
from jax.experimental import pallas as pl
from jax.experimental.pallas import tpu as pltpu
from jax.sharding import PartitionSpec as P

MESH = pl.DeviceIdType.MESH
BF16, F32 = jnp.bfloat16, jnp.float32
CH = 128

NX, NY, NZ = 4, 4, 8
NXY = NX * NY
BLK = 112
HALF = NXY * BLK
ROWS = 2 * HALF
TILE = 16
ZT = BLK // TILE


class Place:
    def __init__(self):
        f, r = lax.axis_index("frame"), lax.axis_index("row")
        self.x, self.z = f // (2 * NZ), (f // 2) % NZ
        self.y, self.core = (r // 2) * 2 + f % 2, r % 2
        self.p = self.x * NY + self.y

    @staticmethod
    def at(x, y, z, core):
        return ((x * NZ + z) * 2 + y % 2, (y // 2) * 2 + core)


def remote(src, dst, send, recv, device):
    return pltpu.make_async_remote_copy(
        src_ref=src, dst_ref=dst, send_sem=send, recv_sem=recv, device_id=device, device_id_type=MESH)


def take(ref, rows, sem):
    view = ref.at[pl.ds(0, rows)]
    pltpu.make_async_copy(view, view, sem).wait()


def rows_of(start, size):
    return pl.ds(pl.multiple_of(start, TILE), size)


class AllReduce:
    def __init__(self, me, part, full, other, slots, piece, tiles, send, recv):
        self.me, self.part, self.full = me, part, full
        self.other, self.slots, self.piece, self.tiles = other, slots, piece, tiles
        self.send, self.recv = send, recv

    def xy_peer(self, o):
        p = (self.me.p + o) % NXY
        return p, Place.at(p // NY, p % NY, self.me.z, self.me.core)

    def z_peer(self, o):
        d = (self.me.z + o) % NZ
        return d, Place.at(self.me.x, self.me.y, d, self.me.core)

    def twin(self):
        return Place.at(self.me.x, self.me.y, self.me.z, 1 - self.me.core)

    def scatter_core(self):
        remote(self.part.at[rows_of((1 - self.me.core) * HALF, HALF)], self.other,
               self.send.at[0], self.recv.at[0], self.twin()).start()

    def scatter_xy(self):
        me = self.me
        take(self.other, HALF, self.recv.at[0])
        base = me.core * HALF

        @pl.loop(0, HALF // 128)
        def _(i):
            mine = rows_of(base + i * 128, 128)
            total = self.part[mine, :].astype(jnp.float32) + self.other[rows_of(i * 128, 128), :].astype(jnp.float32)
            self.part[mine, :] = total.astype(jnp.bfloat16)

        @pl.loop(1, NXY)
        def _(o):
            p, peer = self.xy_peer(o)
            remote(self.part.at[rows_of(base + p * BLK, BLK)], self.slots.at[rows_of(me.p * BLK, BLK)],
                   self.send.at[1], self.recv.at[1], peer).start()

    def scatter_z(self):
        me = self.me
        take(self.slots, (NXY - 1) * BLK, self.recv.at[1])
        total = self.part[rows_of(me.core * HALF + me.p * BLK, BLK), :].astype(jnp.float32)

        def add(o, total):
            p = (me.p + o) % NXY
            return total + self.slots[rows_of(p * BLK, BLK), :].astype(jnp.float32)

        self.piece[...] = lax.fori_loop(1, NXY, add, total).astype(jnp.bfloat16)

        @pl.loop(1, NZ)
        def _(o):
            d, peer = self.z_peer(o)

            @pl.when(d < ZT)
            def _():
                remote(self.piece.at[rows_of(d * TILE, TILE)], self.tiles.at[rows_of(me.z * TILE, TILE)],
                       self.send.at[2], self.recv.at[2], peer).start()

    def gather_z(self):
        me = self.me

        @pl.when(me.z < ZT)
        def _():
            take(self.tiles, (NZ - 1) * TILE, self.recv.at[2])
            total = self.piece[rows_of(me.z * TILE, TILE), :].astype(jnp.float32)
            for o in range(1, NZ):
                d = (me.z + o) % NZ
                total = total + self.tiles[rows_of(d * TILE, TILE), :].astype(jnp.float32)
            mine = rows_of(me.core * HALF + me.p * BLK + me.z * TILE, TILE)
            self.full[mine, :] = total.astype(jnp.bfloat16)

            @pl.loop(1, NZ)
            def _(o):
                d, peer = self.z_peer(o)
                remote(self.full.at[mine], self.full.at[mine], self.send.at[3], self.recv.at[3], peer).start()

    def gather_xy(self):
        me = self.me

        @pl.when(me.z < ZT)
        def _():
            take(self.full, (ZT - 1) * TILE, self.recv.at[3])

        @pl.when(me.z >= ZT)
        def _():
            take(self.full, ZT * TILE, self.recv.at[3])

        mine = rows_of(me.core * HALF + me.p * BLK, BLK)

        @pl.loop(1, NXY)
        def _(o):
            p, peer = self.xy_peer(o)
            remote(self.full.at[mine], self.full.at[mine], self.send.at[4], self.recv.at[4], peer).start()

    def gather_core(self):
        take(self.full, (NXY - 1) * BLK, self.recv.at[4])
        mine = rows_of(self.me.core * HALF, HALF)
        remote(self.full.at[mine], self.full.at[mine], self.send.at[5], self.recv.at[5], self.twin()).start()

    def finish(self):
        me = self.me
        take(self.full, HALF, self.recv.at[5])
        take(self.part, HALF, self.send.at[0])
        take(self.part, (NXY - 1) * BLK, self.send.at[1])

        @pl.when(me.z < ZT)
        def _():
            take(self.piece, (ZT - 1) * TILE, self.send.at[2])
            take(self.full, (NZ - 1) * TILE, self.send.at[3])

        @pl.when(me.z >= ZT)
        def _():
            take(self.piece, ZT * TILE, self.send.at[2])

        take(self.full, (NXY - 1) * BLK, self.send.at[4])
        take(self.full, HALF, self.send.at[5])


def greet_reduce_peers(me, barrier):
    pl.semaphore_signal(barrier, inc=1, device_id=Place.at(me.x, me.y, me.z, 1 - me.core), device_id_type=MESH)

    @pl.loop(1, NXY)
    def _(o):
        p = (me.p + o) % NXY
        pl.semaphore_signal(barrier, inc=1, device_id=Place.at(p // NY, p % NY, me.z, me.core), device_id_type=MESH)

    @pl.loop(1, NZ)
    def _(o):
        d = (me.z + o) % NZ
        pl.semaphore_signal(barrier, inc=1, device_id=Place.at(me.x, me.y, d, me.core), device_id_type=MESH)

    return 1 + NXY - 1 + NZ - 1

GROUP, FR, COLS, ROWN = 8, 4, 32, 16
POS = COLS * ROWN
NG = NX * NZ


class Ring:
    def __init__(self):
        f, r = lax.axis_index("frame"), lax.axis_index("row")
        self.g, self.y_lo, self.r = f // 2, f % 2, r
        self.s = (r // 2) * 4 + self.y_lo * 2 + r % 2

    @staticmethod
    def parts(s):
        return (s // 2) % 2, (s // 4) * 2 + s % 2

    @staticmethod
    def at(g, s):
        y_lo, r = Ring.parts(s)
        return (g * 2 + y_lo, r)


class Field:
    def __init__(self, ref, ring, own, step, send, recv):
        self.ref, self.ring, self.own, self.step, self.send, self.recv = ref, ring, own, step, send, recv
        self.sends = []

    def clear(self):
        far = 0 if self.own else FR
        self.ref[far : far + 2] = jnp.zeros((2, COLS + 2, ROWN, CH), BF16)
        for col in (0, COLS + 1):
            self.ref[self.own : self.own + FR, col] = jnp.zeros((FR, ROWN, CH), BF16)

    def put(self, f, value):
        self.ref[self.own + f, 1 : COLS + 1] = value.astype(BF16).reshape(COLS, ROWN, CH)

    def to_left(self):
        return self.ring.s > 0

    def to_right(self):
        return self.ring.s < GROUP - 1

    def has_target(self):
        return self.ring.g < NG - 1 if self.step > 0 else self.ring.g > 0

    def has_source(self):
        return self.ring.g > 0 if self.step > 0 else self.ring.g < NG - 1

    def copy(self, frames, col, to_frames, to_col, g, s, i):
        return remote(self.ref.at[frames, col], self.ref.at[to_frames, to_col], self.send.at[i], self.recv.at[i], Ring.at(g, s))

    def edges(self, q):
        g, s = self.ring.g, self.ring.s
        frames = pl.ds(self.own + 2 * q, 2)

        @pl.when(self.to_left())
        def _():
            self.copy(frames, 1, frames, COLS + 1, g, s - 1, 2 * q).start()

        @pl.when(self.to_right())
        def _():
            self.copy(frames, COLS, frames, 0, g, s + 1, 2 * q + 1).start()

    def await_edges(self, q):
        self._edges(q, self.recv, self.to_right(), self.to_left())

    def _edges(self, q, sem, left, right):
        view = self.ref.at[pl.ds(self.own + 2 * q, 2), 0]

        @pl.when(left)
        def _():
            pltpu.make_async_copy(view, view, sem.at[2 * q]).wait()

        @pl.when(right)
        def _():
            pltpu.make_async_copy(view, view, sem.at[2 * q + 1]).wait()

    def frames(self):
        g, s = self.ring.g + self.step, self.ring.s
        mine, theirs = (pl.ds(FR, 2), pl.ds(0, 2)) if self.step > 0 else (pl.ds(0, 2), pl.ds(FR, 2))
        body = pl.ds(1, COLS)

        @pl.when(self.has_target())
        def _():
            self.copy(mine, body, theirs, body, g, s, 4).start()

        @pl.when(self.has_target() & self.to_left())
        def _():
            self.copy(mine, 1, theirs, COLS + 1, g, s - 1, 5).start()

        @pl.when(self.has_target() & self.to_right())
        def _():
            self.copy(mine, COLS, theirs, 0, g, s + 1, 6).start()

    def _frames(self, sem, there, left, right):
        body, col = self.ref.at[pl.ds(0, 2), pl.ds(1, COLS)], self.ref.at[pl.ds(0, 2), 0]

        @pl.when(there)
        def _():
            pltpu.make_async_copy(body, body, sem.at[4]).wait()

        @pl.when(there & left)
        def _():
            pltpu.make_async_copy(col, col, sem.at[5]).wait()

        @pl.when(there & right)
        def _():
            pltpu.make_async_copy(col, col, sem.at[6]).wait()

    def await_frames(self):
        self._frames(self.recv, self.has_source(), self.to_right(), self.to_left())

    def finish(self):
        for q in range(2):
            self._edges(q, self.send, self.to_left(), self.to_right())
        self._frames(self.send, self.has_target(), self.to_left(), self.to_right())

    def slab(self, p, k, c):
        return self.ref[2 * p + k, c : c + COLS].reshape(POS, CH)


def build_weights(kernel, ahead, back, sem):
    zero = jnp.zeros((CH, CH), BF16)
    for k, j in ((0, 1), (3, 0)):
        @pl.loop(0, 9)
        def _(bc):
            b, c = bc // 3, bc % 3
            ahead[pl.ds(pl.multiple_of((c * 4 + k) * CH, CH), CH), pl.ds(pl.multiple_of((b * 2 + j) * CH, CH), CH)] = zero
            back[pl.ds(pl.multiple_of((b * 2 + j) * CH, CH), CH), pl.ds(pl.multiple_of((c * 4 + k) * CH, CH), CH)] = zero

    @pl.loop(0, 27)
    def _(tap):
        a, b, c = tap // 9, (tap // 3) % 3, tap % 3
        for j in range(2):
            k = a + j
            pltpu.make_async_copy(
                kernel.at[tap],
                ahead.at[pl.ds(pl.multiple_of((c * 4 + k) * CH, CH), CH), pl.ds(pl.multiple_of((b * 2 + j) * CH, CH), CH)],
                sem.at[0]).start()
            k = j + 2 - a
            pltpu.make_async_copy(
                kernel.at[tap],
                back.at[pl.ds(pl.multiple_of(((2 - b) * 2 + j) * CH, CH), CH), pl.ds(pl.multiple_of(((2 - c) * 4 + k) * CH, CH), CH)],
                sem.at[1]).start()


def await_weights(ahead, back, sem):
    view = ahead.at[pl.ds(0, 54 * CH * CH // ahead.shape[1])]
    pltpu.make_async_copy(view, view, sem.at[0]).wait()
    view = back.at[pl.ds(0, 54 * CH * CH // back.shape[1])]
    pltpu.make_async_copy(view, view, sem.at[1]).wait()


def row_index(width):
    return lax.broadcasted_iota(jnp.int32, (POS, width), 0) % ROWN


def from_above(value):
    return jnp.where(row_index(value.shape[1]) == 0, 0.0, pltpu.roll(value, 1, axis=0))


def from_below(value):
    return jnp.where(row_index(value.shape[1]) == ROWN - 1, 0.0, pltpu.roll(value, POS - 1, axis=0))


def convolve(field, weights, p, contract):
    lhs = jnp.concatenate([field.slab(p, k, c) for c in range(3) for k in range(4)], axis=1)
    rows = lax.dot_general(lhs, weights[...], (((1,), (contract,)), ((), ())), preferred_element_type=F32)
    above, level, below = (rows[:, b * 2 * CH : (b + 1) * 2 * CH] for b in range(3))
    return level + from_above(above) + from_below(below)


def store_turned(turned, delta, p):
    for b, value in enumerate((from_below(delta), delta, from_above(delta))):
        turned[b * 2 * CH : (b + 1) * 2 * CH, p * POS : (p + 1) * POS] = value.astype(BF16).T


def weight_grads(field, turned, part, scale):
    for c in range(3):
        rhs = jnp.concatenate(
            [jnp.concatenate([field.slab(p, k, c) for k in range(4)], axis=1) for p in range(2)], axis=0)
        sums = lax.dot_general(turned[...], rhs, (((1,), (0,)), ((), ())), preferred_element_type=F32)
        for b in range(3):
            for a in range(3):
                one = sums[2 * b * CH : (2 * b + 1) * CH, a * CH : (a + 1) * CH]
                two = sums[(2 * b + 1) * CH : (2 * b + 2) * CH, (a + 1) * CH : (a + 2) * CH]
                tap = (a * 3 + b) * 3 + c
                part[tap * CH : (tap + 1) * CH, :] = ((one + two) * scale).T.astype(BF16)


def swap(value):
    return jnp.swapaxes(value, 0, 1)


def spread(ring, source, stage, send, recv, own):
    @pl.loop(1, GROUP)
    def _(o):
        d = (ring.s + o) % GROUP
        cols = pl.ds(pl.multiple_of(d * COLS, COLS), COLS)
        remote(source.at[:, :, cols], stage.at[pl.ds(2 * ring.y_lo, 2), pl.ds(4 * ring.r, 4)], send, recv, Ring.at(ring.g, d)).start()

    cols = pl.ds(pl.multiple_of(ring.s * COLS, COLS), COLS)
    pltpu.make_async_copy(source.at[:, :, cols], stage.at[pl.ds(2 * ring.y_lo, 2), pl.ds(4 * ring.r, 4)], own).start()


def give_back(ring, stage, result, send, recv, own):
    cols = pl.ds(pl.multiple_of(ring.s * COLS, COLS), COLS)

    @pl.loop(1, GROUP)
    def _(o):
        d = (ring.s + o) % GROUP
        half, quarter = Ring.parts(d)
        remote(stage.at[pl.ds(2 * half, 2), pl.ds(4 * quarter, 4)], result.at[:, :, cols], send, recv, Ring.at(ring.g, d)).start()

    pltpu.make_async_copy(stage.at[pl.ds(2 * ring.y_lo, 2), pl.ds(4 * ring.r, 4)], result.at[:, :, cols], own).start()


def await_blocks(flat, sem, own):
    take(flat, (GROUP - 1) * 2 * 4 * COLS, sem)
    take(flat, 2 * 4 * COLS, own)


def kernel(scale, clip, cotangent, first_kernel, second_kernel, critic_map, clip_grad, full_first, full_second,
           clip_a, act_a, second_a, first_a, first_w, first_wt, second_w, second_wt, stage, cot_f, slopes, turned,
           part, other, slots, piece, tiles,
           red_send, red_recv, halo_send, halo_recv, block_send, block_recv, block_own, weight_sem):
    me, ring = Place(), Ring()
    clips = Field(clip_a, ring, 2, 1, halo_send.at[0], halo_recv.at[0])
    acts = Field(act_a, ring, 2, 1, halo_send.at[1], halo_recv.at[1])
    seconds = Field(second_a, ring, 0, -1, halo_send.at[2], halo_recv.at[2])
    firsts = Field(first_a, ring, 0, -1, halo_send.at[3], halo_recv.at[3])
    fields = (clips, acts, seconds, firsts)
    first_sum, second_sum = (
        AllReduce(me, part.at[i], full, other.at[i], slots.at[i], piece.at[i], tiles.at[i], red_send.at[i], red_recv.at[i])
        for i, full in enumerate((full_first, full_second)))

    for field in fields:
        field.clear()

    barrier = pltpu.get_barrier_semaphore()
    count = greet_reduce_peers(me, barrier)

    @pl.loop(1, GROUP)
    def _(o):
        pl.semaphore_signal(barrier, inc=1, device_id=Ring.at(ring.g, (ring.s + o) % GROUP), device_id_type=MESH)

    count = count + GROUP - 1
    for step in (-1, 1):
        for side in (-1, 0, 1):
            g, s = ring.g + step, ring.s + side
            there = (g >= 0) & (g < NG) & (s >= 0) & (s < GROUP)

            @pl.when(there)
            def _():
                pl.semaphore_signal(barrier, inc=1, device_id=Ring.at(g, s), device_id_type=MESH)

            count = count + jnp.where(there, 1, 0)
    pl.semaphore_wait(barrier, count)

    spread(ring, clip, stage.at[0], block_send.at[0], block_recv.at[0], block_own.at[0])
    spread(ring, cotangent, stage.at[1], block_send.at[1], block_recv.at[1], block_own.at[1])
    build_weights(first_kernel, first_w, first_wt, weight_sem.at[0])
    build_weights(second_kernel, second_w, second_wt, weight_sem.at[1])
    for i in range(2):
        part[i, 27 * CH :, :] = jnp.zeros((CH, CH), BF16)

    await_blocks(full_first, block_recv.at[0], block_own.at[0])
    for f in range(FR):
        clip_a[2 + f, 1 : COLS + 1] = swap(stage[0, f])
    clips.edges(0)
    clips.edges(1)
    clips.frames()
    await_weights(first_w, first_wt, weight_sem.at[0])
    await_weights(second_w, second_wt, weight_sem.at[1])
    clips.await_edges(0)
    clips.await_edges(1)

    def sigmoid_slope(z):
        sigma = jax.nn.sigmoid(z)
        return sigma, sigma * (1.0 + z * (1.0 - sigma))

    def first_layer(p):
        pre = convolve(clips, first_w, p, 0)
        sigma, slope = sigmoid_slope(pre)
        act = pre * sigma
        for j in range(2):
            acts.put(2 * p + j, act[:, j * CH : (j + 1) * CH])
        slopes[p] = slope

    def second_layer(p):
        pre = convolve(acts, second_w, p, 0)
        sigma, slope = sigmoid_slope(pre)
        critic = pre * sigma
        delta = slope * jnp.concatenate(
            [cot_f[2 * p + j].reshape(POS, CH).astype(F32) for j in range(2)], axis=1)
        for j in range(2):
            half = slice(j * CH, (j + 1) * CH)
            stage[2, 2 * p + j] = swap(critic[:, half].astype(BF16).reshape(COLS, ROWN, CH))
            seconds.put(2 * p + j, delta[:, half])
        store_turned(turned, delta, p)

    def back_layer(p):
        delta = convolve(seconds, second_wt, p, 1) * slopes[p]
        for j in range(2):
            firsts.put(2 * p + j, delta[:, j * CH : (j + 1) * CH])
        store_turned(turned, delta, p)

    def input_layer(p):
        back = convolve(firsts, first_wt, p, 1)
        for j in range(2):
            stage[0, 2 * p + j] = swap(back[:, j * CH : (j + 1) * CH].astype(BF16).reshape(COLS, ROWN, CH))

    first_layer(1)
    acts.edges(1)
    acts.frames()
    clips.await_frames()
    first_layer(0)
    acts.edges(0)
    await_blocks(full_first, block_recv.at[1], block_own.at[1])
    for f in range(FR):
        cot_f[f] = swap(stage[1, f])
    acts.await_edges(1)
    acts.await_edges(0)
    second_layer(1)
    seconds.edges(1)
    acts.await_frames()
    second_layer(0)
    seconds.frames()
    seconds.edges(0)
    give_back(ring, stage.at[2], critic_map, block_send.at[2], block_recv.at[2], block_own.at[2])
    weight_grads(acts, turned, part.at[1], scale)
    second_sum.scatter_core()
    seconds.await_edges(0)
    seconds.await_edges(1)
    back_layer(0)
    firsts.frames()
    firsts.edges(0)
    second_sum.scatter_xy()
    seconds.await_frames()
    back_layer(1)
    firsts.edges(1)
    weight_grads(clips, turned, part.at[0], scale)
    first_sum.scatter_core()
    second_sum.scatter_z()
    take(full_first, (GROUP - 1) * 2 * 4 * COLS, block_send.at[0])
    firsts.await_edges(0)
    firsts.await_edges(1)
    first_sum.scatter_xy()
    second_sum.gather_z()
    input_layer(0)
    firsts.await_frames()
    input_layer(1)
    second_sum.gather_xy()
    give_back(ring, stage.at[0], clip_grad, block_send.at[3], block_recv.at[3], block_own.at[3])
    first_sum.scatter_z()
    first_sum.gather_z()
    second_sum.gather_core()
    first_sum.gather_xy()
    first_sum.gather_core()
    second_sum.finish()
    first_sum.finish()
    for field in fields:
        field.finish()
    for i in range(1, 4):
        take(full_first, (GROUP - 1) * 2 * 4 * COLS, block_send.at[i])
    for i in range(2, 4):
        await_blocks(full_first, block_recv.at[i], block_own.at[i])


def on_device(clip, first_kernel, second_kernel, cotangent):
    cells = clip.shape[0] * lax.axis_size("frame") * clip.shape[1] * lax.axis_size("row") * clip.shape[2]
    scale = 1.0 / float(cells) ** 0.5
    vmem, anywhere = pl.BlockSpec(memory_space=pltpu.VMEM), pl.BlockSpec(memory_space=pl.ANY)
    total = jax.ShapeDtypeStruct((ROWS, CH), BF16)
    field = pltpu.VMEM((FR + 2, COLS + 2, ROWN, CH), BF16)
    dma = pltpu.SemaphoreType.DMA
    critic_map, clip_grad, first, second = pl.pallas_call(
        functools.partial(kernel, scale),
        out_shape=(jax.ShapeDtypeStruct(clip.shape, BF16), jax.ShapeDtypeStruct(clip.shape, BF16), total, total),
        in_specs=[vmem, vmem, anywhere, anywhere],
        out_specs=(vmem, vmem, vmem, vmem),
        scratch_shapes=[
            field, field, field, field,
            pltpu.VMEM((12 * CH, 6 * CH), BF16), pltpu.VMEM((6 * CH, 12 * CH), BF16),
            pltpu.VMEM((12 * CH, 6 * CH), BF16), pltpu.VMEM((6 * CH, 12 * CH), BF16),
            pltpu.VMEM((3, FR, ROWN, COLS, CH), BF16),
            pltpu.VMEM((FR, COLS, ROWN, CH), BF16),
            pltpu.VMEM((2, POS, 2 * CH), F32),
            pltpu.VMEM((6 * CH, 2 * POS), BF16),
            pltpu.VMEM((2, ROWS, CH), BF16),
            pltpu.VMEM((2, HALF, CH), BF16),
            pltpu.VMEM((2, NXY * BLK, CH), BF16),
            pltpu.VMEM((2, BLK, CH), BF16),
            pltpu.VMEM((2, NZ * TILE, CH), BF16),
            dma((2, 6)), dma((2, 6)), dma((4, 7)), dma((4, 7)), dma((4,)), dma((4,)), dma((4,)), dma((2, 2)),
        ],
        compiler_params=pltpu.CompilerParams(collective_id=0, has_side_effects=True, vmem_limit_bytes=60 << 20),
    )(clip, cotangent, first_kernel.reshape(27, CH, CH), second_kernel.reshape(27, CH, CH))

    def whole(total):
        return total[: 27 * CH].reshape(3, 3, 3, CH, CH).astype(F32)

    return critic_map, clip_grad, whole(first), whole(second)


def solution(mesh):
    placed = (P("frame", "row", None, None), P(), P(), P("frame", "row", None, None))
    return jax.shard_map(
        on_device,
        mesh=mesh,
        in_specs=placed,
        out_specs=(P("frame", "row", None, None), P("frame", "row", None, None), P(), P()),
        check_vma=False,
    )
```

```python
import functools

import jax
import jax.numpy as jnp
from jax import lax
from jax.experimental import pallas as pl
from jax.experimental.pallas import tpu as pltpu
from jax.sharding import PartitionSpec as P

MESH = pl.DeviceIdType.MESH
BF16, F32 = jnp.bfloat16, jnp.float32
CH = 128

NX, NY, NZ = 4, 4, 8
NXY = NX * NY
BLK = 112
HALF = NXY * BLK
ROWS = 2 * HALF
TILE = 16
ZT = BLK // TILE


class Place:
    def __init__(self):
        f, r = lax.axis_index("frame"), lax.axis_index("row")
        self.x, self.z = f // (2 * NZ), (f // 2) % NZ
        self.y, self.core = (r // 2) * 2 + f % 2, r % 2
        self.p = self.x * NY + self.y

    @staticmethod
    def at(x, y, z, core):
        return ((x * NZ + z) * 2 + y % 2, (y // 2) * 2 + core)


def remote(src, dst, send, recv, device):
    return pltpu.make_async_remote_copy(
        src_ref=src, dst_ref=dst, send_sem=send, recv_sem=recv, device_id=device, device_id_type=MESH)


def take(ref, rows, sem):
    view = ref.at[pl.ds(0, rows)]
    pltpu.make_async_copy(view, view, sem).wait()


def rows_of(start, size):
    return pl.ds(pl.multiple_of(start, TILE), size)


class AllReduce:
    A, B = (256, 64), (192, 48)
    START_B = NX * 256

    def __init__(self, me, part, full, other, slots, near, piece, tiles, send, recv):
        self.me, self.part, self.full = me, part, full
        self.other, self.slots, self.near, self.piece, self.tiles = other, slots, near, piece, tiles
        self.send, self.recv = send, recv
        self.base = me.core * HALF

    def x_peer(self, o):
        x = (self.me.x + o) % NX
        return x, Place.at(x, self.me.y, self.me.z, self.me.core)

    def y_peer(self, o):
        y = (self.me.y + o) % NY
        return y, Place.at(self.me.x, y, self.me.z, self.me.core)

    def z_peer(self, o):
        d = (self.me.z + o) % NZ
        return d, Place.at(self.me.x, self.me.y, d, self.me.core)

    def twin(self):
        return Place.at(self.me.x, self.me.y, self.me.z, 1 - self.me.core)

    def row_a(self, x, y):
        return self.base + x * self.A[0] + y * self.A[1]

    def row_b(self, x, y):
        return self.base + self.START_B + y * self.B[0] + x * self.B[1]

    def push(self, stage, source, start, target, to, size, peer):
        remote(source.at[rows_of(start, size)], target.at[rows_of(to, size)], self.send.at[stage], self.recv.at[stage], peer).start()

    def scatter_core(self):
        self.push(0, self.part, (1 - self.me.core) * HALF, self.other, 0, HALF, self.twin())

    def scatter_far(self):
        me = self.me
        take(self.other, HALF, self.recv.at[0])

        @pl.loop(0, HALF // 128)
        def _(i):
            mine = rows_of(self.base + i * 128, 128)
            total = self.part[mine, :].astype(F32) + self.other[rows_of(i * 128, 128), :].astype(F32)
            self.part[mine, :] = total.astype(BF16)

        @pl.loop(1, NX)
        def _(o):
            x, peer = self.x_peer(o)
            self.push(1, self.part, self.row_a(x, 0), self.slots, me.x * self.A[0], self.A[0], peer)
            y, peer = self.y_peer(o)
            self.push(1, self.part, self.row_b(0, y), self.slots, self.START_B + me.y * self.B[0], self.B[0], peer)

    def scatter_near(self):
        me = self.me
        take(self.slots, 3 * (self.A[0] + self.B[0]), self.recv.at[1])

        @pl.loop(0, 4)
        def _(i):
            for start, slot, mine, pitch, size in (
                (self.row_a(me.x, 0), 0, me.x, self.A[0], self.A[1]),
                (self.row_b(0, me.y), self.START_B, me.y, self.B[0], self.B[1])):
                rows = rows_of(start + i * size, size)
                total = self.part[rows, :].astype(F32)
                for o in range(1, 4):
                    total = total + self.slots[rows_of(slot + ((mine + o) % 4) * pitch + i * size, size), :].astype(F32)
                self.part[rows, :] = total.astype(BF16)

        @pl.loop(1, NX)
        def _(o):
            y, peer = self.y_peer(o)
            self.push(2, self.part, self.row_a(me.x, y), self.near, me.y * self.A[1], self.A[1], peer)
            x, peer = self.x_peer(o)
            self.push(2, self.part, self.row_b(x, me.y), self.near, NY * self.A[1] + me.x * self.B[1], self.B[1], peer)

    def scatter_z(self):
        me = self.me
        take(self.near, 3 * (self.A[1] + self.B[1]), self.recv.at[2])
        for start, slot, mine, size, to in (
            (self.row_a(me.x, me.y), 0, me.y, self.A[1], 0),
            (self.row_b(me.x, me.y), NY * self.A[1], me.x, self.B[1], self.A[1])):
            total = self.part[rows_of(start, size), :].astype(F32)
            for o in range(1, 4):
                total = total + self.near[rows_of(slot + ((mine + o) % 4) * size, size), :].astype(F32)
            self.piece[to : to + size, :] = total.astype(BF16)

        @pl.loop(1, NZ)
        def _(o):
            d, peer = self.z_peer(o)

            @pl.when(d < ZT)
            def _():
                self.push(3, self.piece, d * TILE, self.tiles, me.z * TILE, TILE, peer)

    def gather_z(self):
        me = self.me

        @pl.when(me.z < ZT)
        def _():
            take(self.tiles, (NZ - 1) * TILE, self.recv.at[3])
            total = self.piece[rows_of(me.z * TILE, TILE), :].astype(F32)
            for o in range(1, NZ):
                d = (me.z + o) % NZ
                total = total + self.tiles[rows_of(d * TILE, TILE), :].astype(F32)
            in_a = self.A[1] // TILE
            row = jnp.where(me.z < in_a, self.row_a(me.x, me.y) + me.z * TILE, self.row_b(me.x, me.y) + (me.z - in_a) * TILE)
            self.full[rows_of(row, TILE), :] = total.astype(BF16)

            @pl.loop(1, NZ)
            def _(o):
                d, peer = self.z_peer(o)
                self.push(4, self.full, row, self.full, row, TILE, peer)

    def gather_near(self):
        me = self.me

        @pl.when(me.z < ZT)
        def _():
            take(self.full, (ZT - 1) * TILE, self.recv.at[4])

        @pl.when(me.z >= ZT)
        def _():
            take(self.full, ZT * TILE, self.recv.at[4])

        a, b = self.row_a(me.x, me.y), self.row_b(me.x, me.y)

        @pl.loop(1, NX)
        def _(o):
            self.push(5, self.full, a, self.full, a, self.A[1], self.y_peer(o)[1])
            self.push(5, self.full, b, self.full, b, self.B[1], self.x_peer(o)[1])

    def gather_far(self):
        me = self.me
        take(self.full, 3 * (self.A[1] + self.B[1]), self.recv.at[5])
        a, b = self.row_a(me.x, 0), self.row_b(0, me.y)

        @pl.loop(1, NX)
        def _(o):
            self.push(6, self.full, a, self.full, a, self.A[0], self.x_peer(o)[1])
            self.push(6, self.full, b, self.full, b, self.B[0], self.y_peer(o)[1])

    def gather_core(self):
        take(self.full, 3 * (self.A[0] + self.B[0]), self.recv.at[6])
        self.push(7, self.full, self.base, self.full, self.base, HALF, self.twin())

    def finish(self):
        me = self.me
        take(self.full, HALF, self.recv.at[7])
        take(self.part, HALF, self.send.at[0])
        take(self.part, 3 * (self.A[0] + self.B[0]), self.send.at[1])
        take(self.part, 3 * (self.A[1] + self.B[1]), self.send.at[2])

        @pl.when(me.z < ZT)
        def _():
            take(self.piece, (ZT - 1) * TILE, self.send.at[3])
            take(self.full, (NZ - 1) * TILE, self.send.at[4])

        @pl.when(me.z >= ZT)
        def _():
            take(self.piece, ZT * TILE, self.send.at[3])

        take(self.full, 3 * (self.A[1] + self.B[1]), self.send.at[5])
        take(self.full, 3 * (self.A[0] + self.B[0]), self.send.at[6])
        take(self.full, HALF, self.send.at[7])


def greet_reduce_peers(me, barrier):
    pl.semaphore_signal(barrier, inc=1, device_id=Place.at(me.x, me.y, me.z, 1 - me.core), device_id_type=MESH)

    @pl.loop(1, NXY)
    def _(o):
        p = (me.p + o) % NXY
        pl.semaphore_signal(barrier, inc=1, device_id=Place.at(p // NY, p % NY, me.z, me.core), device_id_type=MESH)

    @pl.loop(1, NZ)
    def _(o):
        d = (me.z + o) % NZ
        pl.semaphore_signal(barrier, inc=1, device_id=Place.at(me.x, me.y, d, me.core), device_id_type=MESH)

    return 1 + NXY - 1 + NZ - 1

GROUP, FR, COLS, ROWN = 8, 4, 32, 16
POS = COLS * ROWN
NG = NX * NZ


class Ring:
    def __init__(self):
        f, r = lax.axis_index("frame"), lax.axis_index("row")
        self.g, self.y_lo, self.r = f // 2, f % 2, r
        self.s = (r // 2) * 4 + self.y_lo * 2 + r % 2

    @staticmethod
    def parts(s):
        return (s // 2) % 2, (s // 4) * 2 + s % 2

    @staticmethod
    def at(g, s):
        y_lo, r = Ring.parts(s)
        return (g * 2 + y_lo, r)


class Field:
    def __init__(self, ref, ring, own, halo, step, whole, send, recv):
        self.ref, self.ring, self.own, self.halo, self.step, self.whole = ref, ring, own, halo, step, whole
        self.send, self.recv = send, recv
        self.width = COLS + 2 * halo

    def clear(self):
        far = 0 if self.own else FR
        self.ref[far : far + 2] = jnp.zeros((2, self.width, ROWN, CH), BF16)
        for col in (0, COLS + self.halo):
            self.ref[self.own : self.own + FR, col : col + self.halo] = jnp.zeros((FR, self.halo, ROWN, CH), BF16)

    def put(self, f, value):
        self.ref[self.own + f, self.halo : self.halo + COLS] = value.astype(BF16).reshape(COLS, ROWN, CH)

    def to_left(self):
        return self.ring.s > 0

    def to_right(self):
        return self.ring.s < GROUP - 1

    def has_target(self):
        return self.ring.g < NG - 1 if self.step > 0 else self.ring.g > 0

    def has_source(self):
        return self.ring.g > 0 if self.step > 0 else self.ring.g < NG - 1

    def copy(self, frames, col, to_frames, to_col, width, g, s, i):
        return remote(self.ref.at[frames, pl.ds(col, width)], self.ref.at[to_frames, pl.ds(to_col, width)],
                      self.send.at[i], self.recv.at[i], Ring.at(g, s))

    def edge(self, frames, to_frames, side, g, i):
        halo, s = self.halo, self.ring.s
        source, target = (halo, COLS + halo) if side < 0 else (COLS, 0)
        self.copy(frames, source, to_frames, target, halo, g, s + side, i).start()

    def edges(self, q):
        frames = pl.ds(self.own + 2 * q, 2)

        @pl.when(self.to_left())
        def _():
            self.edge(frames, frames, -1, self.ring.g, 2 * q)

        @pl.when(self.to_right())
        def _():
            self.edge(frames, frames, 1, self.ring.g, 2 * q + 1)

    def await_edges(self, q):
        self._edges(q, self.recv, self.to_right(), self.to_left())

    def _edges(self, q, sem, left, right):
        view = self.ref.at[pl.ds(self.own + 2 * q, 2), pl.ds(0, self.halo)]

        @pl.when(left)
        def _():
            pltpu.make_async_copy(view, view, sem.at[2 * q]).wait()

        @pl.when(right)
        def _():
            pltpu.make_async_copy(view, view, sem.at[2 * q + 1]).wait()

    def span(self):
        return (0, self.width) if self.whole else (self.halo, COLS)

    def frames(self):
        g, s = self.ring.g + self.step, self.ring.s
        mine, theirs = (pl.ds(FR, 2), pl.ds(0, 2)) if self.step > 0 else (pl.ds(0, 2), pl.ds(FR, 2))
        start, width = self.span()

        @pl.when(self.has_target())
        def _():
            self.copy(mine, start, theirs, start, width, g, s, 4).start()

        if self.whole:
            return

        @pl.when(self.has_target() & self.to_left())
        def _():
            self.edge(mine, theirs, -1, g, 5)

        @pl.when(self.has_target() & self.to_right())
        def _():
            self.edge(mine, theirs, 1, g, 6)

    def _frames(self, sem, there, left, right):
        start, width = self.span()
        body, col = self.ref.at[pl.ds(0, 2), pl.ds(start, width)], self.ref.at[pl.ds(0, 2), pl.ds(0, self.halo)]

        @pl.when(there)
        def _():
            pltpu.make_async_copy(body, body, sem.at[4]).wait()

        if self.whole:
            return

        @pl.when(there & left)
        def _():
            pltpu.make_async_copy(col, col, sem.at[5]).wait()

        @pl.when(there & right)
        def _():
            pltpu.make_async_copy(col, col, sem.at[6]).wait()

    def await_frames(self):
        self._frames(self.recv, self.has_source(), self.to_right(), self.to_left())

    def finish(self):
        if not self.whole:
            for q in range(2):
                self._edges(q, self.send, self.to_left(), self.to_right())
        self._frames(self.send, self.has_target(), self.to_left(), self.to_right())

    def slab(self, p, k, start, width):
        return self.ref[2 * p + k, start : start + width].reshape(width * ROWN, CH)


def build_weights(kernel, ahead, back, sem):
    zero = jnp.zeros((CH, CH), BF16)
    for k, j in ((0, 1), (3, 0)):
        @pl.loop(0, 9)
        def _(bc):
            b, c = bc // 3, bc % 3
            ahead[pl.ds(pl.multiple_of((c * 4 + k) * CH, CH), CH), pl.ds(pl.multiple_of((b * 2 + j) * CH, CH), CH)] = zero
            back[pl.ds(pl.multiple_of((b * 2 + j) * CH, CH), CH), pl.ds(pl.multiple_of((c * 4 + k) * CH, CH), CH)] = zero

    @pl.loop(0, 27)
    def _(tap):
        a, b, c = tap // 9, (tap // 3) % 3, tap % 3
        for j in range(2):
            k = a + j
            pltpu.make_async_copy(
                kernel.at[tap],
                ahead.at[pl.ds(pl.multiple_of((c * 4 + k) * CH, CH), CH), pl.ds(pl.multiple_of((b * 2 + j) * CH, CH), CH)],
                sem.at[0]).start()
            k = j + 2 - a
            pltpu.make_async_copy(
                kernel.at[tap],
                back.at[pl.ds(pl.multiple_of(((2 - b) * 2 + j) * CH, CH), CH), pl.ds(pl.multiple_of(((2 - c) * 4 + k) * CH, CH), CH)],
                sem.at[1]).start()


def await_weights(ahead, back, sem):
    view = ahead.at[pl.ds(0, 54 * CH * CH // ahead.shape[1])]
    pltpu.make_async_copy(view, view, sem.at[0]).wait()
    view = back.at[pl.ds(0, 54 * CH * CH // back.shape[1])]
    pltpu.make_async_copy(view, view, sem.at[1]).wait()


def row_index(shape):
    return lax.broadcasted_iota(jnp.int32, shape, 0) % ROWN


def from_above(value):
    return jnp.where(row_index(value.shape) == 0, 0.0, pltpu.roll(value, 1, axis=0))


def from_below(value):
    return jnp.where(row_index(value.shape) == ROWN - 1, 0.0, pltpu.roll(value, value.shape[0] - 1, axis=0))


def convolve(field, weights, p, contract):
    width = field.width - 2
    lhs = jnp.concatenate([field.slab(p, k, c, width) for c in range(3) for k in range(4)], axis=1)
    rows = lax.dot_general(lhs, weights[...], (((1,), (contract,)), ((), ())), preferred_element_type=F32)
    above, level, below = (rows[:, b * 2 * CH : (b + 1) * 2 * CH] for b in range(3))
    return level + from_above(above) + from_below(below)


def store_turned(turned, delta, p):
    for b, value in enumerate((from_below(delta), delta, from_above(delta))):
        turned[b * 2 * CH : (b + 1) * 2 * CH, p * POS : (p + 1) * POS] = value.astype(BF16).T


def weight_grads(field, turned, part, scale):
    for c in range(3):
        rhs = jnp.concatenate(
            [jnp.concatenate([field.slab(p, k, field.halo - 1 + c, COLS) for k in range(4)], axis=1) for p in range(2)], axis=0)
        sums = lax.dot_general(turned[...], rhs, (((1,), (0,)), ((), ())), preferred_element_type=F32)
        for b in range(3):
            for a in range(3):
                one = sums[2 * b * CH : (2 * b + 1) * CH, a * CH : (a + 1) * CH]
                two = sums[(2 * b + 1) * CH : (2 * b + 2) * CH, (a + 1) * CH : (a + 2) * CH]
                tap = (a * 3 + b) * 3 + c
                part[tap * CH : (tap + 1) * CH, :] = ((one + two) * scale).T.astype(BF16)


def swap(value):
    return jnp.swapaxes(value, 0, 1)


def spread(ring, source, stage, send, recv, own):
    @pl.loop(1, GROUP)
    def _(o):
        d = (ring.s + o) % GROUP
        cols = pl.ds(pl.multiple_of(d * COLS, COLS), COLS)
        remote(source.at[:, :, cols], stage.at[pl.ds(2 * ring.y_lo, 2), pl.ds(4 * ring.r, 4)], send, recv, Ring.at(ring.g, d)).start()

    cols = pl.ds(pl.multiple_of(ring.s * COLS, COLS), COLS)
    pltpu.make_async_copy(source.at[:, :, cols], stage.at[pl.ds(2 * ring.y_lo, 2), pl.ds(4 * ring.r, 4)], own).start()


def give_back(ring, stage, result, send, recv, own):
    cols = pl.ds(pl.multiple_of(ring.s * COLS, COLS), COLS)

    @pl.loop(1, GROUP)
    def _(o):
        d = (ring.s + o) % GROUP
        half, quarter = Ring.parts(d)
        remote(stage.at[pl.ds(2 * half, 2), pl.ds(4 * quarter, 4)], result.at[:, :, cols], send, recv, Ring.at(ring.g, d)).start()

    pltpu.make_async_copy(stage.at[pl.ds(2 * ring.y_lo, 2), pl.ds(4 * ring.r, 4)], result.at[:, :, cols], own).start()


def await_blocks(flat, sem, own):
    take(flat, (GROUP - 1) * 2 * 4 * COLS, sem)
    take(flat, 2 * 4 * COLS, own)


def kernel(scale, clip_in, cotangent_in, first_kernel, second_kernel, critic_map, clip_grad, full_first, full_second,
           clip_a, act_a, second_a, first_a, first_w, first_wt, second_w, second_wt, clip, cotangent, stage, cot_f, slopes,
           turned, part, other, slots, near, piece, tiles,
           red_send, red_recv, halo_send, halo_recv, block_send, block_recv, block_own, weight_sem, load_sem):
    loads = [pltpu.make_async_copy(source, target, load_sem.at[i])
             for i, (source, target) in enumerate(((clip_in, clip), (cotangent_in, cotangent)))]
    for load in loads:
        load.start()
    me, ring = Place(), Ring()
    clips = Field(clip_a, ring, 2, 2, 1, False, halo_send.at[0], halo_recv.at[0])
    acts = Field(act_a, ring, 2, 1, 1, True, halo_send.at[1], halo_recv.at[1])
    seconds = Field(second_a, ring, 0, 1, -1, False, halo_send.at[2], halo_recv.at[2])
    firsts = Field(first_a, ring, 0, 1, -1, False, halo_send.at[3], halo_recv.at[3])
    fields = (clips, acts, seconds, firsts)
    first_sum, second_sum = (
        AllReduce(me, part.at[i], full, other.at[i], slots.at[i], near.at[i], piece.at[i], tiles.at[i],
                  red_send.at[i], red_recv.at[i])
        for i, full in enumerate((full_first, full_second)))

    for field in fields:
        field.clear()

    barrier = pltpu.get_barrier_semaphore()
    count = greet_reduce_peers(me, barrier)

    @pl.loop(1, GROUP)
    def _(o):
        pl.semaphore_signal(barrier, inc=1, device_id=Ring.at(ring.g, (ring.s + o) % GROUP), device_id_type=MESH)

    count = count + GROUP - 1
    for step in (-1, 1):
        for side in (-1, 0, 1):
            g, s = ring.g + step, ring.s + side
            there = (g >= 0) & (g < NG) & (s >= 0) & (s < GROUP)

            @pl.when(there)
            def _():
                pl.semaphore_signal(barrier, inc=1, device_id=Ring.at(g, s), device_id_type=MESH)

            count = count + jnp.where(there, 1, 0)
    build_weights(first_kernel, first_w, first_wt, weight_sem.at[0])
    for i in range(2):
        part[i, 27 * CH :, :] = jnp.zeros((CH, CH), BF16)
    loads[0].wait()
    pl.semaphore_wait(barrier, count)

    spread(ring, clip, stage.at[0], block_send.at[0], block_recv.at[0], block_own.at[0])
    loads[1].wait()
    spread(ring, cotangent, stage.at[1], block_send.at[1], block_recv.at[1], block_own.at[1])
    build_weights(second_kernel, second_w, second_wt, weight_sem.at[1])

    await_blocks(full_first, block_recv.at[0], block_own.at[0])
    for f in range(FR):
        clip_a[2 + f, 2 : COLS + 2] = swap(stage[0, f])
    clips.edges(0)
    clips.edges(1)
    clips.frames()
    await_weights(first_w, first_wt, weight_sem.at[0])
    await_weights(second_w, second_wt, weight_sem.at[1])
    clips.await_edges(0)
    clips.await_edges(1)

    def sigmoid_slope(z):
        sigma = jax.nn.sigmoid(z)
        return sigma, sigma * (1.0 + z * (1.0 - sigma))

    def first_layer(p):
        pre = convolve(clips, first_w, p, 0)
        sigma, slope = sigmoid_slope(pre)
        act = (pre * sigma).astype(BF16)
        for j in range(2):
            act_a[2 + 2 * p + j] = act[:, j * CH : (j + 1) * CH].reshape(COLS + 2, ROWN, CH)
        slopes[p] = slope[ROWN : ROWN + POS]
        pair, edge = pl.ds(2 + 2 * p, 2), jnp.zeros((2, ROWN, CH), BF16)

        @pl.when(ring.s == 0)
        def _():
            act_a[pair, 0] = edge

        @pl.when(ring.s == GROUP - 1)
        def _():
            act_a[pair, COLS + 1] = edge

    def second_layer(p):
        pre = convolve(acts, second_w, p, 0)
        sigma, slope = sigmoid_slope(pre)
        critic = pre * sigma
        delta = slope * jnp.concatenate(
            [cot_f[2 * p + j].reshape(POS, CH).astype(F32) for j in range(2)], axis=1)
        for j in range(2):
            half = slice(j * CH, (j + 1) * CH)
            stage[2, 2 * p + j] = swap(critic[:, half].astype(BF16).reshape(COLS, ROWN, CH))
            seconds.put(2 * p + j, delta[:, half])
        store_turned(turned, delta, p)

    def back_layer(p):
        delta = convolve(seconds, second_wt, p, 1) * slopes[p]
        for j in range(2):
            firsts.put(2 * p + j, delta[:, j * CH : (j + 1) * CH])
        store_turned(turned, delta, p)

    def input_layer(p):
        back = convolve(firsts, first_wt, p, 1)
        for j in range(2):
            stage[0, 2 * p + j] = swap(back[:, j * CH : (j + 1) * CH].astype(BF16).reshape(COLS, ROWN, CH))

    first_layer(1)
    acts.frames()
    clips.await_frames()
    first_layer(0)
    await_blocks(full_first, block_recv.at[1], block_own.at[1])
    for f in range(FR):
        cot_f[f] = swap(stage[1, f])
    second_layer(1)
    seconds.edges(1)
    acts.await_frames()
    second_layer(0)
    seconds.frames()
    seconds.edges(0)
    give_back(ring, stage.at[2], critic_map, block_send.at[2], block_recv.at[2], block_own.at[2])
    weight_grads(acts, turned, part.at[1], scale)
    second_sum.scatter_core()
    seconds.await_edges(0)
    seconds.await_edges(1)
    back_layer(0)
    firsts.frames()
    firsts.edges(0)
    second_sum.scatter_far()
    seconds.await_frames()
    back_layer(1)
    firsts.edges(1)
    second_sum.scatter_near()
    weight_grads(clips, turned, part.at[0], scale)
    first_sum.scatter_core()
    second_sum.scatter_z()
    take(full_first, (GROUP - 1) * 2 * 4 * COLS, block_send.at[0])
    firsts.await_edges(0)
    firsts.await_edges(1)
    first_sum.scatter_far()
    input_layer(0)
    firsts.await_frames()
    input_layer(1)
    second_sum.gather_z()
    first_sum.scatter_near()
    give_back(ring, stage.at[0], clip_grad, block_send.at[3], block_recv.at[3], block_own.at[3])
    second_sum.gather_near()
    first_sum.scatter_z()
    second_sum.gather_far()
    first_sum.gather_z()
    first_sum.gather_near()
    first_sum.gather_far()
    second_sum.gather_core()
    first_sum.gather_core()
    second_sum.finish()
    for field in fields:
        field.finish()
    for i in range(1, 4):
        take(full_first, (GROUP - 1) * 2 * 4 * COLS, block_send.at[i])
    for i in range(2, 4):
        await_blocks(full_first, block_recv.at[i], block_own.at[i])
    first_sum.finish()


def write_out(critic_in, grad_in, first_in, second_in, critic, grad, first, second):
    critic[...] = critic_in[...]
    grad[...] = grad_in[...]
    first[...] = first_in[...].astype(F32)
    second[...] = second_in[...].astype(F32)


def on_device(clip, first_kernel, second_kernel, cotangent):
    cells = clip.shape[0] * lax.axis_size("frame") * clip.shape[1] * lax.axis_size("row") * clip.shape[2]
    scale = 1.0 / float(cells) ** 0.5
    vmem, anywhere = pl.BlockSpec(memory_space=pltpu.VMEM), pl.BlockSpec(memory_space=pl.ANY)
    total = jax.ShapeDtypeStruct((ROWS, CH), BF16)
    dma = pltpu.SemaphoreType.DMA
    flat = (2 * 4 * GROUP * COLS, CH)

    def field(halo):
        return pltpu.VMEM((FR + 2, COLS + 2 * halo, ROWN, CH), BF16)

    results = pl.pallas_call(
        functools.partial(kernel, scale),
        out_shape=(jax.ShapeDtypeStruct(clip.shape, BF16), jax.ShapeDtypeStruct(clip.shape, BF16), total, total),
        in_specs=[anywhere] * 4,
        out_specs=(vmem, vmem, vmem, vmem),
        scratch_shapes=[
            field(2), field(1), field(1), field(1),
            pltpu.VMEM((12 * CH, 6 * CH), BF16), pltpu.VMEM((6 * CH, 12 * CH), BF16),
            pltpu.VMEM((12 * CH, 6 * CH), BF16), pltpu.VMEM((6 * CH, 12 * CH), BF16),
            pltpu.VMEM(clip.shape, BF16), pltpu.VMEM(clip.shape, BF16),
            pltpu.VMEM((3, FR, ROWN, COLS, CH), BF16),
            pltpu.VMEM((FR, COLS, ROWN, CH), BF16),
            pltpu.VMEM((2, POS, 2 * CH), F32),
            pltpu.VMEM((6 * CH, 2 * POS), BF16),
            pltpu.VMEM((2, ROWS, CH), BF16),
            pltpu.VMEM((2, HALF, CH), BF16),
            pltpu.VMEM((2, HALF, CH), BF16),
            pltpu.VMEM((2, HALF // 4, CH), BF16),
            pltpu.VMEM((2, BLK, CH), BF16),
            pltpu.VMEM((2, NZ * TILE, CH), BF16),
            dma((2, 8)), dma((2, 8)), dma((4, 7)), dma((4, 7)), dma((4,)), dma((4,)), dma((4,)), dma((2, 2)), dma((2,)),
        ],
        compiler_params=pltpu.CompilerParams(collective_id=0, has_side_effects=True, vmem_limit_bytes=60 << 20),
    )(clip, cotangent, first_kernel.reshape(27, CH, CH), second_kernel.reshape(27, CH, CH))
    critic_map, clip_grad, first, second = results

    steps = 4
    maps, grads = (pl.BlockSpec((rows // steps, CH), lambda i: (i, 0)) for rows in (flat[0], 27 * CH))
    whole = jax.ShapeDtypeStruct((27 * CH, CH), F32)
    critic_map, clip_grad, first, second = pl.pallas_call(
        write_out,
        grid=(steps,),
        out_shape=(jax.ShapeDtypeStruct(flat, BF16), jax.ShapeDtypeStruct(flat, BF16), whole, whole),
        in_specs=[maps, maps, grads, grads],
        out_specs=(maps, maps, grads, grads),
    )(critic_map.reshape(flat), clip_grad.reshape(flat), first, second)
    taps = (3, 3, 3, CH, CH)
    return critic_map.reshape(clip.shape), clip_grad.reshape(clip.shape), first.reshape(taps), second.reshape(taps)


def solution(mesh):
    placed = (P("frame", "row", None, None), P(), P(), P("frame", "row", None, None))
    return jax.shard_map(
        on_device,
        mesh=mesh,
        in_specs=placed,
        out_specs=(P("frame", "row", None, None), P("frame", "row", None, None), P(), P()),
        check_vma=False,
    )
```

```python
import functools

import jax
import jax.numpy as jnp
from jax import lax
from jax.experimental import pallas as pl
from jax.experimental.pallas import tpu as pltpu
from jax.sharding import PartitionSpec as P

MESH = pl.DeviceIdType.MESH
BF16, F32 = jnp.bfloat16, jnp.float32
CH = 128

NX, NY, NZ = 4, 4, 8
NXY = NX * NY
BLK = 112
HALF = NXY * BLK
ROWS = 2 * HALF
TILE = 16
ZT = BLK // TILE


class Place:
    def __init__(self):
        f, r = lax.axis_index("frame"), lax.axis_index("row")
        self.x, self.z = f // (2 * NZ), (f // 2) % NZ
        self.y, self.core = (r // 2) * 2 + f % 2, r % 2
        self.p = self.x * NY + self.y

    @staticmethod
    def at(x, y, z, core):
        return ((x * NZ + z) * 2 + y % 2, (y // 2) * 2 + core)


def remote(src, dst, send, recv, device):
    return pltpu.make_async_remote_copy(
        src_ref=src, dst_ref=dst, send_sem=send, recv_sem=recv, device_id=device, device_id_type=MESH)


def take(ref, rows, sem):
    view = ref.at[pl.ds(0, rows)]
    pltpu.make_async_copy(view, view, sem).wait()


def rows_of(start, size):
    return pl.ds(pl.multiple_of(start, TILE), size)


class AllReduce:
    A, B = (256, 64), (192, 48)
    START_B = NX * 256

    def __init__(self, me, part, full, other, slots, near, piece, tiles, send, recv):
        self.me, self.part, self.full = me, part, full
        self.other, self.slots, self.near, self.piece, self.tiles = other, slots, near, piece, tiles
        self.send, self.recv = send, recv
        self.base = me.core * HALF

    def x_peer(self, o):
        x = (self.me.x + o) % NX
        return x, Place.at(x, self.me.y, self.me.z, self.me.core)

    def y_peer(self, o):
        y = (self.me.y + o) % NY
        return y, Place.at(self.me.x, y, self.me.z, self.me.core)

    def z_peer(self, o):
        d = (self.me.z + o) % NZ
        return d, Place.at(self.me.x, self.me.y, d, self.me.core)

    def twin(self):
        return Place.at(self.me.x, self.me.y, self.me.z, 1 - self.me.core)

    def row_a(self, x, y):
        return self.base + x * self.A[0] + y * self.A[1]

    def row_b(self, x, y):
        return self.base + self.START_B + y * self.B[0] + x * self.B[1]

    def push(self, stage, source, start, target, to, size, peer):
        remote(source.at[rows_of(start, size)], target.at[rows_of(to, size)], self.send.at[stage], self.recv.at[stage], peer).start()

    def scatter_core(self):
        self.push(0, self.part, (1 - self.me.core) * HALF, self.other, 0, HALF, self.twin())

    def scatter_far(self):
        me = self.me
        take(self.other, HALF, self.recv.at[0])

        @pl.loop(0, HALF // 128)
        def _(i):
            mine = rows_of(self.base + i * 128, 128)
            total = self.part[mine, :].astype(F32) + self.other[rows_of(i * 128, 128), :].astype(F32)
            self.part[mine, :] = total.astype(BF16)

        @pl.loop(1, NX)
        def _(o):
            x, peer = self.x_peer(o)
            self.push(1, self.part, self.row_a(x, 0), self.slots, me.x * self.A[0], self.A[0], peer)
            y, peer = self.y_peer(o)
            self.push(1, self.part, self.row_b(0, y), self.slots, self.START_B + me.y * self.B[0], self.B[0], peer)

    def scatter_near(self):
        me = self.me
        take(self.slots, 3 * (self.A[0] + self.B[0]), self.recv.at[1])

        @pl.loop(0, 4)
        def _(i):
            for start, slot, mine, pitch, size in (
                (self.row_a(me.x, 0), 0, me.x, self.A[0], self.A[1]),
                (self.row_b(0, me.y), self.START_B, me.y, self.B[0], self.B[1])):
                rows = rows_of(start + i * size, size)
                total = self.part[rows, :].astype(F32)
                for o in range(1, 4):
                    total = total + self.slots[rows_of(slot + ((mine + o) % 4) * pitch + i * size, size), :].astype(F32)
                self.part[rows, :] = total.astype(BF16)

        @pl.loop(1, NX)
        def _(o):
            y, peer = self.y_peer(o)
            self.push(2, self.part, self.row_a(me.x, y), self.near, me.y * self.A[1], self.A[1], peer)
            x, peer = self.x_peer(o)
            self.push(2, self.part, self.row_b(x, me.y), self.near, NY * self.A[1] + me.x * self.B[1], self.B[1], peer)

    def scatter_z(self):
        me = self.me
        take(self.near, 3 * (self.A[1] + self.B[1]), self.recv.at[2])
        for start, slot, mine, size, to in (
            (self.row_a(me.x, me.y), 0, me.y, self.A[1], 0),
            (self.row_b(me.x, me.y), NY * self.A[1], me.x, self.B[1], self.A[1])):
            total = self.part[rows_of(start, size), :].astype(F32)
            for o in range(1, 4):
                total = total + self.near[rows_of(slot + ((mine + o) % 4) * size, size), :].astype(F32)
            self.piece[to : to + size, :] = total.astype(BF16)

        @pl.loop(1, NZ)
        def _(o):
            d, peer = self.z_peer(o)

            @pl.when(d < ZT)
            def _():
                self.push(3, self.piece, d * TILE, self.tiles, me.z * TILE, TILE, peer)

    def gather_z(self):
        me = self.me

        @pl.when(me.z < ZT)
        def _():
            take(self.tiles, (NZ - 1) * TILE, self.recv.at[3])
            total = self.piece[rows_of(me.z * TILE, TILE), :].astype(F32)
            for o in range(1, NZ):
                d = (me.z + o) % NZ
                total = total + self.tiles[rows_of(d * TILE, TILE), :].astype(F32)
            in_a = self.A[1] // TILE
            row = jnp.where(me.z < in_a, self.row_a(me.x, me.y) + me.z * TILE, self.row_b(me.x, me.y) + (me.z - in_a) * TILE)
            self.full[rows_of(row, TILE), :] = total.astype(BF16)

            @pl.loop(1, NZ)
            def _(o):
                d, peer = self.z_peer(o)
                self.push(4, self.full, row, self.full, row, TILE, peer)

    def gather_near(self):
        me = self.me

        @pl.when(me.z < ZT)
        def _():
            take(self.full, (ZT - 1) * TILE, self.recv.at[4])

        @pl.when(me.z >= ZT)
        def _():
            take(self.full, ZT * TILE, self.recv.at[4])

        a, b = self.row_a(me.x, me.y), self.row_b(me.x, me.y)

        @pl.loop(1, NX)
        def _(o):
            self.push(5, self.full, a, self.full, a, self.A[1], self.y_peer(o)[1])
            self.push(5, self.full, b, self.full, b, self.B[1], self.x_peer(o)[1])

    def gather_far(self):
        me = self.me
        take(self.full, 3 * (self.A[1] + self.B[1]), self.recv.at[5])
        a, b = self.row_a(me.x, 0), self.row_b(0, me.y)

        @pl.loop(1, NX)
        def _(o):
            self.push(6, self.full, a, self.full, a, self.A[0], self.x_peer(o)[1])
            self.push(6, self.full, b, self.full, b, self.B[0], self.y_peer(o)[1])

    def gather_core(self):
        take(self.full, 3 * (self.A[0] + self.B[0]), self.recv.at[6])
        self.push(7, self.full, self.base, self.full, self.base, HALF, self.twin())

    def finish(self):
        me = self.me
        take(self.full, HALF, self.recv.at[7])
        take(self.part, HALF, self.send.at[0])
        take(self.part, 3 * (self.A[0] + self.B[0]), self.send.at[1])
        take(self.part, 3 * (self.A[1] + self.B[1]), self.send.at[2])

        @pl.when(me.z < ZT)
        def _():
            take(self.piece, (ZT - 1) * TILE, self.send.at[3])
            take(self.full, (NZ - 1) * TILE, self.send.at[4])

        @pl.when(me.z >= ZT)
        def _():
            take(self.piece, ZT * TILE, self.send.at[3])

        take(self.full, 3 * (self.A[1] + self.B[1]), self.send.at[5])
        take(self.full, 3 * (self.A[0] + self.B[0]), self.send.at[6])
        take(self.full, HALF, self.send.at[7])


def greet_reduce_peers(me, barrier):
    pl.semaphore_signal(barrier, inc=1, device_id=Place.at(me.x, me.y, me.z, 1 - me.core), device_id_type=MESH)

    @pl.loop(1, NXY)
    def _(o):
        p = (me.p + o) % NXY
        pl.semaphore_signal(barrier, inc=1, device_id=Place.at(p // NY, p % NY, me.z, me.core), device_id_type=MESH)

    @pl.loop(1, NZ)
    def _(o):
        d = (me.z + o) % NZ
        pl.semaphore_signal(barrier, inc=1, device_id=Place.at(me.x, me.y, d, me.core), device_id_type=MESH)

    return 1 + NXY - 1 + NZ - 1

GROUP, FR, COLS, ROWN = 8, 4, 32, 16
POS = COLS * ROWN
NG = NX * NZ


class Ring:
    def __init__(self):
        f, r = lax.axis_index("frame"), lax.axis_index("row")
        self.g, self.y_lo, self.r = f // 2, f % 2, r
        self.s = (r // 2) * 4 + self.y_lo * 2 + r % 2

    @staticmethod
    def parts(s):
        return (s // 2) % 2, (s // 4) * 2 + s % 2

    @staticmethod
    def at(g, s):
        y_lo, r = Ring.parts(s)
        return (g * 2 + y_lo, r)


class Field:
    def __init__(self, ref, ring, own, halo, step, whole, send, recv):
        self.ref, self.ring, self.own, self.halo, self.step, self.whole = ref, ring, own, halo, step, whole
        self.send, self.recv = send, recv
        self.width = COLS + 2 * halo

    def clear(self):
        far = 0 if self.own else FR
        self.ref[far : far + 2] = jnp.zeros((2, self.width, ROWN, CH), BF16)
        for col in (0, COLS + self.halo):
            self.ref[self.own : self.own + FR, col : col + self.halo] = jnp.zeros((FR, self.halo, ROWN, CH), BF16)

    def put(self, f, start, value):
        width = value.shape[0] // ROWN
        self.ref[self.own + f, self.halo + start : self.halo + start + width] = value.astype(BF16).reshape(width, ROWN, CH)

    def to_left(self):
        return self.ring.s > 0

    def to_right(self):
        return self.ring.s < GROUP - 1

    def has_target(self):
        return self.ring.g < NG - 1 if self.step > 0 else self.ring.g > 0

    def has_source(self):
        return self.ring.g > 0 if self.step > 0 else self.ring.g < NG - 1

    def copy(self, frames, col, to_frames, to_col, width, g, s, i):
        return remote(self.ref.at[frames, pl.ds(col, width)], self.ref.at[to_frames, pl.ds(to_col, width)],
                      self.send.at[i], self.recv.at[i], Ring.at(g, s))

    def edge(self, frames, to_frames, side, g, i):
        halo, s = self.halo, self.ring.s
        source, target = (halo, COLS + halo) if side < 0 else (COLS, 0)
        self.copy(frames, source, to_frames, target, halo, g, s + side, i).start()

    def edges(self, q):
        frames, i = self._pair(q)

        @pl.when(self._held(q) & self.to_left())
        def _():
            self.edge(frames, frames, -1, self.ring.g, i)

        @pl.when(self._held(q) & self.to_right())
        def _():
            self.edge(frames, frames, 1, self.ring.g, i + 1)

    def _pair(self, q):
        return pl.ds(self.own + 2 * q, 2), (2 * q) % 6

    def _held(self, q):
        return self.has_source() if q < 0 else self.ring.g >= 0

    def await_edges(self, q):
        self._edges(q, self.recv, self.to_right(), self.to_left())

    def _edges(self, q, sem, left, right):
        frames, i = self._pair(q)
        view = self.ref.at[frames, pl.ds(0, self.halo)]

        @pl.when(self._held(q) & left)
        def _():
            pltpu.make_async_copy(view, view, sem.at[i]).wait()

        @pl.when(self._held(q) & right)
        def _():
            pltpu.make_async_copy(view, view, sem.at[i + 1]).wait()

    def span(self):
        return (0, self.width) if self.whole else (self.halo, COLS)

    def frames(self):
        g, s = self.ring.g + self.step, self.ring.s
        mine, theirs = (pl.ds(FR, 2), pl.ds(0, 2)) if self.step > 0 else (pl.ds(0, 2), pl.ds(FR, 2))
        start, width = self.span()

        @pl.when(self.has_target())
        def _():
            self.copy(mine, start, theirs, start, width, g, s, 4).start()

        if self.whole:
            return

        @pl.when(self.has_target() & self.to_left())
        def _():
            self.edge(mine, theirs, -1, g, 5)

        @pl.when(self.has_target() & self.to_right())
        def _():
            self.edge(mine, theirs, 1, g, 6)

    def _frames(self, sem, there, left, right):
        start, width = self.span()
        body, col = self.ref.at[pl.ds(0, 2), pl.ds(start, width)], self.ref.at[pl.ds(0, 2), pl.ds(0, self.halo)]

        @pl.when(there)
        def _():
            pltpu.make_async_copy(body, body, sem.at[4]).wait()

        if self.whole:
            return

        @pl.when(there & left)
        def _():
            pltpu.make_async_copy(col, col, sem.at[5]).wait()

        @pl.when(there & right)
        def _():
            pltpu.make_async_copy(col, col, sem.at[6]).wait()

    def await_frames(self):
        self._frames(self.recv, self.has_source(), self.to_right(), self.to_left())

    def finish(self):
        if not self.whole:
            for q in range(-1 if self.step > 0 else 0, 2):
                self._edges(q, self.send, self.to_left(), self.to_right())
        if self.whole or self.step < 0:
            self._frames(self.send, self.has_target(), self.to_left(), self.to_right())

    def slab(self, p, k, start, width):
        return self.ref[2 * p + k, start : start + width].reshape(width * ROWN, CH)


def build_weights(kernel, ahead, back, sem):
    zero = jnp.zeros((CH, CH), BF16)
    for k, j in ((0, 1), (3, 0)):
        @pl.loop(0, 9)
        def _(bc):
            b, c = bc // 3, bc % 3
            ahead[pl.ds(pl.multiple_of((c * 4 + k) * CH, CH), CH), pl.ds(pl.multiple_of((b * 2 + j) * CH, CH), CH)] = zero
            back[pl.ds(pl.multiple_of((b * 2 + j) * CH, CH), CH), pl.ds(pl.multiple_of((c * 4 + k) * CH, CH), CH)] = zero

    @pl.loop(0, 27)
    def _(tap):
        a, b, c = tap // 9, (tap // 3) % 3, tap % 3
        for j in range(2):
            k = a + j
            pltpu.make_async_copy(
                kernel.at[tap],
                ahead.at[pl.ds(pl.multiple_of((c * 4 + k) * CH, CH), CH), pl.ds(pl.multiple_of((b * 2 + j) * CH, CH), CH)],
                sem.at[0]).start()
            k = j + 2 - a
            pltpu.make_async_copy(
                kernel.at[tap],
                back.at[pl.ds(pl.multiple_of(((2 - b) * 2 + j) * CH, CH), CH), pl.ds(pl.multiple_of(((2 - c) * 4 + k) * CH, CH), CH)],
                sem.at[1]).start()


def await_weights(ahead, back, sem):
    view = ahead.at[pl.ds(0, 54 * CH * CH // ahead.shape[1])]
    pltpu.make_async_copy(view, view, sem.at[0]).wait()
    view = back.at[pl.ds(0, 54 * CH * CH // back.shape[1])]
    pltpu.make_async_copy(view, view, sem.at[1]).wait()


def row_index(shape):
    return lax.broadcasted_iota(jnp.int32, shape, 0) % ROWN


def from_above(value):
    return jnp.where(row_index(value.shape) == 0, 0.0, pltpu.roll(value, 1, axis=0))


def from_below(value):
    return jnp.where(row_index(value.shape) == ROWN - 1, 0.0, pltpu.roll(value, value.shape[0] - 1, axis=0))


def convolve(field, weights, p, contract, start, width):
    lhs = jnp.concatenate([field.slab(p, k, start + c, width) for c in range(3) for k in range(4)], axis=1)
    rows = lax.dot_general(lhs, weights[...], (((1,), (contract,)), ((), ())), preferred_element_type=F32)
    above, level, below = (rows[:, b * 2 * CH : (b + 1) * 2 * CH] for b in range(3))
    return level + from_above(above) + from_below(below)


def store_turned(turned, delta, start):
    for b, value in enumerate((from_below(delta), delta, from_above(delta))):
        turned[b * 2 * CH : (b + 1) * 2 * CH, start : start + delta.shape[0]] = value.astype(BF16).T


def pair_sums(field, turned, p, c):
    rhs = jnp.concatenate([field.slab(p, k, field.halo - 1 + c, COLS) for k in range(4)], axis=1)
    return lax.dot_general(turned[:, p * POS : (p + 1) * POS], rhs, (((1,), (0,)), ((), ())), preferred_element_type=F32)


def begin_grads(field, turned, begun, p):
    for c in range(3):
        begun[c] = pair_sums(field, turned, p, c)


def weight_grads(field, turned, part, scale, begun=None):
    for c in range(3):
        if begun is None:
            rhs = jnp.concatenate(
                [jnp.concatenate([field.slab(p, k, field.halo - 1 + c, COLS) for k in range(4)], axis=1) for p in range(2)], axis=0)
            sums = lax.dot_general(turned[...], rhs, (((1,), (0,)), ((), ())), preferred_element_type=F32)
        else:
            sums = begun[c] + pair_sums(field, turned, 1, c)
        for b in range(3):
            for a in range(3):
                one = sums[2 * b * CH : (2 * b + 1) * CH, a * CH : (a + 1) * CH]
                two = sums[(2 * b + 1) * CH : (2 * b + 2) * CH, (a + 1) * CH : (a + 2) * CH]
                tap = (a * 3 + b) * 3 + c
                part[tap * CH : (tap + 1) * CH, :] = ((one + two) * scale).T.astype(BF16)


def swap(value):
    return jnp.swapaxes(value, 0, 1)


def spread(ring, source, stage, send, recv, own):
    @pl.loop(1, GROUP)
    def _(o):
        d = (ring.s + o) % GROUP
        cols = pl.ds(pl.multiple_of(d * COLS, COLS), COLS)
        remote(source.at[:, :, cols], stage.at[pl.ds(2 * ring.y_lo, 2), pl.ds(4 * ring.r, 4)], send, recv, Ring.at(ring.g, d)).start()

    cols = pl.ds(pl.multiple_of(ring.s * COLS, COLS), COLS)
    pltpu.make_async_copy(source.at[:, :, cols], stage.at[pl.ds(2 * ring.y_lo, 2), pl.ds(4 * ring.r, 4)], own).start()


def relay(ring, stage, flat, recv, own, ahead, there, send, landed):
    for turn in (0, 3, 1, 2):
        for core in range(2):
            s = (ring.s + 2 * turn) % GROUP // 2 * 2 + core
            half, quarter = Ring.parts(s)

            @pl.when(s == ring.s)
            def _():
                take(flat, 2 * 4 * COLS, own)

            @pl.when(s != ring.s)
            def _():
                take(flat, 2 * 4 * COLS, recv.at[s])

            @pl.when(there & (half == 1))
            def _():
                rows = pl.ds(4 * quarter, 4)
                remote(stage.at[pl.ds(2, 2), rows], ahead.at[:, rows], send, landed, Ring.at(ring.g + 1, ring.s)).start()


def give_back(ring, stage, result, send, recv, own, half):
    cols = pl.ds(pl.multiple_of(ring.s * COLS, COLS), COLS)
    pair = pl.ds(2 * half, 2)

    @pl.loop(0, 4)
    def _(i):
        quarter = (ring.r + i) % 4
        rows = pl.ds(4 * quarter, 4)
        here = (half == ring.y_lo) & (i == 0)

        @pl.when(here)
        def _():
            pltpu.make_async_copy(stage.at[pair, rows], result.at[:, :, cols], own).start()

        @pl.when(jnp.logical_not(here))
        def _():
            remote(stage.at[pair, rows], result.at[:, :, cols], send, recv, (ring.g * 2 + half, quarter)).start()


def await_blocks(flat, sem, own):
    take(flat, (GROUP - 1) * 2 * 4 * COLS, sem)
    take(flat, 2 * 4 * COLS, own)


def kernel(scale, clip_in, cotangent_in, first_kernel, second_kernel, critic_map, clip_grad, full_first, full_second,
           clip_a, act_a, second_a, first_a, first_w, first_wt, second_w, second_wt, clip, cotangent, stage, cot_f, slopes,
           turned, begun, part, other, slots, near, piece, tiles,
           red_send, red_recv, halo_send, halo_recv, block_send, block_recv, block_own, weight_sem, load_sem,
           ahead, clip_recv, ahead_sem):
    loads = [pltpu.make_async_copy(source, target, load_sem.at[i])
             for i, (source, target) in enumerate(((clip_in, clip), (cotangent_in, cotangent)))]
    for load in loads:
        load.start()
    me, ring = Place(), Ring()
    clips = Field(clip_a, ring, 2, 2, 1, False, halo_send.at[0], halo_recv.at[0])
    acts = Field(act_a, ring, 2, 1, 1, True, halo_send.at[1], halo_recv.at[1])
    seconds = Field(second_a, ring, 0, 1, -1, False, halo_send.at[2], halo_recv.at[2])
    firsts = Field(first_a, ring, 0, 1, -1, False, halo_send.at[3], halo_recv.at[3])
    fields = (clips, acts, seconds, firsts)
    first_sum, second_sum = (
        AllReduce(me, part.at[i], full, other.at[i], slots.at[i], near.at[i], piece.at[i], tiles.at[i],
                  red_send.at[i], red_recv.at[i])
        for i, full in enumerate((full_first, full_second)))

    for field in fields:
        field.clear()

    barrier = pltpu.get_barrier_semaphore()
    count = greet_reduce_peers(me, barrier)

    @pl.loop(1, GROUP)
    def _(o):
        pl.semaphore_signal(barrier, inc=1, device_id=Ring.at(ring.g, (ring.s + o) % GROUP), device_id_type=MESH)

    count = count + GROUP - 1
    for step in (-1, 1):
        for side in (-1, 0, 1):
            g, s = ring.g + step, ring.s + side
            there = (g >= 0) & (g < NG) & (s >= 0) & (s < GROUP)

            @pl.when(there)
            def _():
                pl.semaphore_signal(barrier, inc=1, device_id=Ring.at(g, s), device_id_type=MESH)

            count = count + jnp.where(there, 1, 0)
    build_weights(first_kernel, first_w, first_wt, weight_sem.at[0])
    for i in range(2):
        part[i, 27 * CH :, :] = jnp.zeros((CH, CH), BF16)
    loads[0].wait()
    pl.semaphore_wait(barrier, count)

    spread(ring, clip, stage.at[0], block_send.at[0], clip_recv.at[ring.s], block_own.at[0])
    build_weights(second_kernel, second_w, second_wt, weight_sem.at[1])

    relay(ring, stage.at[0], full_first, clip_recv, block_own.at[0], ahead, clips.has_target(), ahead_sem.at[0], ahead_sem.at[1])
    for f in range(FR):
        clip_a[2 + f, 2 : COLS + 2] = swap(stage[0, f])
    clips.edges(0)
    clips.edges(1)
    loads[1].wait()
    spread(ring, cotangent, stage.at[1], block_send.at[1], block_recv.at[1], block_own.at[1])
    await_weights(first_w, first_wt, weight_sem.at[0])
    await_weights(second_w, second_wt, weight_sem.at[1])
    clips.await_edges(0)
    clips.await_edges(1)

    def sigmoid_slope(z):
        sigma = jax.nn.sigmoid(z)
        return sigma, sigma * (1.0 + z * (1.0 - sigma))

    def first_layer(p):
        width = COLS // 2 + 1
        for half in range(2):
            start = half * width
            pre = convolve(clips, first_w, p, 0, start, width)
            sigma, slope = sigmoid_slope(pre)
            act = (pre * sigma).astype(BF16)
            for j in range(2):
                act_a[2 + 2 * p + j, start : start + width] = act[:, j * CH : (j + 1) * CH].reshape(width, ROWN, CH)
            skip = ROWN if half == 0 else 0
            slopes[p, half * POS // 2 : (half + 1) * POS // 2] = slope[skip : skip + POS // 2]
        pair, edge = pl.ds(2 + 2 * p, 2), jnp.zeros((2, ROWN, CH), BF16)

        @pl.when(ring.s == 0)
        def _():
            act_a[pair, 0] = edge

        @pl.when(ring.s == GROUP - 1)
        def _():
            act_a[pair, COLS + 1] = edge

    width = COLS // 2

    def second_layer(p):
        for start in (0, width):
            pre = convolve(acts, second_w, p, 0, start, width)
            sigma, slope = sigmoid_slope(pre)
            critic = pre * sigma
            delta = slope * jnp.concatenate(
                [cot_f[2 * p + j, start : start + width].reshape(width * ROWN, CH).astype(F32) for j in range(2)], axis=1)
            for j in range(2):
                half = slice(j * CH, (j + 1) * CH)
                stage[2, 2 * p + j, :, start : start + width] = swap(critic[:, half].astype(BF16).reshape(width, ROWN, CH))
                seconds.put(2 * p + j, start, delta[:, half])
            store_turned(turned, delta, p * POS + start * ROWN)

    def back_layer(p):
        for start in (0, width):
            rows = slice(start * ROWN, (start + width) * ROWN)
            delta = convolve(seconds, second_wt, p, 1, start, width) * slopes[p, rows]
            for j in range(2):
                firsts.put(2 * p + j, start, delta[:, j * CH : (j + 1) * CH])
            store_turned(turned, delta, p * POS + start * ROWN)

    def input_layer(p):
        for start in (0, width):
            back = convolve(firsts, first_wt, p, 1, start, width)
            for j in range(2):
                stage[0, 2 * p + j, :, start : start + width] = swap(
                    back[:, j * CH : (j + 1) * CH].astype(BF16).reshape(width, ROWN, CH))

    def give_critic(half):
        give_back(ring, stage.at[2], critic_map, block_send.at[2], block_recv.at[2], block_own.at[2], half)

    def give_grad(half):
        give_back(ring, stage.at[0], clip_grad, block_send.at[3], block_recv.at[3], block_own.at[3], half)

    first_layer(1)
    acts.frames()

    @pl.when(clips.has_source())
    def _():
        take(full_first, 4 * 2 * 4 * COLS, ahead_sem.at[1])
        for f in range(2):
            clip_a[f, 2 : COLS + 2] = swap(ahead[f])

    clips.edges(-1)
    await_blocks(full_first, block_recv.at[1], block_own.at[1])
    for f in range(FR):
        cot_f[f] = swap(stage[1, f])
    clips.await_edges(-1)
    first_layer(0)
    second_layer(1)
    seconds.edges(1)
    give_critic(1)
    acts.await_frames()
    second_layer(0)
    seconds.frames()
    seconds.edges(0)
    give_critic(0)
    weight_grads(acts, turned, part.at[1], scale)
    second_sum.scatter_core()
    seconds.await_edges(0)
    seconds.await_edges(1)
    back_layer(0)
    second_sum.scatter_far()
    firsts.edges(0)

    @pl.when(me.z != 0)
    def _():
        firsts.frames()

    begin_grads(clips, turned, begun, 0)
    seconds.await_frames()
    back_layer(1)
    firsts.edges(1)
    weight_grads(clips, turned, part.at[0], scale, begun)
    first_sum.scatter_core()
    second_sum.scatter_near()
    firsts.await_edges(0)
    firsts.await_edges(1)
    first_sum.scatter_far()
    take(full_first, (GROUP - 1) * 2 * 4 * COLS, block_send.at[0])

    @pl.when(clips.has_target())
    def _():
        take(full_first, 4 * 2 * 4 * COLS, ahead_sem.at[0])

    input_layer(0)
    second_sum.scatter_z()
    first_sum.scatter_near()

    @pl.when(me.z != NZ - 1)
    def _():
        firsts.await_frames()
        input_layer(1)

    give_grad(0)

    @pl.when(me.z != NZ - 1)
    def _():
        give_grad(1)

    second_sum.gather_z()
    first_sum.scatter_z()

    @pl.when(me.z == 0)
    def _():
        firsts.frames()

    second_sum.gather_near()

    @pl.when(me.z == NZ - 1)
    def _():
        firsts.await_frames()
        input_layer(1)
        give_grad(1)

    second_sum.gather_far()
    first_sum.gather_z()
    first_sum.gather_near()
    second_sum.gather_core()
    first_sum.gather_far()
    second_sum.finish()
    for field in fields:
        field.finish()
    for i in range(1, 4):
        take(full_first, (GROUP - 1) * 2 * 4 * COLS, block_send.at[i])
    for i in range(2, 4):
        await_blocks(full_first, block_recv.at[i], block_own.at[i])
    first_sum.gather_core()
    first_sum.finish()


def write_out(critic_in, grad_in, first_in, second_in, critic, grad, first, second, wide, sem):
    half = 27 * CH // 2
    stores = []
    for n, (source, target) in enumerate(((first_in, first), (second_in, second))):
        for h in range(2):
            i = 2 * n + h

            @pl.loop(0, half // 192)
            def _(k):
                wide[i, rows_of(k * 192, 192), :] = source[rows_of(h * half + k * 192, 192), :].astype(F32)

            stores.append(pltpu.make_async_copy(wide.at[i], target.at[pl.ds(h * half, half)], sem.at[i]))
            stores[-1].start()
    for n, (source, target) in enumerate(((critic_in, critic), (grad_in, grad))):
        stores.append(pltpu.make_async_copy(source, target, sem.at[4 + n]))
        stores[-1].start()
    for one in stores:
        one.wait()


def on_device(clip, first_kernel, second_kernel, cotangent):
    cells = clip.shape[0] * lax.axis_size("frame") * clip.shape[1] * lax.axis_size("row") * clip.shape[2]
    scale = 1.0 / float(cells) ** 0.5
    vmem, anywhere = pl.BlockSpec(memory_space=pltpu.VMEM), pl.BlockSpec(memory_space=pl.ANY)
    total = jax.ShapeDtypeStruct((ROWS, CH), BF16)
    dma = pltpu.SemaphoreType.DMA
    flat = (2 * 4 * GROUP * COLS, CH)

    def field(halo):
        return pltpu.VMEM((FR + 2, COLS + 2 * halo, ROWN, CH), BF16)

    results = pl.pallas_call(
        functools.partial(kernel, scale),
        out_shape=(jax.ShapeDtypeStruct(clip.shape, BF16), jax.ShapeDtypeStruct(clip.shape, BF16), total, total),
        in_specs=[pl.BlockSpec(memory_space=pltpu.HBM)] * 4,
        out_specs=(vmem, vmem, vmem, vmem),
        scratch_shapes=[
            field(2), field(1), field(1), field(1),
            pltpu.VMEM((12 * CH, 6 * CH), BF16), pltpu.VMEM((6 * CH, 12 * CH), BF16),
            pltpu.VMEM((12 * CH, 6 * CH), BF16), pltpu.VMEM((6 * CH, 12 * CH), BF16),
            pltpu.VMEM(clip.shape, BF16), pltpu.VMEM(clip.shape, BF16),
            pltpu.VMEM((3, FR, ROWN, COLS, CH), BF16),
            pltpu.VMEM((FR, COLS, ROWN, CH), BF16),
            pltpu.VMEM((2, POS, 2 * CH), F32),
            pltpu.VMEM((6 * CH, 2 * POS), BF16),
            pltpu.VMEM((3, 6 * CH, 4 * CH), F32),
            pltpu.VMEM((2, ROWS, CH), BF16),
            pltpu.VMEM((2, HALF, CH), BF16),
            pltpu.VMEM((2, HALF, CH), BF16),
            pltpu.VMEM((2, HALF // 4, CH), BF16),
            pltpu.VMEM((2, BLK, CH), BF16),
            pltpu.VMEM((2, NZ * TILE, CH), BF16),
            dma((2, 8)), dma((2, 8)), dma((4, 7)), dma((4, 7)), dma((4,)), dma((4,)), dma((4,)), dma((2, 2)), dma((2,)),
            pltpu.VMEM((2, ROWN, COLS, CH), BF16), dma((GROUP,)), dma((2,)),
        ],
        compiler_params=pltpu.CompilerParams(collective_id=0, has_side_effects=True, vmem_limit_bytes=38 << 20),
    )(*(pltpu.with_memory_space_constraint(one, pltpu.HBM) for one in (
        clip, cotangent, first_kernel.reshape(27, CH, CH), second_kernel.reshape(27, CH, CH))))
    critic_map, clip_grad, first, second = results

    whole = jax.ShapeDtypeStruct((27 * CH, CH), F32)
    critic_map, clip_grad, first, second = pl.pallas_call(
        write_out,
        out_shape=(jax.ShapeDtypeStruct(flat, BF16), jax.ShapeDtypeStruct(flat, BF16), whole, whole),
        in_specs=[vmem] * 4,
        out_specs=(anywhere,) * 4,
        scratch_shapes=[pltpu.VMEM((4, 27 * CH // 2, CH), F32), dma((6,))],
        compiler_params=pltpu.CompilerParams(vmem_limit_bytes=10 << 20),
    )(critic_map.reshape(flat), clip_grad.reshape(flat), first, second)
    taps = (3, 3, 3, CH, CH)
    return critic_map.reshape(clip.shape), clip_grad.reshape(clip.shape), first.reshape(taps), second.reshape(taps)


def solution(mesh):
    placed = (P("frame", "row", None, None), P(), P(), P("frame", "row", None, None))
    return jax.shard_map(
        on_device,
        mesh=mesh,
        in_specs=placed,
        out_specs=(P("frame", "row", None, None), P("frame", "row", None, None), P(), P()),
        check_vma=False,
    )
```

```python
import functools

import jax
import jax.numpy as jnp
from jax import lax
from jax.experimental import pallas as pl
from jax.experimental.pallas import tpu as pltpu
from jax.sharding import PartitionSpec as P

MESH = pl.DeviceIdType.MESH
BF16, F32 = jnp.bfloat16, jnp.float32
CH = 128

NX, NY, NZ = 4, 4, 8
NXY = NX * NY
BLK = 112
HALF = NXY * BLK
ROWS = 2 * HALF
TILE = 16
ZT = BLK // TILE


class Place:
    def __init__(self):
        f, r = lax.axis_index("frame"), lax.axis_index("row")
        self.x, self.z = f // (2 * NZ), (f // 2) % NZ
        self.y, self.core = (r // 2) * 2 + f % 2, r % 2
        self.p = self.x * NY + self.y

    @staticmethod
    def at(x, y, z, core):
        return ((x * NZ + z) * 2 + y % 2, (y // 2) * 2 + core)


def remote(src, dst, send, recv, device):
    return pltpu.make_async_remote_copy(
        src_ref=src, dst_ref=dst, send_sem=send, recv_sem=recv, device_id=device, device_id_type=MESH)


def take(ref, rows, sem):
    view = ref.at[pl.ds(0, rows)]
    pltpu.make_async_copy(view, view, sem).wait()


def rows_of(start, size):
    return pl.ds(pl.multiple_of(start, TILE), size)


class AllReduce:
    A, B = (256, 64), (192, 48)
    START_B = NX * 256

    def __init__(self, me, part, full, other, slots, near, piece, tiles, send, recv):
        self.me, self.part, self.full = me, part, full
        self.other, self.slots, self.near, self.piece, self.tiles = other, slots, near, piece, tiles
        self.send, self.recv = send, recv
        self.base = me.core * HALF

    def x_peer(self, o):
        x = (self.me.x + o) % NX
        return x, Place.at(x, self.me.y, self.me.z, self.me.core)

    def y_peer(self, o):
        y = (self.me.y + o) % NY
        return y, Place.at(self.me.x, y, self.me.z, self.me.core)

    def z_peer(self, o):
        d = (self.me.z + o) % NZ
        return d, Place.at(self.me.x, self.me.y, d, self.me.core)

    def twin(self):
        return Place.at(self.me.x, self.me.y, self.me.z, 1 - self.me.core)

    def row_a(self, x, y):
        return self.base + x * self.A[0] + y * self.A[1]

    def row_b(self, x, y):
        return self.base + self.START_B + y * self.B[0] + x * self.B[1]

    def push(self, stage, source, start, target, to, size, peer):
        remote(source.at[rows_of(start, size)], target.at[rows_of(to, size)], self.send.at[stage], self.recv.at[stage], peer).start()

    def scatter_core(self):
        self.push(0, self.part, (1 - self.me.core) * HALF, self.other, 0, HALF, self.twin())

    def scatter_far(self):
        me = self.me
        take(self.other, HALF, self.recv.at[0])

        @pl.loop(0, HALF // 128)
        def _(i):
            mine = rows_of(self.base + i * 128, 128)
            total = self.part[mine, :].astype(F32) + self.other[rows_of(i * 128, 128), :].astype(F32)
            self.part[mine, :] = total.astype(BF16)

        @pl.loop(1, NX)
        def _(o):
            x, peer = self.x_peer(o)
            self.push(1, self.part, self.row_a(x, 0), self.slots, me.x * self.A[0], self.A[0], peer)
            y, peer = self.y_peer(o)
            self.push(1, self.part, self.row_b(0, y), self.slots, self.START_B + me.y * self.B[0], self.B[0], peer)

    def scatter_near(self):
        me = self.me
        take(self.slots, 3 * (self.A[0] + self.B[0]), self.recv.at[1])

        @pl.loop(0, 4)
        def _(i):
            for start, slot, mine, pitch, size in (
                (self.row_a(me.x, 0), 0, me.x, self.A[0], self.A[1]),
                (self.row_b(0, me.y), self.START_B, me.y, self.B[0], self.B[1])):
                rows = rows_of(start + i * size, size)
                total = self.part[rows, :].astype(F32)
                for o in range(1, 4):
                    total = total + self.slots[rows_of(slot + ((mine + o) % 4) * pitch + i * size, size), :].astype(F32)
                self.part[rows, :] = total.astype(BF16)

        @pl.loop(1, NX)
        def _(o):
            y, peer = self.y_peer(o)
            self.push(2, self.part, self.row_a(me.x, y), self.near, me.y * self.A[1], self.A[1], peer)
            x, peer = self.x_peer(o)
            self.push(2, self.part, self.row_b(x, me.y), self.near, NY * self.A[1] + me.x * self.B[1], self.B[1], peer)

    def scatter_z(self):
        me = self.me
        take(self.near, 3 * (self.A[1] + self.B[1]), self.recv.at[2])
        for start, slot, mine, size, to in (
            (self.row_a(me.x, me.y), 0, me.y, self.A[1], 0),
            (self.row_b(me.x, me.y), NY * self.A[1], me.x, self.B[1], self.A[1])):
            total = self.part[rows_of(start, size), :].astype(F32)
            for o in range(1, 4):
                total = total + self.near[rows_of(slot + ((mine + o) % 4) * size, size), :].astype(F32)
            self.piece[to : to + size, :] = total.astype(BF16)

        @pl.loop(1, NZ)
        def _(o):
            d, peer = self.z_peer(o)

            @pl.when(d < ZT)
            def _():
                self.push(3, self.piece, d * TILE, self.tiles, me.z * TILE, TILE, peer)

    def gather_z(self):
        me = self.me

        @pl.when(me.z < ZT)
        def _():
            take(self.tiles, (NZ - 1) * TILE, self.recv.at[3])
            total = self.piece[rows_of(me.z * TILE, TILE), :].astype(F32)
            for o in range(1, NZ):
                d = (me.z + o) % NZ
                total = total + self.tiles[rows_of(d * TILE, TILE), :].astype(F32)
            in_a = self.A[1] // TILE
            row = jnp.where(me.z < in_a, self.row_a(me.x, me.y) + me.z * TILE, self.row_b(me.x, me.y) + (me.z - in_a) * TILE)
            self.full[rows_of(row, TILE), :] = total.astype(BF16)

            @pl.loop(1, NZ)
            def _(o):
                d, peer = self.z_peer(o)
                self.push(4, self.full, row, self.full, row, TILE, peer)

    def gather_near(self):
        me = self.me

        @pl.when(me.z < ZT)
        def _():
            take(self.full, (ZT - 1) * TILE, self.recv.at[4])

        @pl.when(me.z >= ZT)
        def _():
            take(self.full, ZT * TILE, self.recv.at[4])

        a, b = self.row_a(me.x, me.y), self.row_b(me.x, me.y)

        @pl.loop(1, NX)
        def _(o):
            self.push(5, self.full, a, self.full, a, self.A[1], self.y_peer(o)[1])
            self.push(5, self.full, b, self.full, b, self.B[1], self.x_peer(o)[1])

    def gather_far(self):
        me = self.me
        take(self.full, 3 * (self.A[1] + self.B[1]), self.recv.at[5])
        a, b = self.row_a(me.x, 0), self.row_b(0, me.y)

        @pl.loop(1, NX)
        def _(o):
            self.push(6, self.full, a, self.full, a, self.A[0], self.x_peer(o)[1])
            self.push(6, self.full, b, self.full, b, self.B[0], self.y_peer(o)[1])

    def gather_core(self):
        take(self.full, 3 * (self.A[0] + self.B[0]), self.recv.at[6])
        self.push(7, self.full, self.base, self.full, self.base, HALF, self.twin())

    def finish(self):
        me = self.me
        take(self.full, HALF, self.recv.at[7])
        take(self.part, HALF, self.send.at[0])
        take(self.part, 3 * (self.A[0] + self.B[0]), self.send.at[1])
        take(self.part, 3 * (self.A[1] + self.B[1]), self.send.at[2])

        @pl.when(me.z < ZT)
        def _():
            take(self.piece, (ZT - 1) * TILE, self.send.at[3])
            take(self.full, (NZ - 1) * TILE, self.send.at[4])

        @pl.when(me.z >= ZT)
        def _():
            take(self.piece, ZT * TILE, self.send.at[3])

        take(self.full, 3 * (self.A[1] + self.B[1]), self.send.at[5])
        take(self.full, 3 * (self.A[0] + self.B[0]), self.send.at[6])
        take(self.full, HALF, self.send.at[7])


def greet_reduce_peers(me, barrier):
    pl.semaphore_signal(barrier, inc=1, device_id=Place.at(me.x, me.y, me.z, 1 - me.core), device_id_type=MESH)

    @pl.loop(1, NXY)
    def _(o):
        p = (me.p + o) % NXY
        pl.semaphore_signal(barrier, inc=1, device_id=Place.at(p // NY, p % NY, me.z, me.core), device_id_type=MESH)

    @pl.loop(1, NZ)
    def _(o):
        d = (me.z + o) % NZ
        pl.semaphore_signal(barrier, inc=1, device_id=Place.at(me.x, me.y, d, me.core), device_id_type=MESH)

    return 1 + NXY - 1 + NZ - 1

GROUP, FR, COLS, ROWN = 8, 4, 32, 16
POS = COLS * ROWN
NG = NX * NZ


class Ring:
    def __init__(self):
        f, r = lax.axis_index("frame"), lax.axis_index("row")
        self.g, self.y_lo, self.r = f // 2, f % 2, r
        self.s = (r // 2) * 4 + self.y_lo * 2 + r % 2

    @staticmethod
    def parts(s):
        return (s // 2) % 2, (s // 4) * 2 + s % 2

    @staticmethod
    def at(g, s):
        y_lo, r = Ring.parts(s)
        return (g * 2 + y_lo, r)


class Field:
    def __init__(self, ref, ring, own, halo, step, whole, send, recv):
        self.ref, self.ring, self.own, self.halo, self.step, self.whole = ref, ring, own, halo, step, whole
        self.send, self.recv = send, recv
        self.width = COLS + 2 * halo

    def clear(self):
        far = 0 if self.own else FR
        self.ref[far : far + 2] = jnp.zeros((2, self.width, ROWN, CH), BF16)
        for col in (0, COLS + self.halo):
            self.ref[self.own : self.own + FR, col : col + self.halo] = jnp.zeros((FR, self.halo, ROWN, CH), BF16)

    def put(self, f, start, value):
        width = value.shape[0] // ROWN
        self.ref[self.own + f, self.halo + start : self.halo + start + width] = value.astype(BF16).reshape(width, ROWN, CH)

    def to_left(self):
        return self.ring.s > 0

    def to_right(self):
        return self.ring.s < GROUP - 1

    def has_target(self):
        return self.ring.g < NG - 1 if self.step > 0 else self.ring.g > 0

    def has_source(self):
        return self.ring.g > 0 if self.step > 0 else self.ring.g < NG - 1

    def copy(self, frames, col, to_frames, to_col, width, g, s, i):
        return remote(self.ref.at[frames, pl.ds(col, width)], self.ref.at[to_frames, pl.ds(to_col, width)],
                      self.send.at[i], self.recv.at[i], Ring.at(g, s))

    def edge(self, frames, to_frames, side, g, i):
        halo, s = self.halo, self.ring.s
        source, target = (halo, COLS + halo) if side < 0 else (COLS, 0)
        self.copy(frames, source, to_frames, target, halo, g, s + side, i).start()

    def edges(self, q):
        frames, i = self._pair(q)

        @pl.when(self._held(q) & self.to_left())
        def _():
            self.edge(frames, frames, -1, self.ring.g, i)

        @pl.when(self._held(q) & self.to_right())
        def _():
            self.edge(frames, frames, 1, self.ring.g, i + 1)

    def _pair(self, q):
        return pl.ds(self.own + 2 * q, 2), (2 * q) % 6

    def _held(self, q):
        return self.has_source() if q < 0 else self.ring.g >= 0

    def await_edges(self, q):
        self._edges(q, self.recv, self.to_right(), self.to_left())

    def _edges(self, q, sem, left, right):
        frames, i = self._pair(q)
        view = self.ref.at[frames, pl.ds(0, self.halo)]

        @pl.when(self._held(q) & left)
        def _():
            pltpu.make_async_copy(view, view, sem.at[i]).wait()

        @pl.when(self._held(q) & right)
        def _():
            pltpu.make_async_copy(view, view, sem.at[i + 1]).wait()

    def span(self):
        return (0, self.width) if self.whole else (self.halo, COLS)

    def frames(self):
        g, s = self.ring.g + self.step, self.ring.s
        mine, theirs = (pl.ds(FR, 2), pl.ds(0, 2)) if self.step > 0 else (pl.ds(0, 2), pl.ds(FR, 2))
        start, width = self.span()

        @pl.when(self.has_target())
        def _():
            self.copy(mine, start, theirs, start, width, g, s, 4).start()

        if self.whole:
            return

        @pl.when(self.has_target() & self.to_left())
        def _():
            self.edge(mine, theirs, -1, g, 5)

        @pl.when(self.has_target() & self.to_right())
        def _():
            self.edge(mine, theirs, 1, g, 6)

    def _frames(self, sem, there, left, right):
        start, width = self.span()
        body, col = self.ref.at[pl.ds(0, 2), pl.ds(start, width)], self.ref.at[pl.ds(0, 2), pl.ds(0, self.halo)]

        @pl.when(there)
        def _():
            pltpu.make_async_copy(body, body, sem.at[4]).wait()

        if self.whole:
            return

        @pl.when(there & left)
        def _():
            pltpu.make_async_copy(col, col, sem.at[5]).wait()

        @pl.when(there & right)
        def _():
            pltpu.make_async_copy(col, col, sem.at[6]).wait()

    def await_frames(self):
        self._frames(self.recv, self.has_source(), self.to_right(), self.to_left())

    def finish(self):
        if not self.whole:
            for q in range(-1 if self.step > 0 else 0, 2):
                self._edges(q, self.send, self.to_left(), self.to_right())
        if self.whole or self.step < 0:
            self._frames(self.send, self.has_target(), self.to_left(), self.to_right())

    def slab(self, p, k, start, width):
        return self.ref[2 * p + k, start : start + width].reshape(width * ROWN, CH)


def build_weights(kernel, ahead, back, sem):
    zero = jnp.zeros((CH, CH), BF16)
    for k, j in ((0, 1), (3, 0)):
        @pl.loop(0, 9)
        def _(bc):
            b, c = bc // 3, bc % 3
            ahead[pl.ds(pl.multiple_of((c * 4 + k) * CH, CH), CH), pl.ds(pl.multiple_of((b * 2 + j) * CH, CH), CH)] = zero
            back[pl.ds(pl.multiple_of((b * 2 + j) * CH, CH), CH), pl.ds(pl.multiple_of((c * 4 + k) * CH, CH), CH)] = zero

    @pl.loop(0, 27)
    def _(tap):
        a, b, c = tap // 9, (tap // 3) % 3, tap % 3
        for j in range(2):
            k = a + j
            pltpu.make_async_copy(
                kernel.at[tap],
                ahead.at[pl.ds(pl.multiple_of((c * 4 + k) * CH, CH), CH), pl.ds(pl.multiple_of((b * 2 + j) * CH, CH), CH)],
                sem.at[0]).start()
            k = j + 2 - a
            pltpu.make_async_copy(
                kernel.at[tap],
                back.at[pl.ds(pl.multiple_of(((2 - b) * 2 + j) * CH, CH), CH), pl.ds(pl.multiple_of(((2 - c) * 4 + k) * CH, CH), CH)],
                sem.at[1]).start()


def await_weights(ahead, back, sem):
    view = ahead.at[pl.ds(0, 54 * CH * CH // ahead.shape[1])]
    pltpu.make_async_copy(view, view, sem.at[0]).wait()
    view = back.at[pl.ds(0, 54 * CH * CH // back.shape[1])]
    pltpu.make_async_copy(view, view, sem.at[1]).wait()


def row_index(shape):
    return lax.broadcasted_iota(jnp.int32, shape, 0) % ROWN


def from_above(value):
    return jnp.where(row_index(value.shape) == 0, 0.0, pltpu.roll(value, 1, axis=0))


def from_below(value):
    return jnp.where(row_index(value.shape) == ROWN - 1, 0.0, pltpu.roll(value, value.shape[0] - 1, axis=0))


def convolve(field, weights, p, contract, start, width):
    lhs = jnp.concatenate([field.slab(p, k, start + c, width) for c in range(3) for k in range(4)], axis=1)
    rows = lax.dot_general(lhs, weights[...], (((1,), (contract,)), ((), ())), preferred_element_type=F32)
    above, level, below = (rows[:, b * 2 * CH : (b + 1) * 2 * CH] for b in range(3))
    return level + from_above(above) + from_below(below)


def store_turned(turned, delta, start):
    for b, value in enumerate((from_below(delta), delta, from_above(delta))):
        turned[b * 2 * CH : (b + 1) * 2 * CH, start : start + delta.shape[0]] = value.astype(BF16).T


def pair_sums(field, turned, p, c):
    rhs = jnp.concatenate([field.slab(p, k, field.halo - 1 + c, COLS) for k in range(4)], axis=1)
    return lax.dot_general(turned[:, p * POS : (p + 1) * POS], rhs, (((1,), (0,)), ((), ())), preferred_element_type=F32)


def begin_grads(field, turned, begun, p):
    for c in range(3):
        begun[c] = pair_sums(field, turned, p, c)


def weight_grads(field, turned, part, scale, begun=None):
    for c in range(3):
        if begun is None:
            rhs = jnp.concatenate(
                [jnp.concatenate([field.slab(p, k, field.halo - 1 + c, COLS) for k in range(4)], axis=1) for p in range(2)], axis=0)
            sums = lax.dot_general(turned[...], rhs, (((1,), (0,)), ((), ())), preferred_element_type=F32)
        else:
            sums = begun[c] + pair_sums(field, turned, 1, c)
        for b in range(3):
            for a in range(3):
                one = sums[2 * b * CH : (2 * b + 1) * CH, a * CH : (a + 1) * CH]
                two = sums[(2 * b + 1) * CH : (2 * b + 2) * CH, (a + 1) * CH : (a + 2) * CH]
                tap = (a * 3 + b) * 3 + c
                part[tap * CH : (tap + 1) * CH, :] = ((one + two) * scale).T.astype(BF16)


def swap(value):
    return jnp.swapaxes(value, 0, 1)


def spread(ring, source, stage, send, recv, own):
    chip, core = ring.s // 2, ring.s % 2
    for turn, flip in ((0, 1), (1, 0), (3, 0), (1, 1), (3, 1), (2, 0), (2, 1)):
        d = (chip + turn) % 4 * 2 + (core + flip) % 2
        cols = pl.ds(pl.multiple_of(d * COLS, COLS), COLS)
        remote(source.at[:, :, cols], stage.at[pl.ds(2 * ring.y_lo, 2), pl.ds(4 * ring.r, 4)], send, recv, Ring.at(ring.g, d)).start()

    cols = pl.ds(pl.multiple_of(ring.s * COLS, COLS), COLS)
    pltpu.make_async_copy(source.at[:, :, cols], stage.at[pl.ds(2 * ring.y_lo, 2), pl.ds(4 * ring.r, 4)], own).start()


def relay(ring, stage, flat, recv, own, ahead, there, send, landed):
    for turn in (0, 3, 1, 2):
        for core in range(2):
            s = (ring.s + 2 * turn) % GROUP // 2 * 2 + core
            half, quarter = Ring.parts(s)

            @pl.when(s == ring.s)
            def _():
                take(flat, 2 * 4 * COLS, own)

            @pl.when(s != ring.s)
            def _():
                take(flat, 2 * 4 * COLS, recv.at[s])

            @pl.when(there & (half == 1))
            def _():
                rows = pl.ds(4 * quarter, 4)
                remote(stage.at[pl.ds(2, 2), rows], ahead.at[:, rows], send, landed, Ring.at(ring.g + 1, ring.s)).start()


def give_back(ring, stage, result, send, recv, own, half):
    cols = pl.ds(pl.multiple_of(ring.s * COLS, COLS), COLS)
    pair = pl.ds(2 * half, 2)

    @pl.loop(0, 4)
    def _(i):
        quarter = (ring.r + i) % 4
        rows = pl.ds(4 * quarter, 4)
        here = (half == ring.y_lo) & (i == 0)

        @pl.when(here)
        def _():
            pltpu.make_async_copy(stage.at[pair, rows], result.at[:, :, cols], own).start()

        @pl.when(jnp.logical_not(here))
        def _():
            remote(stage.at[pair, rows], result.at[:, :, cols], send, recv, (ring.g * 2 + half, quarter)).start()


def await_blocks(flat, sem, own):
    take(flat, (GROUP - 1) * 2 * 4 * COLS, sem)
    take(flat, 2 * 4 * COLS, own)


def kernel(scale, clip_in, cotangent_in, first_kernel, second_kernel, critic_map, clip_grad, full_first, full_second,
           clip_a, act_a, second_a, first_a, first_w, first_wt, second_w, second_wt, clip, cotangent, stage, cot_f, slopes,
           turned, begun, part, other, slots, near, piece, tiles,
           red_send, red_recv, halo_send, halo_recv, block_send, block_recv, block_own, weight_sem, load_sem,
           ahead, clip_recv, ahead_sem):
    loads = [pltpu.make_async_copy(source, target, load_sem.at[i])
             for i, (source, target) in enumerate(((clip_in, clip), (cotangent_in, cotangent)))]
    for load in loads:
        load.start()
    me, ring = Place(), Ring()
    clips = Field(clip_a, ring, 2, 2, 1, False, halo_send.at[0], halo_recv.at[0])
    acts = Field(act_a, ring, 2, 1, 1, True, halo_send.at[1], halo_recv.at[1])
    seconds = Field(second_a, ring, 0, 1, -1, False, halo_send.at[2], halo_recv.at[2])
    firsts = Field(first_a, ring, 0, 1, -1, False, halo_send.at[3], halo_recv.at[3])
    fields = (clips, acts, seconds, firsts)
    first_sum, second_sum = (
        AllReduce(me, part.at[i], full, other.at[i], slots.at[i], near.at[i], piece.at[i], tiles.at[i],
                  red_send.at[i], red_recv.at[i])
        for i, full in enumerate((full_first, full_second)))

    for field in fields:
        field.clear()

    barrier = pltpu.get_barrier_semaphore()
    count = greet_reduce_peers(me, barrier)

    @pl.loop(1, GROUP)
    def _(o):
        pl.semaphore_signal(barrier, inc=1, device_id=Ring.at(ring.g, (ring.s + o) % GROUP), device_id_type=MESH)

    count = count + GROUP - 1
    for step in (-1, 1):
        for side in (-1, 0, 1):
            g, s = ring.g + step, ring.s + side
            there = (g >= 0) & (g < NG) & (s >= 0) & (s < GROUP)

            @pl.when(there)
            def _():
                pl.semaphore_signal(barrier, inc=1, device_id=Ring.at(g, s), device_id_type=MESH)

            count = count + jnp.where(there, 1, 0)
    build_weights(first_kernel, first_w, first_wt, weight_sem.at[0])
    for i in range(2):
        part[i, 27 * CH :, :] = jnp.zeros((CH, CH), BF16)
    loads[0].wait()
    pl.semaphore_wait(barrier, count)

    spread(ring, clip, stage.at[0], block_send.at[0], clip_recv.at[ring.s], block_own.at[0])
    build_weights(second_kernel, second_w, second_wt, weight_sem.at[1])

    relay(ring, stage.at[0], full_first, clip_recv, block_own.at[0], ahead, clips.has_target(), ahead_sem.at[0], ahead_sem.at[1])
    for f in range(FR):
        clip_a[2 + f, 2 : COLS + 2] = swap(stage[0, f])
    clips.edges(0)
    clips.edges(1)
    loads[1].wait()
    spread(ring, cotangent, stage.at[1], block_send.at[1], block_recv.at[1], block_own.at[1])
    await_weights(first_w, first_wt, weight_sem.at[0])
    await_weights(second_w, second_wt, weight_sem.at[1])
    clips.await_edges(0)
    clips.await_edges(1)

    def sigmoid_slope(z):
        sigma = jax.nn.sigmoid(z)
        return sigma, sigma * (1.0 + z * (1.0 - sigma))

    def first_layer(p):
        width = COLS // 2 + 1
        for half in range(2):
            start = half * width
            pre = convolve(clips, first_w, p, 0, start, width)
            sigma, slope = sigmoid_slope(pre)
            act = (pre * sigma).astype(BF16)
            for j in range(2):
                act_a[2 + 2 * p + j, start : start + width] = act[:, j * CH : (j + 1) * CH].reshape(width, ROWN, CH)
            skip = ROWN if half == 0 else 0
            slopes[p, half * POS // 2 : (half + 1) * POS // 2] = slope[skip : skip + POS // 2]
        pair, edge = pl.ds(2 + 2 * p, 2), jnp.zeros((2, ROWN, CH), BF16)

        @pl.when(ring.s == 0)
        def _():
            act_a[pair, 0] = edge

        @pl.when(ring.s == GROUP - 1)
        def _():
            act_a[pair, COLS + 1] = edge

    width = COLS // 2

    def second_layer(p):
        for start in (0, width):
            pre = convolve(acts, second_w, p, 0, start, width)
            sigma, slope = sigmoid_slope(pre)
            critic = pre * sigma
            delta = slope * jnp.concatenate(
                [cot_f[2 * p + j, start : start + width].reshape(width * ROWN, CH).astype(F32) for j in range(2)], axis=1)
            for j in range(2):
                half = slice(j * CH, (j + 1) * CH)
                stage[2, 2 * p + j, :, start : start + width] = swap(critic[:, half].astype(BF16).reshape(width, ROWN, CH))
                seconds.put(2 * p + j, start, delta[:, half])
            store_turned(turned, delta, p * POS + start * ROWN)

    def back_layer(p):
        for start in (0, width):
            rows = slice(start * ROWN, (start + width) * ROWN)
            delta = convolve(seconds, second_wt, p, 1, start, width) * slopes[p, rows]
            for j in range(2):
                firsts.put(2 * p + j, start, delta[:, j * CH : (j + 1) * CH])
            store_turned(turned, delta, p * POS + start * ROWN)

    def input_layer(p):
        for start in (0, width):
            back = convolve(firsts, first_wt, p, 1, start, width)
            for j in range(2):
                stage[0, 2 * p + j, :, start : start + width] = swap(
                    back[:, j * CH : (j + 1) * CH].astype(BF16).reshape(width, ROWN, CH))

    def give_critic(half):
        give_back(ring, stage.at[2], critic_map, block_send.at[2], block_recv.at[2], block_own.at[2], half)

    def give_grad(half):
        give_back(ring, stage.at[0], clip_grad, block_send.at[3], block_recv.at[3], block_own.at[3], half)

    first_layer(1)
    acts.frames()

    @pl.when(clips.has_source())
    def _():
        take(full_first, 4 * 2 * 4 * COLS, ahead_sem.at[1])
        for f in range(2):
            clip_a[f, 2 : COLS + 2] = swap(ahead[f])

    clips.edges(-1)
    clips.await_edges(-1)
    first_layer(0)
    await_blocks(full_first, block_recv.at[1], block_own.at[1])
    for f in range(FR):
        cot_f[f] = swap(stage[1, f])
    second_layer(1)
    seconds.edges(1)
    give_critic(1)
    acts.await_frames()
    second_layer(0)
    seconds.frames()
    seconds.edges(0)
    weight_grads(acts, turned, part.at[1], scale)
    second_sum.scatter_core()
    seconds.await_edges(0)
    seconds.await_edges(1)
    give_critic(0)
    back_layer(0)
    second_sum.scatter_far()
    firsts.edges(0)

    @pl.when(me.z != 0)
    def _():
        firsts.frames()

    begin_grads(clips, turned, begun, 0)
    seconds.await_frames()

    @pl.when(me.z == 0)
    def _():
        firsts.frames()

    back_layer(1)
    firsts.edges(1)
    weight_grads(clips, turned, part.at[0], scale, begun)
    first_sum.scatter_core()
    second_sum.scatter_near()
    firsts.await_edges(0)
    firsts.await_edges(1)
    first_sum.scatter_far()
    take(full_first, (GROUP - 1) * 2 * 4 * COLS, block_send.at[0])

    @pl.when(clips.has_target())
    def _():
        take(full_first, 4 * 2 * 4 * COLS, ahead_sem.at[0])

    input_layer(0)
    second_sum.scatter_z()
    first_sum.scatter_near()

    firsts.await_frames()
    input_layer(1)
    give_grad(0)
    give_grad(1)
    second_sum.gather_z()
    first_sum.scatter_z()

    second_sum.gather_near()

    first_sum.gather_z()
    second_sum.gather_far()
    first_sum.gather_near()
    first_sum.gather_far()
    second_sum.gather_core()
    second_sum.finish()
    for field in fields:
        field.finish()
    for i in range(1, 4):
        take(full_first, (GROUP - 1) * 2 * 4 * COLS, block_send.at[i])
    for i in range(2, 4):
        await_blocks(full_first, block_recv.at[i], block_own.at[i])
    first_sum.gather_core()
    first_sum.finish()


def write_out(critic_in, grad_in, first_in, second_in, critic, grad, first, second, wide, sem):
    half = 27 * CH // 2
    stores = []
    for n, (source, target) in enumerate(((first_in, first), (second_in, second))):
        for h in range(2):
            i = 2 * n + h

            @pl.loop(0, half // 192)
            def _(k):
                wide[i, rows_of(k * 192, 192), :] = source[rows_of(h * half + k * 192, 192), :].astype(F32)

            stores.append(pltpu.make_async_copy(wide.at[i], target.at[pl.ds(h * half, half)], sem.at[i]))
            stores[-1].start()
    for n, (source, target) in enumerate(((critic_in, critic), (grad_in, grad))):
        stores.append(pltpu.make_async_copy(source, target, sem.at[4 + n]))
        stores[-1].start()
    for one in stores:
        one.wait()


def on_device(clip, first_kernel, second_kernel, cotangent):
    cells = clip.shape[0] * lax.axis_size("frame") * clip.shape[1] * lax.axis_size("row") * clip.shape[2]
    scale = 1.0 / float(cells) ** 0.5
    vmem, anywhere = pl.BlockSpec(memory_space=pltpu.VMEM), pl.BlockSpec(memory_space=pl.ANY)
    total = jax.ShapeDtypeStruct((ROWS, CH), BF16)
    dma = pltpu.SemaphoreType.DMA
    flat = (2 * 4 * GROUP * COLS, CH)

    def field(halo):
        return pltpu.VMEM((FR + 2, COLS + 2 * halo, ROWN, CH), BF16)

    results = pl.pallas_call(
        functools.partial(kernel, scale),
        out_shape=(jax.ShapeDtypeStruct(clip.shape, BF16), jax.ShapeDtypeStruct(clip.shape, BF16), total, total),
        in_specs=[pl.BlockSpec(memory_space=pltpu.HBM)] * 4,
        out_specs=(vmem, vmem, vmem, vmem),
        scratch_shapes=[
            field(2), field(1), field(1), field(1),
            pltpu.VMEM((12 * CH, 6 * CH), BF16), pltpu.VMEM((6 * CH, 12 * CH), BF16),
            pltpu.VMEM((12 * CH, 6 * CH), BF16), pltpu.VMEM((6 * CH, 12 * CH), BF16),
            pltpu.VMEM(clip.shape, BF16), pltpu.VMEM(clip.shape, BF16),
            pltpu.VMEM((3, FR, ROWN, COLS, CH), BF16),
            pltpu.VMEM((FR, COLS, ROWN, CH), BF16),
            pltpu.VMEM((2, POS, 2 * CH), F32),
            pltpu.VMEM((6 * CH, 2 * POS), BF16),
            pltpu.VMEM((3, 6 * CH, 4 * CH), F32),
            pltpu.VMEM((2, ROWS, CH), BF16),
            pltpu.VMEM((2, HALF, CH), BF16),
            pltpu.VMEM((2, HALF, CH), BF16),
            pltpu.VMEM((2, HALF // 4, CH), BF16),
            pltpu.VMEM((2, BLK, CH), BF16),
            pltpu.VMEM((2, NZ * TILE, CH), BF16),
            dma((2, 8)), dma((2, 8)), dma((4, 7)), dma((4, 7)), dma((4,)), dma((4,)), dma((4,)), dma((2, 2)), dma((2,)),
            pltpu.VMEM((2, ROWN, COLS, CH), BF16), dma((GROUP,)), dma((2,)),
        ],
        compiler_params=pltpu.CompilerParams(collective_id=0, has_side_effects=True, vmem_limit_bytes=38 << 20),
    )(*(pltpu.with_memory_space_constraint(one, pltpu.HBM) for one in (
        clip, cotangent, first_kernel.reshape(27, CH, CH), second_kernel.reshape(27, CH, CH))))
    critic_map, clip_grad, first, second = results

    whole = jax.ShapeDtypeStruct((27 * CH, CH), F32)
    critic_map, clip_grad, first, second = pl.pallas_call(
        write_out,
        out_shape=(jax.ShapeDtypeStruct(flat, BF16), jax.ShapeDtypeStruct(flat, BF16), whole, whole),
        in_specs=[vmem] * 4,
        out_specs=(anywhere,) * 4,
        scratch_shapes=[pltpu.VMEM((4, 27 * CH // 2, CH), F32), dma((6,))],
        compiler_params=pltpu.CompilerParams(vmem_limit_bytes=10 << 20),
    )(critic_map.reshape(flat), clip_grad.reshape(flat), first, second)
    taps = (3, 3, 3, CH, CH)
    return critic_map.reshape(clip.shape), clip_grad.reshape(clip.shape), first.reshape(taps), second.reshape(taps)


def solution(mesh):
    placed = (P("frame", "row", None, None), P(), P(), P("frame", "row", None, None))
    return jax.shard_map(
        on_device,
        mesh=mesh,
        in_specs=placed,
        out_specs=(P("frame", "row", None, None), P("frame", "row", None, None), P(), P()),
        check_vma=False,
    )
```

```python
import functools

import jax
import jax.numpy as jnp
from jax import lax
from jax.experimental import pallas as pl
from jax.experimental.pallas import tpu as pltpu
from jax.sharding import PartitionSpec as P

MESH = pl.DeviceIdType.MESH
BF16, F32 = jnp.bfloat16, jnp.float32
CH = 128

NX, NY, NZ = 4, 4, 8
NXY = NX * NY
BLK = 112
HALF = NXY * BLK
ROWS = 2 * HALF
TILE = 16
ZT = BLK // TILE


class Place:
    def __init__(self):
        f, r = lax.axis_index("frame"), lax.axis_index("row")
        self.x, self.z = f // (2 * NZ), (f // 2) % NZ
        self.y, self.core = (r // 2) * 2 + f % 2, r % 2
        self.p = self.x * NY + self.y

    @staticmethod
    def at(x, y, z, core):
        return ((x * NZ + z) * 2 + y % 2, (y // 2) * 2 + core)


def remote(src, dst, send, recv, device):
    return pltpu.make_async_remote_copy(
        src_ref=src, dst_ref=dst, send_sem=send, recv_sem=recv, device_id=device, device_id_type=MESH)


def take(ref, rows, sem):
    view = ref.at[pl.ds(0, rows)]
    pltpu.make_async_copy(view, view, sem).wait()


def rows_of(start, size):
    return pl.ds(pl.multiple_of(start, TILE), size)


class AllReduce:
    A, B = (256, 64), (192, 48)
    START_B = NX * 256

    def __init__(self, me, part, full, other, slots, near, piece, tiles, send, recv):
        self.me, self.part, self.full = me, part, full
        self.other, self.slots, self.near, self.piece, self.tiles = other, slots, near, piece, tiles
        self.send, self.recv = send, recv
        self.base = me.core * HALF

    def x_peer(self, o):
        x = (self.me.x + o) % NX
        return x, Place.at(x, self.me.y, self.me.z, self.me.core)

    def y_peer(self, o):
        y = (self.me.y + o) % NY
        return y, Place.at(self.me.x, y, self.me.z, self.me.core)

    def z_peer(self, o):
        d = (self.me.z + o) % NZ
        return d, Place.at(self.me.x, self.me.y, d, self.me.core)

    def twin(self):
        return Place.at(self.me.x, self.me.y, self.me.z, 1 - self.me.core)

    def row_a(self, x, y):
        return self.base + x * self.A[0] + y * self.A[1]

    def row_b(self, x, y):
        return self.base + self.START_B + y * self.B[0] + x * self.B[1]

    def push(self, stage, source, start, target, to, size, peer):
        remote(source.at[rows_of(start, size)], target.at[rows_of(to, size)], self.send.at[stage], self.recv.at[stage], peer).start()

    def scatter_core(self):
        self.push(0, self.part, (1 - self.me.core) * HALF, self.other, 0, HALF, self.twin())

    def scatter_far(self):
        me = self.me
        take(self.other, HALF, self.recv.at[0])

        @pl.loop(0, HALF // 128)
        def _(i):
            mine = rows_of(self.base + i * 128, 128)
            total = self.part[mine, :].astype(F32) + self.other[rows_of(i * 128, 128), :].astype(F32)
            self.part[mine, :] = total.astype(BF16)

        @pl.loop(1, NX)
        def _(o):
            x, peer = self.x_peer(o)
            self.push(1, self.part, self.row_a(x, 0), self.slots, me.x * self.A[0], self.A[0], peer)
            y, peer = self.y_peer(o)
            self.push(1, self.part, self.row_b(0, y), self.slots, self.START_B + me.y * self.B[0], self.B[0], peer)

    def scatter_near(self):
        me = self.me
        take(self.slots, 3 * (self.A[0] + self.B[0]), self.recv.at[1])

        @pl.loop(0, 4)
        def _(i):
            for start, slot, mine, pitch, size in (
                (self.row_a(me.x, 0), 0, me.x, self.A[0], self.A[1]),
                (self.row_b(0, me.y), self.START_B, me.y, self.B[0], self.B[1])):
                rows = rows_of(start + i * size, size)
                total = self.part[rows, :].astype(F32)
                for o in range(1, 4):
                    total = total + self.slots[rows_of(slot + ((mine + o) % 4) * pitch + i * size, size), :].astype(F32)
                self.part[rows, :] = total.astype(BF16)

        @pl.loop(1, NX)
        def _(o):
            y, peer = self.y_peer(o)
            self.push(2, self.part, self.row_a(me.x, y), self.near, me.y * self.A[1], self.A[1], peer)
            x, peer = self.x_peer(o)
            self.push(2, self.part, self.row_b(x, me.y), self.near, NY * self.A[1] + me.x * self.B[1], self.B[1], peer)

    def scatter_z(self):
        me = self.me
        take(self.near, 3 * (self.A[1] + self.B[1]), self.recv.at[2])
        for start, slot, mine, size, to in (
            (self.row_a(me.x, me.y), 0, me.y, self.A[1], 0),
            (self.row_b(me.x, me.y), NY * self.A[1], me.x, self.B[1], self.A[1])):
            total = self.part[rows_of(start, size), :].astype(F32)
            for o in range(1, 4):
                total = total + self.near[rows_of(slot + ((mine + o) % 4) * size, size), :].astype(F32)
            self.piece[to : to + size, :] = total.astype(BF16)

        @pl.loop(1, NZ)
        def _(o):
            d, peer = self.z_peer(o)

            @pl.when(d < ZT)
            def _():
                self.push(3, self.piece, d * TILE, self.tiles, me.z * TILE, TILE, peer)

    def gather_z(self):
        me = self.me

        @pl.when(me.z < ZT)
        def _():
            take(self.tiles, (NZ - 1) * TILE, self.recv.at[3])
            total = self.piece[rows_of(me.z * TILE, TILE), :].astype(F32)
            for o in range(1, NZ):
                d = (me.z + o) % NZ
                total = total + self.tiles[rows_of(d * TILE, TILE), :].astype(F32)
            in_a = self.A[1] // TILE
            row = jnp.where(me.z < in_a, self.row_a(me.x, me.y) + me.z * TILE, self.row_b(me.x, me.y) + (me.z - in_a) * TILE)
            self.full[rows_of(row, TILE), :] = total.astype(BF16)

            @pl.loop(1, NZ)
            def _(o):
                d, peer = self.z_peer(o)
                self.push(4, self.full, row, self.full, row, TILE, peer)

    def gather_near(self):
        me = self.me

        @pl.when(me.z < ZT)
        def _():
            take(self.full, (ZT - 1) * TILE, self.recv.at[4])

        @pl.when(me.z >= ZT)
        def _():
            take(self.full, ZT * TILE, self.recv.at[4])

        a, b = self.row_a(me.x, me.y), self.row_b(me.x, me.y)

        @pl.loop(1, NX)
        def _(o):
            self.push(5, self.full, a, self.full, a, self.A[1], self.y_peer(o)[1])
            self.push(5, self.full, b, self.full, b, self.B[1], self.x_peer(o)[1])

    def gather_far(self):
        me = self.me
        take(self.full, 3 * (self.A[1] + self.B[1]), self.recv.at[5])
        a, b = self.row_a(me.x, 0), self.row_b(0, me.y)

        @pl.loop(1, NX)
        def _(o):
            self.push(6, self.full, a, self.full, a, self.A[0], self.x_peer(o)[1])
            self.push(6, self.full, b, self.full, b, self.B[0], self.y_peer(o)[1])

    def gather_core(self):
        take(self.full, 3 * (self.A[0] + self.B[0]), self.recv.at[6])
        self.push(7, self.full, self.base, self.full, self.base, HALF, self.twin())

    def finish(self):
        me = self.me
        take(self.full, HALF, self.recv.at[7])
        take(self.part, HALF, self.send.at[0])
        take(self.part, 3 * (self.A[0] + self.B[0]), self.send.at[1])
        take(self.part, 3 * (self.A[1] + self.B[1]), self.send.at[2])

        @pl.when(me.z < ZT)
        def _():
            take(self.piece, (ZT - 1) * TILE, self.send.at[3])
            take(self.full, (NZ - 1) * TILE, self.send.at[4])

        @pl.when(me.z >= ZT)
        def _():
            take(self.piece, ZT * TILE, self.send.at[3])

        take(self.full, 3 * (self.A[1] + self.B[1]), self.send.at[5])
        take(self.full, 3 * (self.A[0] + self.B[0]), self.send.at[6])
        take(self.full, HALF, self.send.at[7])


def greet_reduce_peers(me, barrier):
    pl.semaphore_signal(barrier, inc=1, device_id=Place.at(me.x, me.y, me.z, 1 - me.core), device_id_type=MESH)

    @pl.loop(1, NXY)
    def _(o):
        p = (me.p + o) % NXY
        pl.semaphore_signal(barrier, inc=1, device_id=Place.at(p // NY, p % NY, me.z, me.core), device_id_type=MESH)

    @pl.loop(1, NZ)
    def _(o):
        d = (me.z + o) % NZ
        pl.semaphore_signal(barrier, inc=1, device_id=Place.at(me.x, me.y, d, me.core), device_id_type=MESH)

    return 1 + NXY - 1 + NZ - 1

GROUP, FR, COLS, ROWN = 8, 4, 32, 16
POS = COLS * ROWN
NG = NX * NZ


class Ring:
    def __init__(self):
        f, r = lax.axis_index("frame"), lax.axis_index("row")
        self.g, self.y_lo, self.r = f // 2, f % 2, r
        self.s = (r // 2) * 4 + self.y_lo * 2 + r % 2

    @staticmethod
    def parts(s):
        return (s // 2) % 2, (s // 4) * 2 + s % 2

    @staticmethod
    def at(g, s):
        y_lo, r = Ring.parts(s)
        return (g * 2 + y_lo, r)


class Field:
    def __init__(self, ref, ring, own, halo, step, whole, send, recv):
        self.ref, self.ring, self.own, self.halo, self.step, self.whole = ref, ring, own, halo, step, whole
        self.send, self.recv = send, recv
        self.width = COLS + 2 * halo

    def clear(self):
        far = 0 if self.own else FR
        self.ref[far : far + 2] = jnp.zeros((2, self.width, ROWN, CH), BF16)
        for col in (0, COLS + self.halo):
            self.ref[self.own : self.own + FR, col : col + self.halo] = jnp.zeros((FR, self.halo, ROWN, CH), BF16)

    def put(self, f, start, value):
        width = value.shape[0] // ROWN
        self.ref[self.own + f, self.halo + start : self.halo + start + width] = value.astype(BF16).reshape(width, ROWN, CH)

    def to_left(self):
        return self.ring.s > 0

    def to_right(self):
        return self.ring.s < GROUP - 1

    def has_target(self):
        return self.ring.g < NG - 1 if self.step > 0 else self.ring.g > 0

    def has_source(self):
        return self.ring.g > 0 if self.step > 0 else self.ring.g < NG - 1

    def copy(self, frames, col, to_frames, to_col, width, g, s, i):
        return remote(self.ref.at[frames, pl.ds(col, width)], self.ref.at[to_frames, pl.ds(to_col, width)],
                      self.send.at[i], self.recv.at[i], Ring.at(g, s))

    def edge(self, frames, to_frames, side, g, i):
        halo, s = self.halo, self.ring.s
        source, target = (halo, COLS + halo) if side < 0 else (COLS, 0)
        self.copy(frames, source, to_frames, target, halo, g, s + side, i).start()

    def edges(self, q):
        frames, i = self._pair(q)

        @pl.when(self._held(q) & self.to_left())
        def _():
            self.edge(frames, frames, -1, self.ring.g, i)

        @pl.when(self._held(q) & self.to_right())
        def _():
            self.edge(frames, frames, 1, self.ring.g, i + 1)

    def _pair(self, q):
        return pl.ds(self.own + 2 * q, 2), (2 * q) % 6

    def _held(self, q):
        return self.has_source() if q < 0 else self.ring.g >= 0

    def await_edges(self, q):
        self._edges(q, self.recv, self.to_right(), self.to_left())

    def _edges(self, q, sem, left, right):
        frames, i = self._pair(q)
        view = self.ref.at[frames, pl.ds(0, self.halo)]

        @pl.when(self._held(q) & left)
        def _():
            pltpu.make_async_copy(view, view, sem.at[i]).wait()

        @pl.when(self._held(q) & right)
        def _():
            pltpu.make_async_copy(view, view, sem.at[i + 1]).wait()

    def span(self):
        return (0, self.width) if self.whole else (self.halo, COLS)

    def frames(self):
        g, s = self.ring.g + self.step, self.ring.s
        mine, theirs = (pl.ds(FR, 2), pl.ds(0, 2)) if self.step > 0 else (pl.ds(0, 2), pl.ds(FR, 2))
        start, width = self.span()

        @pl.when(self.has_target())
        def _():
            self.copy(mine, start, theirs, start, width, g, s, 4).start()

        if self.whole:
            return

        @pl.when(self.has_target() & self.to_left())
        def _():
            self.edge(mine, theirs, -1, g, 5)

        @pl.when(self.has_target() & self.to_right())
        def _():
            self.edge(mine, theirs, 1, g, 6)

    def _frames(self, sem, there, left, right):
        start, width = self.span()
        body, col = self.ref.at[pl.ds(0, 2), pl.ds(start, width)], self.ref.at[pl.ds(0, 2), pl.ds(0, self.halo)]

        @pl.when(there)
        def _():
            pltpu.make_async_copy(body, body, sem.at[4]).wait()

        if self.whole:
            return

        @pl.when(there & left)
        def _():
            pltpu.make_async_copy(col, col, sem.at[5]).wait()

        @pl.when(there & right)
        def _():
            pltpu.make_async_copy(col, col, sem.at[6]).wait()

    def await_frames(self):
        self._frames(self.recv, self.has_source(), self.to_right(), self.to_left())

    def finish(self):
        if not self.whole:
            for q in range(-1 if self.step > 0 else 0, 2):
                self._edges(q, self.send, self.to_left(), self.to_right())
        if self.whole or self.step < 0:
            self._frames(self.send, self.has_target(), self.to_left(), self.to_right())

    def slab(self, p, k, start, width):
        return self.ref[2 * p + k, start : start + width].reshape(width * ROWN, CH)


def build_weights(kernel, ahead, back, sem):
    zero = jnp.zeros((CH, CH), BF16)
    for k, j in ((0, 1), (3, 0)):
        @pl.loop(0, 9)
        def _(bc):
            b, c = bc // 3, bc % 3
            ahead[pl.ds(pl.multiple_of((c * 4 + k) * CH, CH), CH), pl.ds(pl.multiple_of((b * 2 + j) * CH, CH), CH)] = zero
            back[pl.ds(pl.multiple_of((b * 2 + j) * CH, CH), CH), pl.ds(pl.multiple_of((c * 4 + k) * CH, CH), CH)] = zero

    @pl.loop(0, 27)
    def _(tap):
        a, b, c = tap // 9, (tap // 3) % 3, tap % 3
        for j in range(2):
            k = a + j
            pltpu.make_async_copy(
                kernel.at[tap],
                ahead.at[pl.ds(pl.multiple_of((c * 4 + k) * CH, CH), CH), pl.ds(pl.multiple_of((b * 2 + j) * CH, CH), CH)],
                sem.at[0]).start()
            k = j + 2 - a
            pltpu.make_async_copy(
                kernel.at[tap],
                back.at[pl.ds(pl.multiple_of(((2 - b) * 2 + j) * CH, CH), CH), pl.ds(pl.multiple_of(((2 - c) * 4 + k) * CH, CH), CH)],
                sem.at[1]).start()


def await_weights(ahead, back, sem):
    view = ahead.at[pl.ds(0, 54 * CH * CH // ahead.shape[1])]
    pltpu.make_async_copy(view, view, sem.at[0]).wait()
    view = back.at[pl.ds(0, 54 * CH * CH // back.shape[1])]
    pltpu.make_async_copy(view, view, sem.at[1]).wait()


def row_index(shape):
    return lax.broadcasted_iota(jnp.int32, shape, 0) % ROWN


def from_above(value):
    return jnp.where(row_index(value.shape) == 0, 0.0, pltpu.roll(value, 1, axis=0))


def from_below(value):
    return jnp.where(row_index(value.shape) == ROWN - 1, 0.0, pltpu.roll(value, value.shape[0] - 1, axis=0))


def convolve(field, weights, p, contract, start, width):
    lhs = jnp.concatenate([field.slab(p, k, start + c, width) for c in range(3) for k in range(4)], axis=1)
    rows = lax.dot_general(lhs, weights[...], (((1,), (contract,)), ((), ())), preferred_element_type=F32)
    above, level, below = (rows[:, b * 2 * CH : (b + 1) * 2 * CH] for b in range(3))
    return level + from_above(above) + from_below(below)


def store_turned(turned, delta, start):
    for b, value in enumerate((from_below(delta), delta, from_above(delta))):
        turned[b * 2 * CH : (b + 1) * 2 * CH, start : start + delta.shape[0]] = value.astype(BF16).T


def pair_sums(field, turned, p, c):
    rhs = jnp.concatenate([field.slab(p, k, field.halo - 1 + c, COLS) for k in range(4)], axis=1)
    return lax.dot_general(turned[:, p * POS : (p + 1) * POS], rhs, (((1,), (0,)), ((), ())), preferred_element_type=F32)


def begin_grads(field, turned, begun, p):
    for c in range(3):
        begun[c] = pair_sums(field, turned, p, c)


def weight_grads(field, turned, part, scale, begun=None):
    for c in range(3):
        if begun is None:
            rhs = jnp.concatenate(
                [jnp.concatenate([field.slab(p, k, field.halo - 1 + c, COLS) for k in range(4)], axis=1) for p in range(2)], axis=0)
            sums = lax.dot_general(turned[...], rhs, (((1,), (0,)), ((), ())), preferred_element_type=F32)
        else:
            sums = begun[c] + pair_sums(field, turned, 1, c)
        for b in range(3):
            for a in range(3):
                one = sums[2 * b * CH : (2 * b + 1) * CH, a * CH : (a + 1) * CH]
                two = sums[(2 * b + 1) * CH : (2 * b + 2) * CH, (a + 1) * CH : (a + 2) * CH]
                tap = (a * 3 + b) * 3 + c
                part[tap * CH : (tap + 1) * CH, :] = ((one + two) * scale).T.astype(BF16)


def swap(value):
    return jnp.swapaxes(value, 0, 1)


def spread(ring, source, stage, send, recv, own):
    chip, core = ring.s // 2, ring.s % 2
    for turn, flip in ((0, 1), (1, 0), (3, 0), (1, 1), (3, 1), (2, 0), (2, 1)):
        d = (chip + turn) % 4 * 2 + (core + flip) % 2
        cols = pl.ds(pl.multiple_of(d * COLS, COLS), COLS)
        remote(source.at[:, :, cols], stage.at[pl.ds(2 * ring.y_lo, 2), pl.ds(4 * ring.r, 4)], send, recv, Ring.at(ring.g, d)).start()

    cols = pl.ds(pl.multiple_of(ring.s * COLS, COLS), COLS)
    pltpu.make_async_copy(source.at[:, :, cols], stage.at[pl.ds(2 * ring.y_lo, 2), pl.ds(4 * ring.r, 4)], own).start()


def relay(ring, stage, flat, recv, own, ahead, there, send, landed):
    for turn in (0, 3, 1, 2):
        for core in range(2):
            s = (ring.s + 2 * turn) % GROUP // 2 * 2 + core
            half, quarter = Ring.parts(s)

            @pl.when(s == ring.s)
            def _():
                take(flat, 2 * 4 * COLS, own)

            @pl.when(s != ring.s)
            def _():
                take(flat, 2 * 4 * COLS, recv.at[s])

            @pl.when(there & (half == 1))
            def _():
                rows = pl.ds(4 * quarter, 4)
                remote(stage.at[pl.ds(2, 2), rows], ahead.at[:, rows], send, landed, Ring.at(ring.g + 1, ring.s)).start()


def give_back(ring, stage, result, send, recv, own, half):
    cols = pl.ds(pl.multiple_of(ring.s * COLS, COLS), COLS)
    pair = pl.ds(2 * half, 2)

    @pl.loop(0, 4)
    def _(i):
        quarter = (ring.r + i) % 4
        rows = pl.ds(4 * quarter, 4)
        here = (half == ring.y_lo) & (i == 0)

        @pl.when(here)
        def _():
            pltpu.make_async_copy(stage.at[pair, rows], result.at[:, :, cols], own).start()

        @pl.when(jnp.logical_not(here))
        def _():
            remote(stage.at[pair, rows], result.at[:, :, cols], send, recv, (ring.g * 2 + half, quarter)).start()


def await_blocks(flat, sem, own):
    take(flat, (GROUP - 1) * 2 * 4 * COLS, sem)
    take(flat, 2 * 4 * COLS, own)


def kernel(scale, clip_in, cotangent_in, first_kernel, second_kernel, critic_map, clip_grad, full_first, full_second,
           clip_a, act_a, second_a, first_a, first_w, first_wt, second_w, second_wt, clip, cotangent, stage, cot_f, slopes,
           turned, begun, part, other, slots, near, piece, tiles,
           red_send, red_recv, halo_send, halo_recv, block_send, block_recv, block_own, weight_sem, load_sem,
           ahead, clip_recv, ahead_sem):
    loads = [pltpu.make_async_copy(source, target, load_sem.at[i])
             for i, (source, target) in enumerate(((clip_in, clip), (cotangent_in, cotangent)))]
    for load in loads:
        load.start()
    me, ring = Place(), Ring()
    clips = Field(clip_a, ring, 2, 2, 1, False, halo_send.at[0], halo_recv.at[0])
    acts = Field(act_a, ring, 2, 1, 1, True, halo_send.at[1], halo_recv.at[1])
    seconds = Field(second_a, ring, 0, 1, -1, False, halo_send.at[2], halo_recv.at[2])
    firsts = Field(first_a, ring, 0, 1, -1, False, halo_send.at[3], halo_recv.at[3])
    fields = (clips, acts, seconds, firsts)
    first_sum, second_sum = (
        AllReduce(me, part.at[i], full, other.at[i], slots.at[i], near.at[i], piece.at[i], tiles.at[i],
                  red_send.at[i], red_recv.at[i])
        for i, full in enumerate((full_first, full_second)))

    for field in fields:
        field.clear()

    barrier = pltpu.get_barrier_semaphore()
    count = greet_reduce_peers(me, barrier)

    @pl.loop(1, GROUP)
    def _(o):
        pl.semaphore_signal(barrier, inc=1, device_id=Ring.at(ring.g, (ring.s + o) % GROUP), device_id_type=MESH)

    count = count + GROUP - 1
    for step in (-1, 1):
        for side in (-1, 0, 1):
            g, s = ring.g + step, ring.s + side
            there = (g >= 0) & (g < NG) & (s >= 0) & (s < GROUP)

            @pl.when(there)
            def _():
                pl.semaphore_signal(barrier, inc=1, device_id=Ring.at(g, s), device_id_type=MESH)

            count = count + jnp.where(there, 1, 0)
    build_weights(first_kernel, first_w, first_wt, weight_sem.at[0])
    for i in range(2):
        part[i, 27 * CH :, :] = jnp.zeros((CH, CH), BF16)
    loads[0].wait()
    pl.semaphore_wait(barrier, count)

    spread(ring, clip, stage.at[0], block_send.at[0], clip_recv.at[ring.s], block_own.at[0])
    build_weights(second_kernel, second_w, second_wt, weight_sem.at[1])

    relay(ring, stage.at[0], full_first, clip_recv, block_own.at[0], ahead, clips.has_target(), ahead_sem.at[0], ahead_sem.at[1])
    for f in range(FR):
        clip_a[2 + f, 2 : COLS + 2] = swap(stage[0, f])
    clips.edges(0)
    clips.edges(1)
    loads[1].wait()
    spread(ring, cotangent, stage.at[1], block_send.at[1], block_recv.at[1], block_own.at[1])
    await_weights(first_w, first_wt, weight_sem.at[0])
    await_weights(second_w, second_wt, weight_sem.at[1])
    clips.await_edges(0)
    clips.await_edges(1)

    def sigmoid_slope(z):
        sigma = jax.nn.sigmoid(z)
        return sigma, sigma * (1.0 + z * (1.0 - sigma))

    def first_layer(p):
        width = COLS // 2 + 1
        for half in range(2):
            start = half * width
            pre = convolve(clips, first_w, p, 0, start, width)
            sigma, slope = sigmoid_slope(pre)
            act = (pre * sigma).astype(BF16)
            for j in range(2):
                act_a[2 + 2 * p + j, start : start + width] = act[:, j * CH : (j + 1) * CH].reshape(width, ROWN, CH)
            skip = ROWN if half == 0 else 0
            slopes[p, half * POS // 2 : (half + 1) * POS // 2] = slope[skip : skip + POS // 2]
        pair, edge = pl.ds(2 + 2 * p, 2), jnp.zeros((2, ROWN, CH), BF16)

        @pl.when(ring.s == 0)
        def _():
            act_a[pair, 0] = edge

        @pl.when(ring.s == GROUP - 1)
        def _():
            act_a[pair, COLS + 1] = edge

    width = COLS // 2

    def second_layer(p):
        for start in (0, width):
            pre = convolve(acts, second_w, p, 0, start, width)
            sigma, slope = sigmoid_slope(pre)
            critic = pre * sigma
            delta = slope * jnp.concatenate(
                [cot_f[2 * p + j, start : start + width].reshape(width * ROWN, CH).astype(F32) for j in range(2)], axis=1)
            for j in range(2):
                half = slice(j * CH, (j + 1) * CH)
                stage[2, 2 * p + j, :, start : start + width] = swap(critic[:, half].astype(BF16).reshape(width, ROWN, CH))
                seconds.put(2 * p + j, start, delta[:, half])
            store_turned(turned, delta, p * POS + start * ROWN)

    def back_layer(p):
        for start in (0, width):
            rows = slice(start * ROWN, (start + width) * ROWN)
            delta = convolve(seconds, second_wt, p, 1, start, width) * slopes[p, rows]
            for j in range(2):
                firsts.put(2 * p + j, start, delta[:, j * CH : (j + 1) * CH])
            store_turned(turned, delta, p * POS + start * ROWN)

    def input_layer(p):
        for start in (0, width):
            back = convolve(firsts, first_wt, p, 1, start, width)
            for j in range(2):
                stage[0, 2 * p + j, :, start : start + width] = swap(
                    back[:, j * CH : (j + 1) * CH].astype(BF16).reshape(width, ROWN, CH))

    def give_critic(half):
        give_back(ring, stage.at[2], critic_map, block_send.at[2], block_recv.at[2], block_own.at[2], half)

    def give_grad(half):
        give_back(ring, stage.at[0], clip_grad, block_send.at[3], block_recv.at[3], block_own.at[3], half)

    first_layer(1)
    acts.frames()

    @pl.when(clips.has_source())
    def _():
        take(full_first, 4 * 2 * 4 * COLS, ahead_sem.at[1])
        for f in range(2):
            clip_a[f, 2 : COLS + 2] = swap(ahead[f])

    clips.edges(-1)
    clips.await_edges(-1)
    first_layer(0)
    await_blocks(full_first, block_recv.at[1], block_own.at[1])
    for f in range(FR):
        cot_f[f] = swap(stage[1, f])
    second_layer(1)
    seconds.edges(1)
    give_critic(1)
    acts.await_frames()
    second_layer(0)
    seconds.frames()
    seconds.edges(0)
    weight_grads(acts, turned, part.at[1], scale)
    second_sum.scatter_core()
    seconds.await_edges(0)
    seconds.await_edges(1)
    give_critic(0)
    back_layer(0)
    second_sum.scatter_far()
    firsts.edges(0)

    @pl.when(me.z != 0)
    def _():
        firsts.frames()

    begin_grads(clips, turned, begun, 0)
    seconds.await_frames()
    back_layer(1)
    firsts.edges(1)
    weight_grads(clips, turned, part.at[0], scale, begun)
    first_sum.scatter_core()
    second_sum.scatter_near()
    firsts.await_edges(0)
    firsts.await_edges(1)
    first_sum.scatter_far()
    take(full_first, (GROUP - 1) * 2 * 4 * COLS, block_send.at[0])

    @pl.when(clips.has_target())
    def _():
        take(full_first, 4 * 2 * 4 * COLS, ahead_sem.at[0])

    input_layer(0)
    second_sum.scatter_z()
    first_sum.scatter_near()

    @pl.when(me.z != NZ - 1)
    def _():
        firsts.await_frames()
        input_layer(1)

    give_grad(0)

    @pl.when(me.z != NZ - 1)
    def _():
        give_grad(1)

    second_sum.gather_z()
    first_sum.scatter_z()


    @pl.when(me.z == 0)
    def _():
        firsts.frames()

    second_sum.gather_near()
    first_sum.gather_z()
    second_sum.gather_far()
    first_sum.gather_near()

    @pl.when(me.z == NZ - 1)
    def _():
        firsts.await_frames()
        input_layer(1)
        give_grad(1)

    first_sum.gather_far()
    second_sum.gather_core()
    second_sum.finish()
    for field in fields:
        field.finish()
    for i in range(1, 4):
        take(full_first, (GROUP - 1) * 2 * 4 * COLS, block_send.at[i])
    for i in range(2, 4):
        await_blocks(full_first, block_recv.at[i], block_own.at[i])
    first_sum.gather_core()
    first_sum.finish()


def write_out(critic_in, grad_in, first_in, second_in, critic, grad, first, second, wide, sem):
    half = 27 * CH // 2
    stores = []
    for n, (source, target) in enumerate(((first_in, first), (second_in, second))):
        for h in range(2):
            i = 2 * n + h

            @pl.loop(0, half // 192)
            def _(k):
                wide[i, rows_of(k * 192, 192), :] = source[rows_of(h * half + k * 192, 192), :].astype(F32)

            stores.append(pltpu.make_async_copy(wide.at[i], target.at[pl.ds(h * half, half)], sem.at[i]))
            stores[-1].start()
    for n, (source, target) in enumerate(((critic_in, critic), (grad_in, grad))):
        stores.append(pltpu.make_async_copy(source, target, sem.at[4 + n]))
        stores[-1].start()
    for one in stores:
        one.wait()


def on_device(clip, first_kernel, second_kernel, cotangent):
    cells = clip.shape[0] * lax.axis_size("frame") * clip.shape[1] * lax.axis_size("row") * clip.shape[2]
    scale = 1.0 / float(cells) ** 0.5
    vmem, anywhere = pl.BlockSpec(memory_space=pltpu.VMEM), pl.BlockSpec(memory_space=pl.ANY)
    total = jax.ShapeDtypeStruct((ROWS, CH), BF16)
    dma = pltpu.SemaphoreType.DMA
    flat = (2 * 4 * GROUP * COLS, CH)

    def field(halo):
        return pltpu.VMEM((FR + 2, COLS + 2 * halo, ROWN, CH), BF16)

    results = pl.pallas_call(
        functools.partial(kernel, scale),
        out_shape=(jax.ShapeDtypeStruct(clip.shape, BF16), jax.ShapeDtypeStruct(clip.shape, BF16), total, total),
        in_specs=[pl.BlockSpec(memory_space=pltpu.HBM)] * 4,
        out_specs=(vmem, vmem, vmem, vmem),
        scratch_shapes=[
            field(2), field(1), field(1), field(1),
            pltpu.VMEM((12 * CH, 6 * CH), BF16), pltpu.VMEM((6 * CH, 12 * CH), BF16),
            pltpu.VMEM((12 * CH, 6 * CH), BF16), pltpu.VMEM((6 * CH, 12 * CH), BF16),
            pltpu.VMEM(clip.shape, BF16), pltpu.VMEM(clip.shape, BF16),
            pltpu.VMEM((3, FR, ROWN, COLS, CH), BF16),
            pltpu.VMEM((FR, COLS, ROWN, CH), BF16),
            pltpu.VMEM((2, POS, 2 * CH), F32),
            pltpu.VMEM((6 * CH, 2 * POS), BF16),
            pltpu.VMEM((3, 6 * CH, 4 * CH), F32),
            pltpu.VMEM((2, ROWS, CH), BF16),
            pltpu.VMEM((2, HALF, CH), BF16),
            pltpu.VMEM((2, HALF, CH), BF16),
            pltpu.VMEM((2, HALF // 4, CH), BF16),
            pltpu.VMEM((2, BLK, CH), BF16),
            pltpu.VMEM((2, NZ * TILE, CH), BF16),
            dma((2, 8)), dma((2, 8)), dma((4, 7)), dma((4, 7)), dma((4,)), dma((4,)), dma((4,)), dma((2, 2)), dma((2,)),
            pltpu.VMEM((2, ROWN, COLS, CH), BF16), dma((GROUP,)), dma((2,)),
        ],
        compiler_params=pltpu.CompilerParams(collective_id=0, has_side_effects=True, vmem_limit_bytes=38 << 20),
    )(*(pltpu.with_memory_space_constraint(one, pltpu.HBM) for one in (
        clip, cotangent, first_kernel.reshape(27, CH, CH), second_kernel.reshape(27, CH, CH))))
    critic_map, clip_grad, first, second = results

    whole = jax.ShapeDtypeStruct((27 * CH, CH), F32)
    critic_map, clip_grad, first, second = pl.pallas_call(
        write_out,
        out_shape=(jax.ShapeDtypeStruct(flat, BF16), jax.ShapeDtypeStruct(flat, BF16), whole, whole),
        in_specs=[vmem] * 4,
        out_specs=(anywhere,) * 4,
        scratch_shapes=[pltpu.VMEM((4, 27 * CH // 2, CH), F32), dma((6,))],
        compiler_params=pltpu.CompilerParams(vmem_limit_bytes=10 << 20),
    )(critic_map.reshape(flat), clip_grad.reshape(flat), first, second)
    taps = (3, 3, 3, CH, CH)
    return critic_map.reshape(clip.shape), clip_grad.reshape(clip.shape), first.reshape(taps), second.reshape(taps)


def solution(mesh):
    placed = (P("frame", "row", None, None), P(), P(), P("frame", "row", None, None))
    return jax.shard_map(
        on_device,
        mesh=mesh,
        in_specs=placed,
        out_specs=(P("frame", "row", None, None), P("frame", "row", None, None), P(), P()),
        check_vma=False,
    )
```

```python
import functools

import jax
import jax.numpy as jnp
from jax import lax
from jax.experimental import pallas as pl
from jax.experimental.pallas import tpu as pltpu
from jax.sharding import PartitionSpec as P

MESH = pl.DeviceIdType.MESH
BF16, F32 = jnp.bfloat16, jnp.float32
CH = 128

NX, NY, NZ = 4, 4, 8
NXY = NX * NY
BLK = 112
HALF = NXY * BLK
ROWS = 2 * HALF
TILE = 16
ZT = BLK // TILE


class Place:
    def __init__(self):
        f, r = lax.axis_index("frame"), lax.axis_index("row")
        self.x, self.z = f // (2 * NZ), (f // 2) % NZ
        self.y, self.core = (r // 2) * 2 + f % 2, r % 2
        self.p = self.x * NY + self.y

    @staticmethod
    def at(x, y, z, core):
        return ((x * NZ + z) * 2 + y % 2, (y // 2) * 2 + core)


def remote(src, dst, send, recv, device):
    return pltpu.make_async_remote_copy(
        src_ref=src, dst_ref=dst, send_sem=send, recv_sem=recv, device_id=device, device_id_type=MESH)


def take(ref, rows, sem):
    view = ref.at[pl.ds(0, rows)]
    pltpu.make_async_copy(view, view, sem).wait()


def rows_of(start, size):
    return pl.ds(pl.multiple_of(start, TILE), size)


class AllReduce:
    A, B = (256, 64), (192, 48)
    START_B = NX * 256

    def __init__(self, me, part, full, other, slots, near, piece, tiles, send, recv):
        self.me, self.part, self.full = me, part, full
        self.other, self.slots, self.near, self.piece, self.tiles = other, slots, near, piece, tiles
        self.send, self.recv = send, recv
        self.base = me.core * HALF

    def x_peer(self, o):
        x = (self.me.x + o) % NX
        return x, Place.at(x, self.me.y, self.me.z, self.me.core)

    def y_peer(self, o):
        y = (self.me.y + o) % NY
        return y, Place.at(self.me.x, y, self.me.z, self.me.core)

    def z_peer(self, o):
        d = (self.me.z + o) % NZ
        return d, Place.at(self.me.x, self.me.y, d, self.me.core)

    def twin(self):
        return Place.at(self.me.x, self.me.y, self.me.z, 1 - self.me.core)

    def row_a(self, x, y):
        return self.base + x * self.A[0] + y * self.A[1]

    def row_b(self, x, y):
        return self.base + self.START_B + y * self.B[0] + x * self.B[1]

    def push(self, stage, source, start, target, to, size, peer):
        remote(source.at[rows_of(start, size)], target.at[rows_of(to, size)], self.send.at[stage], self.recv.at[stage], peer).start()

    def scatter_core(self):
        self.push(0, self.part, (1 - self.me.core) * HALF, self.other, 0, HALF, self.twin())

    def scatter_far(self):
        me = self.me
        take(self.other, HALF, self.recv.at[0])

        @pl.loop(0, HALF // 128)
        def _(i):
            mine = rows_of(self.base + i * 128, 128)
            total = self.part[mine, :].astype(F32) + self.other[rows_of(i * 128, 128), :].astype(F32)
            self.part[mine, :] = total.astype(BF16)

        @pl.loop(1, NX)
        def _(o):
            x, peer = self.x_peer(o)
            self.push(1, self.part, self.row_a(x, 0), self.slots, me.x * self.A[0], self.A[0], peer)
            y, peer = self.y_peer(o)
            self.push(1, self.part, self.row_b(0, y), self.slots, self.START_B + me.y * self.B[0], self.B[0], peer)

    def scatter_near(self):
        me = self.me
        take(self.slots, 3 * (self.A[0] + self.B[0]), self.recv.at[1])

        @pl.loop(0, 4)
        def _(i):
            for start, slot, mine, pitch, size in (
                (self.row_a(me.x, 0), 0, me.x, self.A[0], self.A[1]),
                (self.row_b(0, me.y), self.START_B, me.y, self.B[0], self.B[1])):
                rows = rows_of(start + i * size, size)
                total = self.part[rows, :].astype(F32)
                for o in range(1, 4):
                    total = total + self.slots[rows_of(slot + ((mine + o) % 4) * pitch + i * size, size), :].astype(F32)
                self.part[rows, :] = total.astype(BF16)

        @pl.loop(1, NX)
        def _(o):
            y, peer = self.y_peer(o)
            self.push(2, self.part, self.row_a(me.x, y), self.near, me.y * self.A[1], self.A[1], peer)
            x, peer = self.x_peer(o)
            self.push(2, self.part, self.row_b(x, me.y), self.near, NY * self.A[1] + me.x * self.B[1], self.B[1], peer)

    def scatter_z(self):
        me = self.me
        take(self.near, 3 * (self.A[1] + self.B[1]), self.recv.at[2])
        for start, slot, mine, size, to in (
            (self.row_a(me.x, me.y), 0, me.y, self.A[1], 0),
            (self.row_b(me.x, me.y), NY * self.A[1], me.x, self.B[1], self.A[1])):
            total = self.part[rows_of(start, size), :].astype(F32)
            for o in range(1, 4):
                total = total + self.near[rows_of(slot + ((mine + o) % 4) * size, size), :].astype(F32)
            self.piece[to : to + size, :] = total.astype(BF16)

        @pl.loop(1, NZ)
        def _(o):
            d, peer = self.z_peer(o)

            @pl.when(d < ZT)
            def _():
                self.push(3, self.piece, d * TILE, self.tiles, me.z * TILE, TILE, peer)

    def gather_z(self):
        me = self.me

        @pl.when(me.z < ZT)
        def _():
            take(self.tiles, (NZ - 1) * TILE, self.recv.at[3])
            total = self.piece[rows_of(me.z * TILE, TILE), :].astype(F32)
            for o in range(1, NZ):
                d = (me.z + o) % NZ
                total = total + self.tiles[rows_of(d * TILE, TILE), :].astype(F32)
            in_a = self.A[1] // TILE
            row = jnp.where(me.z < in_a, self.row_a(me.x, me.y) + me.z * TILE, self.row_b(me.x, me.y) + (me.z - in_a) * TILE)
            self.full[rows_of(row, TILE), :] = total.astype(BF16)

            @pl.loop(1, NZ)
            def _(o):
                d, peer = self.z_peer(o)
                self.push(4, self.full, row, self.full, row, TILE, peer)

    def gather_near(self):
        me = self.me

        @pl.when(me.z < ZT)
        def _():
            take(self.full, (ZT - 1) * TILE, self.recv.at[4])

        @pl.when(me.z >= ZT)
        def _():
            take(self.full, ZT * TILE, self.recv.at[4])

        a, b = self.row_a(me.x, me.y), self.row_b(me.x, me.y)

        @pl.loop(1, NX)
        def _(o):
            self.push(5, self.full, a, self.full, a, self.A[1], self.y_peer(o)[1])
            self.push(5, self.full, b, self.full, b, self.B[1], self.x_peer(o)[1])

    def gather_far(self):
        me = self.me
        take(self.full, 3 * (self.A[1] + self.B[1]), self.recv.at[5])
        a, b = self.row_a(me.x, 0), self.row_b(0, me.y)

        @pl.loop(1, NX)
        def _(o):
            self.push(6, self.full, a, self.full, a, self.A[0], self.x_peer(o)[1])
            self.push(6, self.full, b, self.full, b, self.B[0], self.y_peer(o)[1])

    def gather_core(self):
        take(self.full, 3 * (self.A[0] + self.B[0]), self.recv.at[6])
        self.push(7, self.full, self.base, self.full, self.base, HALF, self.twin())

    def finish(self):
        me = self.me
        take(self.full, HALF, self.recv.at[7])
        take(self.part, HALF, self.send.at[0])
        take(self.part, 3 * (self.A[0] + self.B[0]), self.send.at[1])
        take(self.part, 3 * (self.A[1] + self.B[1]), self.send.at[2])

        @pl.when(me.z < ZT)
        def _():
            take(self.piece, (ZT - 1) * TILE, self.send.at[3])
            take(self.full, (NZ - 1) * TILE, self.send.at[4])

        @pl.when(me.z >= ZT)
        def _():
            take(self.piece, ZT * TILE, self.send.at[3])

        take(self.full, 3 * (self.A[1] + self.B[1]), self.send.at[5])
        take(self.full, 3 * (self.A[0] + self.B[0]), self.send.at[6])
        take(self.full, HALF, self.send.at[7])


def greet_reduce_peers(me, barrier):
    pl.semaphore_signal(barrier, inc=1, device_id=Place.at(me.x, me.y, me.z, 1 - me.core), device_id_type=MESH)

    @pl.loop(1, NXY)
    def _(o):
        p = (me.p + o) % NXY
        pl.semaphore_signal(barrier, inc=1, device_id=Place.at(p // NY, p % NY, me.z, me.core), device_id_type=MESH)

    @pl.loop(1, NZ)
    def _(o):
        d = (me.z + o) % NZ
        pl.semaphore_signal(barrier, inc=1, device_id=Place.at(me.x, me.y, d, me.core), device_id_type=MESH)

    return 1 + NXY - 1 + NZ - 1

GROUP, FR, COLS, ROWN = 8, 4, 32, 16
POS = COLS * ROWN
NG = NX * NZ


class Ring:
    def __init__(self):
        f, r = lax.axis_index("frame"), lax.axis_index("row")
        self.g, self.y_lo, self.r = f // 2, f % 2, r
        self.s = (r // 2) * 4 + self.y_lo * 2 + r % 2

    @staticmethod
    def parts(s):
        return (s // 2) % 2, (s // 4) * 2 + s % 2

    @staticmethod
    def at(g, s):
        y_lo, r = Ring.parts(s)
        return (g * 2 + y_lo, r)


class Field:
    def __init__(self, ref, ring, own, halo, step, whole, send, recv):
        self.ref, self.ring, self.own, self.halo, self.step, self.whole = ref, ring, own, halo, step, whole
        self.send, self.recv = send, recv
        self.width = COLS + 2 * halo

    def clear(self):
        far = 0 if self.own else FR
        self.ref[far : far + 2] = jnp.zeros((2, self.width, ROWN, CH), BF16)
        for col in (0, COLS + self.halo):
            self.ref[self.own : self.own + FR, col : col + self.halo] = jnp.zeros((FR, self.halo, ROWN, CH), BF16)

    def put(self, f, start, value):
        width = value.shape[0] // ROWN
        self.ref[self.own + f, self.halo + start : self.halo + start + width] = value.astype(BF16).reshape(width, ROWN, CH)

    def to_left(self):
        return self.ring.s > 0

    def to_right(self):
        return self.ring.s < GROUP - 1

    def has_target(self):
        return self.ring.g < NG - 1 if self.step > 0 else self.ring.g > 0

    def has_source(self):
        return self.ring.g > 0 if self.step > 0 else self.ring.g < NG - 1

    def copy(self, frames, col, to_frames, to_col, width, g, s, i):
        return remote(self.ref.at[frames, pl.ds(col, width)], self.ref.at[to_frames, pl.ds(to_col, width)],
                      self.send.at[i], self.recv.at[i], Ring.at(g, s))

    def edge(self, frames, to_frames, side, g, i):
        halo, s = self.halo, self.ring.s
        source, target = (halo, COLS + halo) if side < 0 else (COLS, 0)
        self.copy(frames, source, to_frames, target, halo, g, s + side, i).start()

    def edges(self, q):
        frames, i = self._pair(q)

        @pl.when(self._held(q) & self.to_left())
        def _():
            self.edge(frames, frames, -1, self.ring.g, i)

        @pl.when(self._held(q) & self.to_right())
        def _():
            self.edge(frames, frames, 1, self.ring.g, i + 1)

    def _pair(self, q):
        return pl.ds(self.own + 2 * q, 2), (2 * q) % 6

    def _held(self, q):
        return self.has_source() if q < 0 else self.ring.g >= 0

    def await_edges(self, q):
        self._edges(q, self.recv, self.to_right(), self.to_left())

    def _edges(self, q, sem, left, right):
        frames, i = self._pair(q)
        view = self.ref.at[frames, pl.ds(0, self.halo)]

        @pl.when(self._held(q) & left)
        def _():
            pltpu.make_async_copy(view, view, sem.at[i]).wait()

        @pl.when(self._held(q) & right)
        def _():
            pltpu.make_async_copy(view, view, sem.at[i + 1]).wait()

    def span(self):
        return (0, self.width) if self.whole else (self.halo, COLS)

    def frames(self, quarter=None):
        g, s = self.ring.g + self.step, self.ring.s
        mine, theirs = (pl.ds(FR, 2), pl.ds(0, 2)) if self.step > 0 else (pl.ds(0, 2), pl.ds(FR, 2))
        start, width = self.span()
        if quarter is not None:
            start, width = start + quarter * (width // 4), width // 4

        @pl.when(self.has_target())
        def _():
            self.copy(mine, start, theirs, start, width, g, s, 4).start()

        if self.whole or quarter:
            return

        @pl.when(self.has_target() & self.to_left())
        def _():
            self.edge(mine, theirs, -1, g, 5)

        @pl.when(self.has_target() & self.to_right())
        def _():
            self.edge(mine, theirs, 1, g, 6)

    def _frames(self, sem, there, left, right):
        start, width = self.span()
        body, col = self.ref.at[pl.ds(0, 2), pl.ds(start, width)], self.ref.at[pl.ds(0, 2), pl.ds(0, self.halo)]

        @pl.when(there)
        def _():
            pltpu.make_async_copy(body, body, sem.at[4]).wait()

        if self.whole:
            return

        @pl.when(there & left)
        def _():
            pltpu.make_async_copy(col, col, sem.at[5]).wait()

        @pl.when(there & right)
        def _():
            pltpu.make_async_copy(col, col, sem.at[6]).wait()

    def await_frames(self):
        self._frames(self.recv, self.has_source(), self.to_right(), self.to_left())

    def finish(self):
        if not self.whole:
            for q in range(-1 if self.step > 0 else 0, 2):
                self._edges(q, self.send, self.to_left(), self.to_right())
        if self.whole or self.step < 0:
            self._frames(self.send, self.has_target(), self.to_left(), self.to_right())

    def slab(self, p, k, start, width):
        return self.ref[2 * p + k, start : start + width].reshape(width * ROWN, CH)


def build_weights(kernel, ahead, back, sem):
    zero = jnp.zeros((CH, CH), BF16)
    for k, j in ((0, 1), (3, 0)):
        @pl.loop(0, 9)
        def _(bc):
            b, c = bc // 3, bc % 3
            ahead[pl.ds(pl.multiple_of((c * 4 + k) * CH, CH), CH), pl.ds(pl.multiple_of((b * 2 + j) * CH, CH), CH)] = zero
            back[pl.ds(pl.multiple_of((b * 2 + j) * CH, CH), CH), pl.ds(pl.multiple_of((c * 4 + k) * CH, CH), CH)] = zero

    @pl.loop(0, 27)
    def _(tap):
        a, b, c = tap // 9, (tap // 3) % 3, tap % 3
        for j in range(2):
            k = a + j
            pltpu.make_async_copy(
                kernel.at[tap],
                ahead.at[pl.ds(pl.multiple_of((c * 4 + k) * CH, CH), CH), pl.ds(pl.multiple_of((b * 2 + j) * CH, CH), CH)],
                sem.at[0]).start()
            k = j + 2 - a
            pltpu.make_async_copy(
                kernel.at[tap],
                back.at[pl.ds(pl.multiple_of(((2 - b) * 2 + j) * CH, CH), CH), pl.ds(pl.multiple_of(((2 - c) * 4 + k) * CH, CH), CH)],
                sem.at[1]).start()


def await_weights(ahead, back, sem):
    view = ahead.at[pl.ds(0, 54 * CH * CH // ahead.shape[1])]
    pltpu.make_async_copy(view, view, sem.at[0]).wait()
    view = back.at[pl.ds(0, 54 * CH * CH // back.shape[1])]
    pltpu.make_async_copy(view, view, sem.at[1]).wait()


def row_index(shape):
    return lax.broadcasted_iota(jnp.int32, shape, 0) % ROWN


def from_above(value):
    return jnp.where(row_index(value.shape) == 0, 0.0, pltpu.roll(value, 1, axis=0))


def from_below(value):
    return jnp.where(row_index(value.shape) == ROWN - 1, 0.0, pltpu.roll(value, value.shape[0] - 1, axis=0))


def convolve(field, weights, p, contract, start, width):
    lhs = jnp.concatenate([field.slab(p, k, start + c, width) for c in range(3) for k in range(4)], axis=1)
    rows = lax.dot_general(lhs, weights[...], (((1,), (contract,)), ((), ())), preferred_element_type=F32)
    above, level, below = (rows[:, b * 2 * CH : (b + 1) * 2 * CH] for b in range(3))
    return level + from_above(above) + from_below(below)


def store_turned(turned, delta, start):
    for b, value in enumerate((from_below(delta), delta, from_above(delta))):
        turned[b * 2 * CH : (b + 1) * 2 * CH, start : start + delta.shape[0]] = value.astype(BF16).T


def pair_sums(field, turned, p, c):
    rhs = jnp.concatenate([field.slab(p, k, field.halo - 1 + c, COLS) for k in range(4)], axis=1)
    return lax.dot_general(turned[:, p * POS : (p + 1) * POS], rhs, (((1,), (0,)), ((), ())), preferred_element_type=F32)


def begin_grads(field, turned, begun, p):
    for c in range(3):
        begun[c] = pair_sums(field, turned, p, c)


def weight_grads(field, turned, part, scale, begun=None):
    for c in range(3):
        if begun is None:
            rhs = jnp.concatenate(
                [jnp.concatenate([field.slab(p, k, field.halo - 1 + c, COLS) for k in range(4)], axis=1) for p in range(2)], axis=0)
            sums = lax.dot_general(turned[...], rhs, (((1,), (0,)), ((), ())), preferred_element_type=F32)
        else:
            sums = begun[c] + pair_sums(field, turned, 1, c)
        for b in range(3):
            for a in range(3):
                one = sums[2 * b * CH : (2 * b + 1) * CH, a * CH : (a + 1) * CH]
                two = sums[(2 * b + 1) * CH : (2 * b + 2) * CH, (a + 1) * CH : (a + 2) * CH]
                tap = (a * 3 + b) * 3 + c
                part[tap * CH : (tap + 1) * CH, :] = ((one + two) * scale).T.astype(BF16)


def swap(value):
    return jnp.swapaxes(value, 0, 1)


def spread(ring, source, stage, send, recv, own):
    chip, core = ring.s // 2, ring.s % 2
    for turn, flip in ((0, 1), (1, 0), (3, 0), (1, 1), (3, 1), (2, 0), (2, 1)):
        d = (chip + turn) % 4 * 2 + (core + flip) % 2
        cols = pl.ds(pl.multiple_of(d * COLS, COLS), COLS)
        remote(source.at[:, :, cols], stage.at[pl.ds(2 * ring.y_lo, 2), pl.ds(4 * ring.r, 4)], send, recv, Ring.at(ring.g, d)).start()

    cols = pl.ds(pl.multiple_of(ring.s * COLS, COLS), COLS)
    pltpu.make_async_copy(source.at[:, :, cols], stage.at[pl.ds(2 * ring.y_lo, 2), pl.ds(4 * ring.r, 4)], own).start()


def relay(ring, stage, flat, recv, own, ahead, there, send, landed):
    for turn in (0, 3, 1, 2):
        for core in range(2):
            s = (ring.s + 2 * turn) % GROUP // 2 * 2 + core
            half, quarter = Ring.parts(s)

            @pl.when(s == ring.s)
            def _():
                take(flat, 2 * 4 * COLS, own)

            @pl.when(s != ring.s)
            def _():
                take(flat, 2 * 4 * COLS, recv.at[s])

            @pl.when(there & (half == 1))
            def _():
                rows = pl.ds(4 * quarter, 4)
                remote(stage.at[pl.ds(2, 2), rows], ahead.at[:, rows], send, landed, Ring.at(ring.g + 1, ring.s)).start()


def give_back(ring, stage, result, send, recv, own, half):
    cols = pl.ds(pl.multiple_of(ring.s * COLS, COLS), COLS)
    pair = pl.ds(2 * half, 2)

    @pl.loop(0, 4)
    def _(i):
        quarter = (ring.r + i) % 4
        rows = pl.ds(4 * quarter, 4)
        here = (half == ring.y_lo) & (i == 0)

        @pl.when(here)
        def _():
            pltpu.make_async_copy(stage.at[pair, rows], result.at[:, :, cols], own).start()

        @pl.when(jnp.logical_not(here))
        def _():
            remote(stage.at[pair, rows], result.at[:, :, cols], send, recv, (ring.g * 2 + half, quarter)).start()


def await_blocks(flat, sem, own):
    take(flat, (GROUP - 1) * 2 * 4 * COLS, sem)
    take(flat, 2 * 4 * COLS, own)


def kernel(scale, clip_in, cotangent_in, first_kernel, second_kernel, critic_map, clip_grad, full_first, full_second,
           clip_a, act_a, second_a, first_a, first_w, first_wt, second_w, second_wt, clip, cotangent, stage, cot_f, slopes,
           turned, begun, part, other, slots, near, piece, tiles,
           red_send, red_recv, halo_send, halo_recv, block_send, block_recv, block_own, weight_sem, load_sem,
           ahead, clip_recv, ahead_sem):
    loads = [pltpu.make_async_copy(source, target, load_sem.at[i])
             for i, (source, target) in enumerate(((clip_in, clip), (cotangent_in, cotangent)))]
    for load in loads:
        load.start()
    me, ring = Place(), Ring()
    clips = Field(clip_a, ring, 2, 2, 1, False, halo_send.at[0], halo_recv.at[0])
    acts = Field(act_a, ring, 2, 1, 1, True, halo_send.at[1], halo_recv.at[1])
    seconds = Field(second_a, ring, 0, 1, -1, False, halo_send.at[2], halo_recv.at[2])
    firsts = Field(first_a, ring, 0, 1, -1, False, halo_send.at[3], halo_recv.at[3])
    fields = (clips, acts, seconds, firsts)
    first_sum, second_sum = (
        AllReduce(me, part.at[i], full, other.at[i], slots.at[i], near.at[i], piece.at[i], tiles.at[i],
                  red_send.at[i], red_recv.at[i])
        for i, full in enumerate((full_first, full_second)))

    for field in fields:
        field.clear()

    barrier = pltpu.get_barrier_semaphore()
    count = greet_reduce_peers(me, barrier)

    @pl.loop(1, GROUP)
    def _(o):
        pl.semaphore_signal(barrier, inc=1, device_id=Ring.at(ring.g, (ring.s + o) % GROUP), device_id_type=MESH)

    count = count + GROUP - 1
    for step in (-1, 1):
        for side in (-1, 0, 1):
            g, s = ring.g + step, ring.s + side
            there = (g >= 0) & (g < NG) & (s >= 0) & (s < GROUP)

            @pl.when(there)
            def _():
                pl.semaphore_signal(barrier, inc=1, device_id=Ring.at(g, s), device_id_type=MESH)

            count = count + jnp.where(there, 1, 0)
    build_weights(first_kernel, first_w, first_wt, weight_sem.at[0])
    for i in range(2):
        part[i, 27 * CH :, :] = jnp.zeros((CH, CH), BF16)
    loads[0].wait()
    pl.semaphore_wait(barrier, count)

    spread(ring, clip, stage.at[0], block_send.at[0], clip_recv.at[ring.s], block_own.at[0])
    build_weights(second_kernel, second_w, second_wt, weight_sem.at[1])

    relay(ring, stage.at[0], full_first, clip_recv, block_own.at[0], ahead, clips.has_target(), ahead_sem.at[0], ahead_sem.at[1])
    for f in range(FR):
        clip_a[2 + f, 2 : COLS + 2] = swap(stage[0, f])
    clips.edges(0)
    clips.edges(1)
    loads[1].wait()
    spread(ring, cotangent, stage.at[1], block_send.at[1], block_recv.at[1], block_own.at[1])
    await_weights(first_w, first_wt, weight_sem.at[0])
    await_weights(second_w, second_wt, weight_sem.at[1])
    clips.await_edges(0)
    clips.await_edges(1)

    def sigmoid_slope(z):
        sigma = jax.nn.sigmoid(z)
        return sigma, sigma * (1.0 + z * (1.0 - sigma))

    def first_layer(p):
        width = COLS // 2 + 1
        for half in range(2):
            start = half * width
            pre = convolve(clips, first_w, p, 0, start, width)
            sigma, slope = sigmoid_slope(pre)
            act = (pre * sigma).astype(BF16)
            for j in range(2):
                act_a[2 + 2 * p + j, start : start + width] = act[:, j * CH : (j + 1) * CH].reshape(width, ROWN, CH)
            skip = ROWN if half == 0 else 0
            slopes[p, half * POS // 2 : (half + 1) * POS // 2] = slope[skip : skip + POS // 2]
        pair, edge = pl.ds(2 + 2 * p, 2), jnp.zeros((2, ROWN, CH), BF16)

        @pl.when(ring.s == 0)
        def _():
            act_a[pair, 0] = edge

        @pl.when(ring.s == GROUP - 1)
        def _():
            act_a[pair, COLS + 1] = edge

    width = COLS // 2

    def second_layer(p):
        for start in (0, width):
            pre = convolve(acts, second_w, p, 0, start, width)
            sigma, slope = sigmoid_slope(pre)
            critic = pre * sigma
            delta = slope * jnp.concatenate(
                [cot_f[2 * p + j, start : start + width].reshape(width * ROWN, CH).astype(F32) for j in range(2)], axis=1)
            for j in range(2):
                half = slice(j * CH, (j + 1) * CH)
                stage[2, 2 * p + j, :, start : start + width] = swap(critic[:, half].astype(BF16).reshape(width, ROWN, CH))
                seconds.put(2 * p + j, start, delta[:, half])
            store_turned(turned, delta, p * POS + start * ROWN)

    def back_layer(p):
        for start in (0, width):
            rows = slice(start * ROWN, (start + width) * ROWN)
            delta = convolve(seconds, second_wt, p, 1, start, width) * slopes[p, rows]
            for j in range(2):
                firsts.put(2 * p + j, start, delta[:, j * CH : (j + 1) * CH])
            store_turned(turned, delta, p * POS + start * ROWN)

    def input_layer(p):
        for start in (0, width):
            back = convolve(firsts, first_wt, p, 1, start, width)
            for j in range(2):
                stage[0, 2 * p + j, :, start : start + width] = swap(
                    back[:, j * CH : (j + 1) * CH].astype(BF16).reshape(width, ROWN, CH))

    def cross(quarter):
        @pl.when(me.z == 0)
        def _():
            firsts.frames(quarter)

    def give_critic(half):
        give_back(ring, stage.at[2], critic_map, block_send.at[2], block_recv.at[2], block_own.at[2], half)

    def give_grad(half):
        give_back(ring, stage.at[0], clip_grad, block_send.at[3], block_recv.at[3], block_own.at[3], half)

    first_layer(1)
    acts.frames()

    @pl.when(clips.has_source())
    def _():
        take(full_first, 4 * 2 * 4 * COLS, ahead_sem.at[1])
        for f in range(2):
            clip_a[f, 2 : COLS + 2] = swap(ahead[f])

    clips.edges(-1)
    clips.await_edges(-1)
    first_layer(0)
    await_blocks(full_first, block_recv.at[1], block_own.at[1])
    for f in range(FR):
        cot_f[f] = swap(stage[1, f])
    second_layer(1)
    seconds.edges(1)
    give_critic(1)
    acts.await_frames()
    second_layer(0)
    seconds.frames()
    seconds.edges(0)
    weight_grads(acts, turned, part.at[1], scale)
    second_sum.scatter_core()
    seconds.await_edges(0)
    seconds.await_edges(1)
    give_critic(0)
    back_layer(0)
    second_sum.scatter_far()
    firsts.edges(0)

    @pl.when(me.z != 0)
    def _():
        firsts.frames()

    begin_grads(clips, turned, begun, 0)
    seconds.await_frames()
    cross(0)
    back_layer(1)
    firsts.edges(1)
    cross(1)
    weight_grads(clips, turned, part.at[0], scale, begun)
    first_sum.scatter_core()
    cross(2)
    second_sum.scatter_near()
    firsts.await_edges(0)
    firsts.await_edges(1)
    first_sum.scatter_far()
    take(full_first, (GROUP - 1) * 2 * 4 * COLS, block_send.at[0])

    @pl.when(clips.has_target())
    def _():
        take(full_first, 4 * 2 * 4 * COLS, ahead_sem.at[0])

    input_layer(0)
    cross(3)
    second_sum.scatter_z()
    first_sum.scatter_near()

    firsts.await_frames()
    input_layer(1)
    give_grad(0)
    give_grad(1)
    second_sum.gather_z()
    first_sum.scatter_z()

    second_sum.gather_near()
    first_sum.gather_z()
    second_sum.gather_far()
    first_sum.gather_near()

    first_sum.gather_far()
    second_sum.gather_core()
    second_sum.finish()
    for field in fields:
        field.finish()
    for i in range(1, 4):
        take(full_first, (GROUP - 1) * 2 * 4 * COLS, block_send.at[i])
    for i in range(2, 4):
        await_blocks(full_first, block_recv.at[i], block_own.at[i])
    first_sum.gather_core()
    first_sum.finish()


def write_out(critic_in, grad_in, first_in, second_in, critic, grad, first, second, wide, sem):
    half = 27 * CH // 2
    stores = []
    for n, (source, target) in enumerate(((first_in, first), (second_in, second))):
        for h in range(2):
            i = 2 * n + h

            @pl.loop(0, half // 192)
            def _(k):
                wide[i, rows_of(k * 192, 192), :] = source[rows_of(h * half + k * 192, 192), :].astype(F32)

            stores.append(pltpu.make_async_copy(wide.at[i], target.at[pl.ds(h * half, half)], sem.at[i]))
            stores[-1].start()
    for n, (source, target) in enumerate(((critic_in, critic), (grad_in, grad))):
        stores.append(pltpu.make_async_copy(source, target, sem.at[4 + n]))
        stores[-1].start()
    for one in stores:
        one.wait()


def on_device(clip, first_kernel, second_kernel, cotangent):
    cells = clip.shape[0] * lax.axis_size("frame") * clip.shape[1] * lax.axis_size("row") * clip.shape[2]
    scale = 1.0 / float(cells) ** 0.5
    vmem, anywhere = pl.BlockSpec(memory_space=pltpu.VMEM), pl.BlockSpec(memory_space=pl.ANY)
    total = jax.ShapeDtypeStruct((ROWS, CH), BF16)
    dma = pltpu.SemaphoreType.DMA
    flat = (2 * 4 * GROUP * COLS, CH)

    def field(halo):
        return pltpu.VMEM((FR + 2, COLS + 2 * halo, ROWN, CH), BF16)

    results = pl.pallas_call(
        functools.partial(kernel, scale),
        out_shape=(jax.ShapeDtypeStruct(clip.shape, BF16), jax.ShapeDtypeStruct(clip.shape, BF16), total, total),
        in_specs=[pl.BlockSpec(memory_space=pltpu.HBM)] * 4,
        out_specs=(vmem, vmem, vmem, vmem),
        scratch_shapes=[
            field(2), field(1), field(1), field(1),
            pltpu.VMEM((12 * CH, 6 * CH), BF16), pltpu.VMEM((6 * CH, 12 * CH), BF16),
            pltpu.VMEM((12 * CH, 6 * CH), BF16), pltpu.VMEM((6 * CH, 12 * CH), BF16),
            pltpu.VMEM(clip.shape, BF16), pltpu.VMEM(clip.shape, BF16),
            pltpu.VMEM((3, FR, ROWN, COLS, CH), BF16),
            pltpu.VMEM((FR, COLS, ROWN, CH), BF16),
            pltpu.VMEM((2, POS, 2 * CH), F32),
            pltpu.VMEM((6 * CH, 2 * POS), BF16),
            pltpu.VMEM((3, 6 * CH, 4 * CH), F32),
            pltpu.VMEM((2, ROWS, CH), BF16),
            pltpu.VMEM((2, HALF, CH), BF16),
            pltpu.VMEM((2, HALF, CH), BF16),
            pltpu.VMEM((2, HALF // 4, CH), BF16),
            pltpu.VMEM((2, BLK, CH), BF16),
            pltpu.VMEM((2, NZ * TILE, CH), BF16),
            dma((2, 8)), dma((2, 8)), dma((4, 7)), dma((4, 7)), dma((4,)), dma((4,)), dma((4,)), dma((2, 2)), dma((2,)),
            pltpu.VMEM((2, ROWN, COLS, CH), BF16), dma((GROUP,)), dma((2,)),
        ],
        compiler_params=pltpu.CompilerParams(collective_id=0, has_side_effects=True, vmem_limit_bytes=38 << 20),
    )(*(pltpu.with_memory_space_constraint(one, pltpu.HBM) for one in (
        clip, cotangent, first_kernel.reshape(27, CH, CH), second_kernel.reshape(27, CH, CH))))
    critic_map, clip_grad, first, second = results

    whole = jax.ShapeDtypeStruct((27 * CH, CH), F32)
    critic_map, clip_grad, first, second = pl.pallas_call(
        write_out,
        out_shape=(jax.ShapeDtypeStruct(flat, BF16), jax.ShapeDtypeStruct(flat, BF16), whole, whole),
        in_specs=[vmem] * 4,
        out_specs=(anywhere,) * 4,
        scratch_shapes=[pltpu.VMEM((4, 27 * CH // 2, CH), F32), dma((6,))],
        compiler_params=pltpu.CompilerParams(vmem_limit_bytes=10 << 20),
    )(critic_map.reshape(flat), clip_grad.reshape(flat), first, second)
    taps = (3, 3, 3, CH, CH)
    return critic_map.reshape(clip.shape), clip_grad.reshape(clip.shape), first.reshape(taps), second.reshape(taps)


def solution(mesh):
    placed = (P("frame", "row", None, None), P(), P(), P("frame", "row", None, None))
    return jax.shard_map(
        on_device,
        mesh=mesh,
        in_specs=placed,
        out_specs=(P("frame", "row", None, None), P("frame", "row", None, None), P(), P()),
        check_vma=False,
    )
```

```python
import functools

import jax
import jax.numpy as jnp
from jax import lax
from jax.experimental import pallas as pl
from jax.experimental.pallas import tpu as pltpu
from jax.sharding import PartitionSpec as P

MESH = pl.DeviceIdType.MESH
BF16, F32 = jnp.bfloat16, jnp.float32
CH = 128

NX, NY, NZ = 4, 4, 8
NXY = NX * NY
BLK = 112
HALF = NXY * BLK
ROWS = 2 * HALF
TILE = 16
ZT = BLK // TILE


class Place:
    def __init__(self):
        f, r = lax.axis_index("frame"), lax.axis_index("row")
        self.x, self.z = f // (2 * NZ), (f // 2) % NZ
        self.y, self.core = (r // 2) * 2 + f % 2, r % 2
        self.p = self.x * NY + self.y

    @staticmethod
    def at(x, y, z, core):
        return ((x * NZ + z) * 2 + y % 2, (y // 2) * 2 + core)


def remote(src, dst, send, recv, device):
    return pltpu.make_async_remote_copy(
        src_ref=src, dst_ref=dst, send_sem=send, recv_sem=recv, device_id=device, device_id_type=MESH)


def take(ref, rows, sem):
    view = ref.at[pl.ds(0, rows)]
    pltpu.make_async_copy(view, view, sem).wait()


def rows_of(start, size):
    return pl.ds(pl.multiple_of(start, TILE), size)


class AllReduce:
    A, B = (256, 64), (192, 48)
    START_B = NX * 256

    def __init__(self, me, part, full, other, slots, near, piece, tiles, send, recv):
        self.me, self.part, self.full = me, part, full
        self.other, self.slots, self.near, self.piece, self.tiles = other, slots, near, piece, tiles
        self.send, self.recv = send, recv
        self.base = me.core * HALF

    def x_peer(self, o):
        x = (self.me.x + o) % NX
        return x, Place.at(x, self.me.y, self.me.z, self.me.core)

    def y_peer(self, o):
        y = (self.me.y + o) % NY
        return y, Place.at(self.me.x, y, self.me.z, self.me.core)

    def z_peer(self, o):
        d = (self.me.z + o) % NZ
        return d, Place.at(self.me.x, self.me.y, d, self.me.core)

    def twin(self):
        return Place.at(self.me.x, self.me.y, self.me.z, 1 - self.me.core)

    def row_a(self, x, y):
        return self.base + x * self.A[0] + y * self.A[1]

    def row_b(self, x, y):
        return self.base + self.START_B + y * self.B[0] + x * self.B[1]

    def push(self, stage, source, start, target, to, size, peer):
        remote(source.at[rows_of(start, size)], target.at[rows_of(to, size)], self.send.at[stage], self.recv.at[stage], peer).start()

    def scatter_core(self):
        self.push(0, self.part, (1 - self.me.core) * HALF, self.other, 0, HALF, self.twin())

    def scatter_far(self):
        me = self.me
        take(self.other, HALF, self.recv.at[0])

        @pl.loop(0, HALF // 128)
        def _(i):
            mine = rows_of(self.base + i * 128, 128)
            total = self.part[mine, :].astype(F32) + self.other[rows_of(i * 128, 128), :].astype(F32)
            self.part[mine, :] = total.astype(BF16)

        @pl.loop(1, NX)
        def _(o):
            x, peer = self.x_peer(o)
            self.push(1, self.part, self.row_a(x, 0), self.slots, me.x * self.A[0], self.A[0], peer)
            y, peer = self.y_peer(o)
            self.push(1, self.part, self.row_b(0, y), self.slots, self.START_B + me.y * self.B[0], self.B[0], peer)

    def scatter_near(self):
        me = self.me
        take(self.slots, 3 * (self.A[0] + self.B[0]), self.recv.at[1])

        @pl.loop(0, 4)
        def _(i):
            for start, slot, mine, pitch, size in (
                (self.row_a(me.x, 0), 0, me.x, self.A[0], self.A[1]),
                (self.row_b(0, me.y), self.START_B, me.y, self.B[0], self.B[1])):
                rows = rows_of(start + i * size, size)
                total = self.part[rows, :].astype(F32)
                for o in range(1, 4):
                    total = total + self.slots[rows_of(slot + ((mine + o) % 4) * pitch + i * size, size), :].astype(F32)
                self.part[rows, :] = total.astype(BF16)

        @pl.loop(1, NX)
        def _(o):
            y, peer = self.y_peer(o)
            self.push(2, self.part, self.row_a(me.x, y), self.near, me.y * self.A[1], self.A[1], peer)
            x, peer = self.x_peer(o)
            self.push(2, self.part, self.row_b(x, me.y), self.near, NY * self.A[1] + me.x * self.B[1], self.B[1], peer)

    def scatter_z(self):
        me = self.me
        take(self.near, 3 * (self.A[1] + self.B[1]), self.recv.at[2])
        for start, slot, mine, size, to in (
            (self.row_a(me.x, me.y), 0, me.y, self.A[1], 0),
            (self.row_b(me.x, me.y), NY * self.A[1], me.x, self.B[1], self.A[1])):
            total = self.part[rows_of(start, size), :].astype(F32)
            for o in range(1, 4):
                total = total + self.near[rows_of(slot + ((mine + o) % 4) * size, size), :].astype(F32)
            self.piece[to : to + size, :] = total.astype(BF16)

        @pl.loop(1, NZ)
        def _(o):
            d, peer = self.z_peer(o)

            @pl.when(d < ZT)
            def _():
                self.push(3, self.piece, d * TILE, self.tiles, me.z * TILE, TILE, peer)

    def gather_z(self):
        me = self.me

        @pl.when(me.z < ZT)
        def _():
            take(self.tiles, (NZ - 1) * TILE, self.recv.at[3])
            total = self.piece[rows_of(me.z * TILE, TILE), :].astype(F32)
            for o in range(1, NZ):
                d = (me.z + o) % NZ
                total = total + self.tiles[rows_of(d * TILE, TILE), :].astype(F32)
            in_a = self.A[1] // TILE
            row = jnp.where(me.z < in_a, self.row_a(me.x, me.y) + me.z * TILE, self.row_b(me.x, me.y) + (me.z - in_a) * TILE)
            self.full[rows_of(row, TILE), :] = total.astype(BF16)

            @pl.loop(1, NZ)
            def _(o):
                d, peer = self.z_peer(o)
                self.push(4, self.full, row, self.full, row, TILE, peer)

    def gather_near(self):
        me = self.me

        @pl.when(me.z < ZT)
        def _():
            take(self.full, (ZT - 1) * TILE, self.recv.at[4])

        @pl.when(me.z >= ZT)
        def _():
            take(self.full, ZT * TILE, self.recv.at[4])

        a, b = self.row_a(me.x, me.y), self.row_b(me.x, me.y)

        @pl.loop(1, NX)
        def _(o):
            self.push(5, self.full, a, self.full, a, self.A[1], self.y_peer(o)[1])
            self.push(5, self.full, b, self.full, b, self.B[1], self.x_peer(o)[1])

    def gather_far(self):
        me = self.me
        take(self.full, 3 * (self.A[1] + self.B[1]), self.recv.at[5])
        a, b = self.row_a(me.x, 0), self.row_b(0, me.y)

        @pl.loop(1, NX)
        def _(o):
            self.push(6, self.full, a, self.full, a, self.A[0], self.x_peer(o)[1])
            self.push(6, self.full, b, self.full, b, self.B[0], self.y_peer(o)[1])

    def gather_core(self):
        take(self.full, 3 * (self.A[0] + self.B[0]), self.recv.at[6])
        self.push(7, self.full, self.base, self.full, self.base, HALF, self.twin())

    def finish(self):
        me = self.me
        take(self.full, HALF, self.recv.at[7])
        take(self.part, HALF, self.send.at[0])
        take(self.part, 3 * (self.A[0] + self.B[0]), self.send.at[1])
        take(self.part, 3 * (self.A[1] + self.B[1]), self.send.at[2])

        @pl.when(me.z < ZT)
        def _():
            take(self.piece, (ZT - 1) * TILE, self.send.at[3])
            take(self.full, (NZ - 1) * TILE, self.send.at[4])

        @pl.when(me.z >= ZT)
        def _():
            take(self.piece, ZT * TILE, self.send.at[3])

        take(self.full, 3 * (self.A[1] + self.B[1]), self.send.at[5])
        take(self.full, 3 * (self.A[0] + self.B[0]), self.send.at[6])
        take(self.full, HALF, self.send.at[7])


def greet_reduce_peers(me, barrier):
    pl.semaphore_signal(barrier, inc=1, device_id=Place.at(me.x, me.y, me.z, 1 - me.core), device_id_type=MESH)

    @pl.loop(1, NXY)
    def _(o):
        p = (me.p + o) % NXY
        pl.semaphore_signal(barrier, inc=1, device_id=Place.at(p // NY, p % NY, me.z, me.core), device_id_type=MESH)

    @pl.loop(1, NZ)
    def _(o):
        d = (me.z + o) % NZ
        pl.semaphore_signal(barrier, inc=1, device_id=Place.at(me.x, me.y, d, me.core), device_id_type=MESH)

    return 1 + NXY - 1 + NZ - 1

GROUP, FR, COLS, ROWN = 8, 4, 32, 16
POS = COLS * ROWN
NG = NX * NZ


class Ring:
    def __init__(self):
        f, r = lax.axis_index("frame"), lax.axis_index("row")
        self.g, self.y_lo, self.r = f // 2, f % 2, r
        self.s = (r // 2) * 4 + self.y_lo * 2 + r % 2

    @staticmethod
    def parts(s):
        return (s // 2) % 2, (s // 4) * 2 + s % 2

    @staticmethod
    def at(g, s):
        y_lo, r = Ring.parts(s)
        return (g * 2 + y_lo, r)


class Field:
    def __init__(self, ref, ring, own, halo, step, whole, send, recv):
        self.ref, self.ring, self.own, self.halo, self.step, self.whole = ref, ring, own, halo, step, whole
        self.send, self.recv = send, recv
        self.width = COLS + 2 * halo

    def clear(self):
        far = 0 if self.own else FR

        @pl.when(jnp.logical_not(self.has_source()))
        def _():
            self.ref[far : far + 2] = jnp.zeros((2, self.width, ROWN, CH), BF16)

        edge = jnp.zeros((FR + 2, self.halo, ROWN, CH), BF16)

        @pl.when(jnp.logical_not(self.to_left()))
        def _():
            self.ref[:, 0 : self.halo] = edge

        @pl.when(jnp.logical_not(self.to_right()))
        def _():
            self.ref[:, COLS + self.halo :] = edge

    def put(self, f, start, value):
        width = value.shape[0] // ROWN
        self.ref[self.own + f, self.halo + start : self.halo + start + width] = value.astype(BF16).reshape(width, ROWN, CH)

    def to_left(self):
        return self.ring.s > 0

    def to_right(self):
        return self.ring.s < GROUP - 1

    def has_target(self):
        return self.ring.g < NG - 1 if self.step > 0 else self.ring.g > 0

    def has_source(self):
        return self.ring.g > 0 if self.step > 0 else self.ring.g < NG - 1

    def copy(self, frames, col, to_frames, to_col, width, g, s, i):
        return remote(self.ref.at[frames, pl.ds(col, width)], self.ref.at[to_frames, pl.ds(to_col, width)],
                      self.send.at[i], self.recv.at[i], Ring.at(g, s))

    def edge(self, frames, to_frames, side, g, i):
        halo, s = self.halo, self.ring.s
        source, target = (halo, COLS + halo) if side < 0 else (COLS, 0)
        self.copy(frames, source, to_frames, target, halo, g, s + side, i).start()

    def edges(self, q):
        frames, i = self._pair(q)

        @pl.when(self._held(q) & self.to_left())
        def _():
            self.edge(frames, frames, -1, self.ring.g, i)

        @pl.when(self._held(q) & self.to_right())
        def _():
            self.edge(frames, frames, 1, self.ring.g, i + 1)

    def _pair(self, q):
        return pl.ds(self.own + 2 * q, 2), (2 * q) % 6

    def _held(self, q):
        return self.has_source() if q < 0 else self.ring.g >= 0

    def await_edges(self, q):
        self._edges(q, self.recv, self.to_right(), self.to_left())

    def _edges(self, q, sem, left, right):
        frames, i = self._pair(q)
        view = self.ref.at[frames, pl.ds(0, self.halo)]

        @pl.when(self._held(q) & left)
        def _():
            pltpu.make_async_copy(view, view, sem.at[i]).wait()

        @pl.when(self._held(q) & right)
        def _():
            pltpu.make_async_copy(view, view, sem.at[i + 1]).wait()

    def span(self):
        return (0, self.width) if self.whole else (self.halo, COLS)

    def frames(self):
        g, s = self.ring.g + self.step, self.ring.s
        mine, theirs = (pl.ds(FR, 2), pl.ds(0, 2)) if self.step > 0 else (pl.ds(0, 2), pl.ds(FR, 2))
        start, width = self.span()

        @pl.when(self.has_target())
        def _():
            self.copy(mine, start, theirs, start, width, g, s, 4).start()

        if self.whole:
            return

        @pl.when(self.has_target() & self.to_left())
        def _():
            self.edge(mine, theirs, -1, g, 5)

        @pl.when(self.has_target() & self.to_right())
        def _():
            self.edge(mine, theirs, 1, g, 6)

    def _frames(self, sem, there, left, right):
        start, width = self.span()
        body, col = self.ref.at[pl.ds(0, 2), pl.ds(start, width)], self.ref.at[pl.ds(0, 2), pl.ds(0, self.halo)]

        @pl.when(there)
        def _():
            pltpu.make_async_copy(body, body, sem.at[4]).wait()

        if self.whole:
            return

        @pl.when(there & left)
        def _():
            pltpu.make_async_copy(col, col, sem.at[5]).wait()

        @pl.when(there & right)
        def _():
            pltpu.make_async_copy(col, col, sem.at[6]).wait()

    def await_frames(self):
        self._frames(self.recv, self.has_source(), self.to_right(), self.to_left())

    def finish(self):
        if not self.whole:
            for q in range(-1 if self.step > 0 else 0, 2):
                self._edges(q, self.send, self.to_left(), self.to_right())
        if self.whole or self.step < 0:
            self._frames(self.send, self.has_target(), self.to_left(), self.to_right())

    def slab(self, p, k, start, width):
        return self.ref[2 * p + k, start : start + width].reshape(width * ROWN, CH)


def build_weights(kernel, ahead, back, sem):
    zero = jnp.zeros((CH, CH), BF16)
    for k, j in ((0, 1), (3, 0)):
        @pl.loop(0, 9)
        def _(bc):
            b, c = bc // 3, bc % 3
            ahead[pl.ds(pl.multiple_of((c * 4 + k) * CH, CH), CH), pl.ds(pl.multiple_of((b * 2 + j) * CH, CH), CH)] = zero
            back[pl.ds(pl.multiple_of((b * 2 + j) * CH, CH), CH), pl.ds(pl.multiple_of((c * 4 + k) * CH, CH), CH)] = zero

    @pl.loop(0, 27)
    def _(tap):
        a, b, c = tap // 9, (tap // 3) % 3, tap % 3
        for j in range(2):
            k = a + j
            pltpu.make_async_copy(
                kernel.at[tap],
                ahead.at[pl.ds(pl.multiple_of((c * 4 + k) * CH, CH), CH), pl.ds(pl.multiple_of((b * 2 + j) * CH, CH), CH)],
                sem.at[0]).start()
            k = j + 2 - a
            pltpu.make_async_copy(
                kernel.at[tap],
                back.at[pl.ds(pl.multiple_of(((2 - b) * 2 + j) * CH, CH), CH), pl.ds(pl.multiple_of(((2 - c) * 4 + k) * CH, CH), CH)],
                sem.at[1]).start()


def await_weights(ahead, back, sem):
    view = ahead.at[pl.ds(0, 54 * CH * CH // ahead.shape[1])]
    pltpu.make_async_copy(view, view, sem.at[0]).wait()
    view = back.at[pl.ds(0, 54 * CH * CH // back.shape[1])]
    pltpu.make_async_copy(view, view, sem.at[1]).wait()


def row_index(shape):
    return lax.broadcasted_iota(jnp.int32, shape, 0) % ROWN


def from_above(value):
    return jnp.where(row_index(value.shape) == 0, 0.0, pltpu.roll(value, 1, axis=0))


def from_below(value):
    return jnp.where(row_index(value.shape) == ROWN - 1, 0.0, pltpu.roll(value, value.shape[0] - 1, axis=0))


def convolve(field, weights, p, contract, start, width):
    lhs = jnp.concatenate([field.slab(p, k, start + c, width) for c in range(3) for k in range(4)], axis=1)
    rows = lax.dot_general(lhs, weights[...], (((1,), (contract,)), ((), ())), preferred_element_type=F32)
    above, level, below = (rows[:, b * 2 * CH : (b + 1) * 2 * CH] for b in range(3))
    return level + from_above(above) + from_below(below)


def store_turned(turned, delta, start):
    for b, value in enumerate((from_below(delta), delta, from_above(delta))):
        turned[b * 2 * CH : (b + 1) * 2 * CH, start : start + delta.shape[0]] = value.astype(BF16).T


def pair_sums(field, turned, p, c):
    rhs = jnp.concatenate([field.slab(p, k, field.halo - 1 + c, COLS) for k in range(4)], axis=1)
    return lax.dot_general(turned[:, p * POS : (p + 1) * POS], rhs, (((1,), (0,)), ((), ())), preferred_element_type=F32)


def begin_grads(field, turned, begun, p):
    for c in range(3):
        begun[c] = pair_sums(field, turned, p, c)


def weight_grads(field, turned, part, scale, begun=None):
    for c in range(3):
        if begun is None:
            rhs = jnp.concatenate(
                [jnp.concatenate([field.slab(p, k, field.halo - 1 + c, COLS) for k in range(4)], axis=1) for p in range(2)], axis=0)
            sums = lax.dot_general(turned[...], rhs, (((1,), (0,)), ((), ())), preferred_element_type=F32)
        else:
            sums = begun[c] + pair_sums(field, turned, 1, c)
        for b in range(3):
            for a in range(3):
                one = sums[2 * b * CH : (2 * b + 1) * CH, a * CH : (a + 1) * CH]
                two = sums[(2 * b + 1) * CH : (2 * b + 2) * CH, (a + 1) * CH : (a + 2) * CH]
                tap = (a * 3 + b) * 3 + c
                part[tap * CH : (tap + 1) * CH, :] = ((one + two) * scale).T.astype(BF16)


def swap(value):
    return jnp.swapaxes(value, 0, 1)


def spread(ring, source, stage, send, recv, own):
    chip, core = ring.s // 2, ring.s % 2
    for turn, flip in ((0, 1), (1, 0), (3, 0), (1, 1), (3, 1), (2, 0), (2, 1)):
        d = (chip + turn) % 4 * 2 + (core + flip) % 2
        cols = pl.ds(pl.multiple_of(d * COLS, COLS), COLS)
        remote(source.at[:, :, cols], stage.at[pl.ds(2 * ring.y_lo, 2), pl.ds(4 * ring.r, 4)], send, recv, Ring.at(ring.g, d)).start()

    cols = pl.ds(pl.multiple_of(ring.s * COLS, COLS), COLS)
    pltpu.make_async_copy(source.at[:, :, cols], stage.at[pl.ds(2 * ring.y_lo, 2), pl.ds(4 * ring.r, 4)], own).start()


def relay(ring, stage, flat, recv, own, ahead, there, send, landed):
    for turn in (0, 3, 1, 2):
        for core in range(2):
            s = (ring.s + 2 * turn) % GROUP // 2 * 2 + core
            half, quarter = Ring.parts(s)

            @pl.when(s == ring.s)
            def _():
                take(flat, 2 * 4 * COLS, own)

            @pl.when(s != ring.s)
            def _():
                take(flat, 2 * 4 * COLS, recv.at[s])

            @pl.when(there & (half == 1))
            def _():
                rows = pl.ds(4 * quarter, 4)
                remote(stage.at[pl.ds(2, 2), rows], ahead.at[:, rows], send, landed, Ring.at(ring.g + 1, ring.s)).start()


def give_back(ring, stage, result, send, recv, own, half):
    cols = pl.ds(pl.multiple_of(ring.s * COLS, COLS), COLS)
    pair = pl.ds(2 * half, 2)

    @pl.loop(0, 4)
    def _(i):
        quarter = (ring.r + i) % 4
        rows = pl.ds(4 * quarter, 4)
        here = (half == ring.y_lo) & (i == 0)

        @pl.when(here)
        def _():
            pltpu.make_async_copy(stage.at[pair, rows], result.at[:, :, cols], own).start()

        @pl.when(jnp.logical_not(here))
        def _():
            remote(stage.at[pair, rows], result.at[:, :, cols], send, recv, (ring.g * 2 + half, quarter)).start()


def await_blocks(flat, sem, own):
    take(flat, (GROUP - 1) * 2 * 4 * COLS, sem)
    take(flat, 2 * 4 * COLS, own)


def kernel(scale, clip_in, cotangent_in, first_kernel, second_kernel, critic_map, clip_grad, full_first, second_out,
           clip_a, act_a, second_a, first_a, first_w, first_wt, second_w, second_wt, clip, cotangent, stage, cot_f, slopes,
           turned, begun, part, other, slots, near, piece, tiles,
           red_send, red_recv, halo_send, halo_recv, block_send, block_recv, block_own, weight_sem, load_sem,
           ahead, clip_recv, ahead_sem, full_second):
    loads = [pltpu.make_async_copy(source, target, load_sem.at[i])
             for i, (source, target) in enumerate(((clip_in, clip), (cotangent_in, cotangent)))]
    for load in loads:
        load.start()
    me, ring = Place(), Ring()
    clips = Field(clip_a, ring, 2, 2, 1, False, halo_send.at[0], halo_recv.at[0])
    acts = Field(act_a, ring, 2, 1, 1, True, halo_send.at[1], halo_recv.at[1])
    seconds = Field(second_a, ring, 0, 1, -1, False, halo_send.at[2], halo_recv.at[2])
    firsts = Field(first_a, ring, 0, 1, -1, False, halo_send.at[3], halo_recv.at[3])
    fields = (clips, acts, seconds, firsts)
    first_sum, second_sum = (
        AllReduce(me, part.at[i], full, other.at[i], slots.at[i], near.at[i], piece.at[i], tiles.at[i],
                  red_send.at[i], red_recv.at[i])
        for i, full in enumerate((full_first, full_second)))

    for field in fields:
        field.clear()

    barrier = pltpu.get_barrier_semaphore()
    count = greet_reduce_peers(me, barrier)

    @pl.loop(1, GROUP)
    def _(o):
        pl.semaphore_signal(barrier, inc=1, device_id=Ring.at(ring.g, (ring.s + o) % GROUP), device_id_type=MESH)

    count = count + GROUP - 1
    for step in (-1, 1):
        for side in (-1, 0, 1):
            g, s = ring.g + step, ring.s + side
            there = (g >= 0) & (g < NG) & (s >= 0) & (s < GROUP)

            @pl.when(there)
            def _():
                pl.semaphore_signal(barrier, inc=1, device_id=Ring.at(g, s), device_id_type=MESH)

            count = count + jnp.where(there, 1, 0)
    build_weights(first_kernel, first_w, first_wt, weight_sem.at[0])
    for i in range(2):
        part[i, 27 * CH :, :] = jnp.zeros((CH, CH), BF16)
    loads[0].wait()
    pl.semaphore_wait(barrier, count)

    spread(ring, clip, stage.at[0], block_send.at[0], clip_recv.at[ring.s], block_own.at[0])
    build_weights(second_kernel, second_w, second_wt, weight_sem.at[1])

    relay(ring, stage.at[0], full_first, clip_recv, block_own.at[0], ahead, clips.has_target(), ahead_sem.at[0], ahead_sem.at[1])
    for f in range(FR):
        clip_a[2 + f, 2 : COLS + 2] = swap(stage[0, f])
    clips.edges(0)
    clips.edges(1)
    loads[1].wait()
    spread(ring, cotangent, stage.at[1], block_send.at[1], block_recv.at[1], block_own.at[1])
    await_weights(first_w, first_wt, weight_sem.at[0])
    await_weights(second_w, second_wt, weight_sem.at[1])
    clips.await_edges(0)
    clips.await_edges(1)

    def sigmoid_slope(z):
        sigma = jax.nn.sigmoid(z)
        return sigma, sigma * (1.0 + z * (1.0 - sigma))

    def first_layer(p):
        width = COLS // 2 + 1
        for half in range(2):
            start = half * width
            pre = convolve(clips, first_w, p, 0, start, width)
            sigma, slope = sigmoid_slope(pre)
            act = (pre * sigma).astype(BF16)
            for j in range(2):
                act_a[2 + 2 * p + j, start : start + width] = act[:, j * CH : (j + 1) * CH].reshape(width, ROWN, CH)
            skip = ROWN if half == 0 else 0
            slopes[p, half * POS // 2 : (half + 1) * POS // 2] = slope[skip : skip + POS // 2]
        pair, edge = pl.ds(2 + 2 * p, 2), jnp.zeros((2, ROWN, CH), BF16)

        @pl.when(ring.s == 0)
        def _():
            act_a[pair, 0] = edge

        @pl.when(ring.s == GROUP - 1)
        def _():
            act_a[pair, COLS + 1] = edge

    width = COLS // 2

    def second_layer(p):
        for start in (0, width):
            pre = convolve(acts, second_w, p, 0, start, width)
            sigma, slope = sigmoid_slope(pre)
            critic = pre * sigma
            delta = slope * jnp.concatenate(
                [cot_f[2 * p + j, start : start + width].reshape(width * ROWN, CH).astype(F32) for j in range(2)], axis=1)
            for j in range(2):
                half = slice(j * CH, (j + 1) * CH)
                stage[2, 2 * p + j, :, start : start + width] = swap(critic[:, half].astype(BF16).reshape(width, ROWN, CH))
                seconds.put(2 * p + j, start, delta[:, half])
            store_turned(turned, delta, p * POS + start * ROWN)

    def back_layer(p):
        for start in (0, width):
            rows = slice(start * ROWN, (start + width) * ROWN)
            delta = convolve(seconds, second_wt, p, 1, start, width) * slopes[p, rows]
            for j in range(2):
                firsts.put(2 * p + j, start, delta[:, j * CH : (j + 1) * CH])
            store_turned(turned, delta, p * POS + start * ROWN)

    def input_layer(p):
        for start in (0, width):
            back = convolve(firsts, first_wt, p, 1, start, width)
            for j in range(2):
                stage[0, 2 * p + j, :, start : start + width] = swap(
                    back[:, j * CH : (j + 1) * CH].astype(BF16).reshape(width, ROWN, CH))

    def give_critic(half):
        give_back(ring, stage.at[2], critic_map, block_send.at[2], block_recv.at[2], block_own.at[2], half)

    def give_grad(half):
        give_back(ring, stage.at[0], clip_grad, block_send.at[3], block_recv.at[3], block_own.at[3], half)

    first_layer(1)
    acts.frames()

    @pl.when(clips.has_source())
    def _():
        take(full_first, 4 * 2 * 4 * COLS, ahead_sem.at[1])
        for f in range(2):
            clip_a[f, 2 : COLS + 2] = swap(ahead[f])

    clips.edges(-1)
    clips.await_edges(-1)
    first_layer(0)
    await_blocks(full_first, block_recv.at[1], block_own.at[1])
    for f in range(FR):
        cot_f[f] = swap(stage[1, f])
    second_layer(1)
    seconds.edges(1)
    give_critic(1)
    acts.await_frames()
    second_layer(0)
    seconds.frames()
    seconds.edges(0)
    weight_grads(acts, turned, part.at[1], scale)
    second_sum.scatter_core()
    seconds.await_edges(0)
    seconds.await_edges(1)
    give_critic(0)
    back_layer(0)
    second_sum.scatter_far()
    firsts.edges(0)

    @pl.when(me.z != 0)
    def _():
        firsts.frames()

    begin_grads(clips, turned, begun, 0)
    seconds.await_frames()
    back_layer(1)
    firsts.edges(1)
    weight_grads(clips, turned, part.at[0], scale, begun)
    first_sum.scatter_core()
    second_sum.scatter_near()
    firsts.await_edges(0)
    firsts.await_edges(1)
    first_sum.scatter_far()
    take(full_first, (GROUP - 1) * 2 * 4 * COLS, block_send.at[0])

    @pl.when(clips.has_target())
    def _():
        take(full_first, 4 * 2 * 4 * COLS, ahead_sem.at[0])

    input_layer(0)
    second_sum.scatter_z()
    first_sum.scatter_near()

    @pl.when(me.z != NZ - 1)
    def _():
        firsts.await_frames()
        input_layer(1)

    give_grad(0)

    @pl.when(me.z != NZ - 1)
    def _():
        give_grad(1)

    second_sum.gather_z()
    first_sum.scatter_z()


    @pl.when(me.z == 0)
    def _():
        firsts.frames()

    second_sum.gather_near()
    first_sum.gather_z()
    second_sum.gather_far()
    first_sum.gather_near()

    @pl.when(me.z == NZ - 1)
    def _():
        firsts.await_frames()
        input_layer(1)
        give_grad(1)

    first_sum.gather_far()
    second_sum.gather_core()
    second_sum.finish()

    @pl.loop(0, 27 * CH // 192)
    def _(k):
        rows = rows_of(k * 192, 192)
        second_out[rows, :] = full_second[rows, :].astype(F32)

    for field in fields:
        field.finish()
    for i in range(1, 4):
        take(full_first, (GROUP - 1) * 2 * 4 * COLS, block_send.at[i])
    for i in range(2, 4):
        await_blocks(full_first, block_recv.at[i], block_own.at[i])
    first_sum.gather_core()
    first_sum.finish()


def write_out(critic_in, grad_in, first_in, second_in, critic, grad, first, second, wide, sem):
    half = 27 * CH // 2
    stores = []

    def store(source, target):
        stores.append(pltpu.make_async_copy(source, target, sem.at[len(stores)]))
        stores[-1].start()

    store(second_in, second)
    for h in range(2):
        @pl.loop(0, half // 192)
        def _(k):
            wide[h, rows_of(k * 192, 192), :] = first_in[rows_of(h * half + k * 192, 192), :].astype(F32)

        store(wide.at[h], first.at[pl.ds(h * half, half)])
    store(critic_in, critic)
    store(grad_in, grad)
    for one in stores:
        one.wait()


def on_device(clip, first_kernel, second_kernel, cotangent):
    cells = clip.shape[0] * lax.axis_size("frame") * clip.shape[1] * lax.axis_size("row") * clip.shape[2]
    scale = 1.0 / float(cells) ** 0.5
    vmem, anywhere = pl.BlockSpec(memory_space=pltpu.VMEM), pl.BlockSpec(memory_space=pl.ANY)
    total = jax.ShapeDtypeStruct((ROWS, CH), BF16)
    dma = pltpu.SemaphoreType.DMA
    flat = (2 * 4 * GROUP * COLS, CH)

    def field(halo):
        return pltpu.VMEM((FR + 2, COLS + 2 * halo, ROWN, CH), BF16)

    results = pl.pallas_call(
        functools.partial(kernel, scale),
        out_shape=(jax.ShapeDtypeStruct(clip.shape, BF16), jax.ShapeDtypeStruct(clip.shape, BF16), total,
                   jax.ShapeDtypeStruct((27 * CH, CH), F32)),
        in_specs=[pl.BlockSpec(memory_space=pltpu.HBM)] * 4,
        out_specs=(vmem, vmem, vmem, vmem),
        scratch_shapes=[
            field(2), field(1), field(1), field(1),
            pltpu.VMEM((12 * CH, 6 * CH), BF16), pltpu.VMEM((6 * CH, 12 * CH), BF16),
            pltpu.VMEM((12 * CH, 6 * CH), BF16), pltpu.VMEM((6 * CH, 12 * CH), BF16),
            pltpu.VMEM(clip.shape, BF16), pltpu.VMEM(clip.shape, BF16),
            pltpu.VMEM((3, FR, ROWN, COLS, CH), BF16),
            pltpu.VMEM((FR, COLS, ROWN, CH), BF16),
            pltpu.VMEM((2, POS, 2 * CH), F32),
            pltpu.VMEM((6 * CH, 2 * POS), BF16),
            pltpu.VMEM((3, 6 * CH, 4 * CH), F32),
            pltpu.VMEM((2, ROWS, CH), BF16),
            pltpu.VMEM((2, HALF, CH), BF16),
            pltpu.VMEM((2, HALF, CH), BF16),
            pltpu.VMEM((2, HALF // 4, CH), BF16),
            pltpu.VMEM((2, BLK, CH), BF16),
            pltpu.VMEM((2, NZ * TILE, CH), BF16),
            dma((2, 8)), dma((2, 8)), dma((4, 7)), dma((4, 7)), dma((4,)), dma((4,)), dma((4,)), dma((2, 2)), dma((2,)),
            pltpu.VMEM((2, ROWN, COLS, CH), BF16), dma((GROUP,)), dma((2,)),
            pltpu.VMEM((ROWS, CH), BF16),
        ],
        compiler_params=pltpu.CompilerParams(collective_id=0, has_side_effects=True, vmem_limit_bytes=38 << 20),
    )(*(pltpu.with_memory_space_constraint(one, pltpu.HBM) for one in (
        clip, cotangent, first_kernel.reshape(27, CH, CH), second_kernel.reshape(27, CH, CH))))
    critic_map, clip_grad, first, second = results

    whole = jax.ShapeDtypeStruct((27 * CH, CH), F32)
    critic_map, clip_grad, first, second = pl.pallas_call(
        write_out,
        out_shape=(jax.ShapeDtypeStruct(flat, BF16), jax.ShapeDtypeStruct(flat, BF16), whole, whole),
        in_specs=[vmem] * 4,
        out_specs=(anywhere,) * 4,
        scratch_shapes=[pltpu.VMEM((2, 27 * CH // 2, CH), F32), dma((5,))],
        compiler_params=pltpu.CompilerParams(vmem_limit_bytes=10 << 20),
    )(critic_map.reshape(flat), clip_grad.reshape(flat), first, second)
    taps = (3, 3, 3, CH, CH)
    return critic_map.reshape(clip.shape), clip_grad.reshape(clip.shape), first.reshape(taps), second.reshape(taps)


def solution(mesh):
    placed = (P("frame", "row", None, None), P(), P(), P("frame", "row", None, None))
    return jax.shard_map(
        on_device,
        mesh=mesh,
        in_specs=placed,
        out_specs=(P("frame", "row", None, None), P("frame", "row", None, None), P(), P()),
        check_vma=False,
    )
```

```python
import functools

import jax
import jax.numpy as jnp
from jax import lax
from jax.experimental import pallas as pl
from jax.experimental.pallas import tpu as pltpu
from jax.sharding import PartitionSpec as P

MESH = pl.DeviceIdType.MESH
BF16, F32 = jnp.bfloat16, jnp.float32
CH = 128

NX, NY, NZ = 4, 4, 8
NXY = NX * NY
BLK = 112
HALF = NXY * BLK
ROWS = 2 * HALF
TILE = 16
ZT = BLK // TILE


class Place:
    def __init__(self):
        f, r = lax.axis_index("frame"), lax.axis_index("row")
        self.x, self.z = f // (2 * NZ), (f // 2) % NZ
        self.y, self.core = (r // 2) * 2 + f % 2, r % 2
        self.p = self.x * NY + self.y

    @staticmethod
    def at(x, y, z, core):
        return ((x * NZ + z) * 2 + y % 2, (y // 2) * 2 + core)


def remote(src, dst, send, recv, device):
    return pltpu.make_async_remote_copy(
        src_ref=src, dst_ref=dst, send_sem=send, recv_sem=recv, device_id=device, device_id_type=MESH)


def take(ref, rows, sem):
    view = ref.at[pl.ds(0, rows)]
    pltpu.make_async_copy(view, view, sem).wait()


def rows_of(start, size):
    return pl.ds(pl.multiple_of(start, TILE), size)


class AllReduce:
    A, B = (256, 64), (192, 48)
    START_B = NX * 256

    def __init__(self, me, part, full, other, slots, near, piece, tiles, send, recv):
        self.me, self.part, self.full = me, part, full
        self.other, self.slots, self.near, self.piece, self.tiles = other, slots, near, piece, tiles
        self.send, self.recv = send, recv
        self.base = me.core * HALF

    def x_peer(self, o):
        x = (self.me.x + o) % NX
        return x, Place.at(x, self.me.y, self.me.z, self.me.core)

    def y_peer(self, o):
        y = (self.me.y + o) % NY
        return y, Place.at(self.me.x, y, self.me.z, self.me.core)

    def z_peer(self, o):
        d = (self.me.z + o) % NZ
        return d, Place.at(self.me.x, self.me.y, d, self.me.core)

    def twin(self):
        return Place.at(self.me.x, self.me.y, self.me.z, 1 - self.me.core)

    def row_a(self, x, y):
        return self.base + x * self.A[0] + y * self.A[1]

    def row_b(self, x, y):
        return self.base + self.START_B + y * self.B[0] + x * self.B[1]

    def push(self, stage, source, start, target, to, size, peer):
        remote(source.at[rows_of(start, size)], target.at[rows_of(to, size)], self.send.at[stage], self.recv.at[stage], peer).start()

    def scatter_core(self):
        self.push(0, self.part, (1 - self.me.core) * HALF, self.other, 0, HALF, self.twin())

    def scatter_far(self):
        me = self.me
        take(self.other, HALF, self.recv.at[0])

        @pl.loop(0, HALF // 128)
        def _(i):
            mine = rows_of(self.base + i * 128, 128)
            total = self.part[mine, :].astype(F32) + self.other[rows_of(i * 128, 128), :].astype(F32)
            self.part[mine, :] = total.astype(BF16)

        @pl.loop(1, NX)
        def _(o):
            x, peer = self.x_peer(o)
            self.push(1, self.part, self.row_a(x, 0), self.slots, me.x * self.A[0], self.A[0], peer)
            y, peer = self.y_peer(o)
            self.push(1, self.part, self.row_b(0, y), self.slots, self.START_B + me.y * self.B[0], self.B[0], peer)

    def scatter_near(self):
        me = self.me
        take(self.slots, 3 * (self.A[0] + self.B[0]), self.recv.at[1])

        @pl.loop(0, 4)
        def _(i):
            for start, slot, mine, pitch, size in (
                (self.row_a(me.x, 0), 0, me.x, self.A[0], self.A[1]),
                (self.row_b(0, me.y), self.START_B, me.y, self.B[0], self.B[1])):
                rows = rows_of(start + i * size, size)
                total = self.part[rows, :].astype(F32)
                for o in range(1, 4):
                    total = total + self.slots[rows_of(slot + ((mine + o) % 4) * pitch + i * size, size), :].astype(F32)
                self.part[rows, :] = total.astype(BF16)

        @pl.loop(1, NX)
        def _(o):
            y, peer = self.y_peer(o)
            self.push(2, self.part, self.row_a(me.x, y), self.near, me.y * self.A[1], self.A[1], peer)
            x, peer = self.x_peer(o)
            self.push(2, self.part, self.row_b(x, me.y), self.near, NY * self.A[1] + me.x * self.B[1], self.B[1], peer)

    def scatter_z(self):
        me = self.me
        take(self.near, 3 * (self.A[1] + self.B[1]), self.recv.at[2])
        for start, slot, mine, size, to in (
            (self.row_a(me.x, me.y), 0, me.y, self.A[1], 0),
            (self.row_b(me.x, me.y), NY * self.A[1], me.x, self.B[1], self.A[1])):
            total = self.part[rows_of(start, size), :].astype(F32)
            for o in range(1, 4):
                total = total + self.near[rows_of(slot + ((mine + o) % 4) * size, size), :].astype(F32)
            self.piece[to : to + size, :] = total.astype(BF16)

        @pl.loop(1, NZ)
        def _(o):
            d, peer = self.z_peer(o)

            @pl.when(d < ZT)
            def _():
                self.push(3, self.piece, d * TILE, self.tiles, me.z * TILE, TILE, peer)

    def gather_z(self):
        me = self.me

        @pl.when(me.z < ZT)
        def _():
            take(self.tiles, (NZ - 1) * TILE, self.recv.at[3])
            total = self.piece[rows_of(me.z * TILE, TILE), :].astype(F32)
            for o in range(1, NZ):
                d = (me.z + o) % NZ
                total = total + self.tiles[rows_of(d * TILE, TILE), :].astype(F32)
            in_a = self.A[1] // TILE
            row = jnp.where(me.z < in_a, self.row_a(me.x, me.y) + me.z * TILE, self.row_b(me.x, me.y) + (me.z - in_a) * TILE)
            self.full[rows_of(row, TILE), :] = total.astype(BF16)

            @pl.loop(1, NZ)
            def _(o):
                d, peer = self.z_peer(o)
                self.push(4, self.full, row, self.full, row, TILE, peer)

    def gather_near(self):
        me = self.me

        @pl.when(me.z < ZT)
        def _():
            take(self.full, (ZT - 1) * TILE, self.recv.at[4])

        @pl.when(me.z >= ZT)
        def _():
            take(self.full, ZT * TILE, self.recv.at[4])

        a, b = self.row_a(me.x, me.y), self.row_b(me.x, me.y)

        @pl.loop(1, NX)
        def _(o):
            self.push(5, self.full, a, self.full, a, self.A[1], self.y_peer(o)[1])
            self.push(5, self.full, b, self.full, b, self.B[1], self.x_peer(o)[1])

    def gather_far(self):
        me = self.me
        take(self.full, 3 * (self.A[1] + self.B[1]), self.recv.at[5])
        a, b = self.row_a(me.x, 0), self.row_b(0, me.y)

        @pl.loop(1, NX)
        def _(o):
            self.push(6, self.full, a, self.full, a, self.A[0], self.x_peer(o)[1])
            self.push(6, self.full, b, self.full, b, self.B[0], self.y_peer(o)[1])

    def gather_core(self):
        take(self.full, 3 * (self.A[0] + self.B[0]), self.recv.at[6])
        self.push(7, self.full, self.base, self.full, self.base, HALF, self.twin())

    def finish(self):
        me = self.me
        take(self.full, HALF, self.recv.at[7])
        take(self.part, HALF, self.send.at[0])
        take(self.part, 3 * (self.A[0] + self.B[0]), self.send.at[1])
        take(self.part, 3 * (self.A[1] + self.B[1]), self.send.at[2])

        @pl.when(me.z < ZT)
        def _():
            take(self.piece, (ZT - 1) * TILE, self.send.at[3])
            take(self.full, (NZ - 1) * TILE, self.send.at[4])

        @pl.when(me.z >= ZT)
        def _():
            take(self.piece, ZT * TILE, self.send.at[3])

        take(self.full, 3 * (self.A[1] + self.B[1]), self.send.at[5])
        take(self.full, 3 * (self.A[0] + self.B[0]), self.send.at[6])
        take(self.full, HALF, self.send.at[7])


def greet_reduce_peers(me, barrier):
    pl.semaphore_signal(barrier, inc=1, device_id=Place.at(me.x, me.y, me.z, 1 - me.core), device_id_type=MESH)

    @pl.loop(1, NXY)
    def _(o):
        p = (me.p + o) % NXY
        pl.semaphore_signal(barrier, inc=1, device_id=Place.at(p // NY, p % NY, me.z, me.core), device_id_type=MESH)

    @pl.loop(1, NZ)
    def _(o):
        d = (me.z + o) % NZ
        pl.semaphore_signal(barrier, inc=1, device_id=Place.at(me.x, me.y, d, me.core), device_id_type=MESH)

    return 1 + NXY - 1 + NZ - 1

GROUP, FR, COLS, ROWN = 8, 4, 32, 16
POS = COLS * ROWN
NG = NX * NZ


class Ring:
    def __init__(self):
        f, r = lax.axis_index("frame"), lax.axis_index("row")
        self.g, self.y_lo, self.r = f // 2, f % 2, r
        self.s = (r // 2) * 4 + self.y_lo * 2 + r % 2

    @staticmethod
    def parts(s):
        return (s // 2) % 2, (s // 4) * 2 + s % 2

    @staticmethod
    def at(g, s):
        y_lo, r = Ring.parts(s)
        return (g * 2 + y_lo, r)


class Field:
    def __init__(self, ref, ring, own, halo, step, whole, send, recv):
        self.ref, self.ring, self.own, self.halo, self.step, self.whole = ref, ring, own, halo, step, whole
        self.send, self.recv = send, recv
        self.width = COLS + 2 * halo

    def clear(self):
        far = 0 if self.own else FR

        @pl.when(jnp.logical_not(self.has_source()))
        def _():
            self.ref[far : far + 2] = jnp.zeros((2, self.width, ROWN, CH), BF16)

        edge = jnp.zeros((FR + 2, self.halo, ROWN, CH), BF16)

        @pl.when(jnp.logical_not(self.to_left()))
        def _():
            self.ref[:, 0 : self.halo] = edge

        @pl.when(jnp.logical_not(self.to_right()))
        def _():
            self.ref[:, COLS + self.halo :] = edge

    def put(self, f, start, value):
        width = value.shape[0] // ROWN
        self.ref[self.own + f, self.halo + start : self.halo + start + width] = value.astype(BF16).reshape(width, ROWN, CH)

    def to_left(self):
        return self.ring.s > 0

    def to_right(self):
        return self.ring.s < GROUP - 1

    def has_target(self):
        return self.ring.g < NG - 1 if self.step > 0 else self.ring.g > 0

    def has_source(self):
        return self.ring.g > 0 if self.step > 0 else self.ring.g < NG - 1

    def copy(self, frames, col, to_frames, to_col, width, g, s, i):
        return remote(self.ref.at[frames, pl.ds(col, width)], self.ref.at[to_frames, pl.ds(to_col, width)],
                      self.send.at[i], self.recv.at[i], Ring.at(g, s))

    def edge(self, frames, to_frames, side, g, i):
        halo, s = self.halo, self.ring.s
        source, target = (halo, COLS + halo) if side < 0 else (COLS, 0)
        self.copy(frames, source, to_frames, target, halo, g, s + side, i).start()

    def edges(self, q):
        frames, i = self._pair(q)

        @pl.when(self._held(q) & self.to_left())
        def _():
            self.edge(frames, frames, -1, self.ring.g, i)

        @pl.when(self._held(q) & self.to_right())
        def _():
            self.edge(frames, frames, 1, self.ring.g, i + 1)

    def _pair(self, q):
        return pl.ds(self.own + 2 * q, 2), (2 * q) % 6

    def _held(self, q):
        return self.has_source() if q < 0 else self.ring.g >= 0

    def await_edges(self, q):
        self._edges(q, self.recv, self.to_right(), self.to_left())

    def _edges(self, q, sem, left, right):
        frames, i = self._pair(q)
        view = self.ref.at[frames, pl.ds(0, self.halo)]

        @pl.when(self._held(q) & left)
        def _():
            pltpu.make_async_copy(view, view, sem.at[i]).wait()

        @pl.when(self._held(q) & right)
        def _():
            pltpu.make_async_copy(view, view, sem.at[i + 1]).wait()

    def span(self):
        return (0, self.width) if self.whole else (self.halo, COLS)

    def frames(self):
        g, s = self.ring.g + self.step, self.ring.s
        mine, theirs = (pl.ds(FR, 2), pl.ds(0, 2)) if self.step > 0 else (pl.ds(0, 2), pl.ds(FR, 2))
        start, width = self.span()

        @pl.when(self.has_target())
        def _():
            self.copy(mine, start, theirs, start, width, g, s, 4).start()

        if self.whole:
            return

        @pl.when(self.has_target() & self.to_left())
        def _():
            self.edge(mine, theirs, -1, g, 5)

        @pl.when(self.has_target() & self.to_right())
        def _():
            self.edge(mine, theirs, 1, g, 6)

    def _frames(self, sem, there, left, right):
        start, width = self.span()
        body, col = self.ref.at[pl.ds(0, 2), pl.ds(start, width)], self.ref.at[pl.ds(0, 2), pl.ds(0, self.halo)]

        @pl.when(there)
        def _():
            pltpu.make_async_copy(body, body, sem.at[4]).wait()

        if self.whole:
            return

        @pl.when(there & left)
        def _():
            pltpu.make_async_copy(col, col, sem.at[5]).wait()

        @pl.when(there & right)
        def _():
            pltpu.make_async_copy(col, col, sem.at[6]).wait()

    def await_frames(self):
        self._frames(self.recv, self.has_source(), self.to_right(), self.to_left())

    def finish(self):
        if not self.whole:
            for q in range(-1 if self.step > 0 else 0, 2):
                self._edges(q, self.send, self.to_left(), self.to_right())
        if self.whole or self.step < 0:
            self._frames(self.send, self.has_target(), self.to_left(), self.to_right())

    def slab(self, p, k, start, width):
        return self.ref[2 * p + k, start : start + width].reshape(width * ROWN, CH)


def build_weights(kernel, ahead, back, sem):
    zero = jnp.zeros((CH, CH), BF16)
    for k, j in ((0, 1), (3, 0)):
        @pl.loop(0, 9)
        def _(bc):
            b, c = bc // 3, bc % 3
            ahead[pl.ds(pl.multiple_of((c * 4 + k) * CH, CH), CH), pl.ds(pl.multiple_of((b * 2 + j) * CH, CH), CH)] = zero
            back[pl.ds(pl.multiple_of((b * 2 + j) * CH, CH), CH), pl.ds(pl.multiple_of((c * 4 + k) * CH, CH), CH)] = zero

    @pl.loop(0, 27)
    def _(tap):
        a, b, c = tap // 9, (tap // 3) % 3, tap % 3
        for j in range(2):
            k = a + j
            pltpu.make_async_copy(
                kernel.at[tap],
                ahead.at[pl.ds(pl.multiple_of((c * 4 + k) * CH, CH), CH), pl.ds(pl.multiple_of((b * 2 + j) * CH, CH), CH)],
                sem.at[0]).start()
            k = j + 2 - a
            pltpu.make_async_copy(
                kernel.at[tap],
                back.at[pl.ds(pl.multiple_of(((2 - b) * 2 + j) * CH, CH), CH), pl.ds(pl.multiple_of(((2 - c) * 4 + k) * CH, CH), CH)],
                sem.at[1]).start()


def await_weights(ahead, back, sem):
    view = ahead.at[pl.ds(0, 54 * CH * CH // ahead.shape[1])]
    pltpu.make_async_copy(view, view, sem.at[0]).wait()
    view = back.at[pl.ds(0, 54 * CH * CH // back.shape[1])]
    pltpu.make_async_copy(view, view, sem.at[1]).wait()


def row_index(shape):
    return lax.broadcasted_iota(jnp.int32, shape, 0) % ROWN


def from_above(value):
    return jnp.where(row_index(value.shape) == 0, 0.0, pltpu.roll(value, 1, axis=0))


def from_below(value):
    return jnp.where(row_index(value.shape) == ROWN - 1, 0.0, pltpu.roll(value, value.shape[0] - 1, axis=0))


def convolve(field, weights, p, contract, start, width):
    lhs = jnp.concatenate([field.slab(p, k, start + c, width) for c in range(3) for k in range(4)], axis=1)
    rows = lax.dot_general(lhs, weights[...], (((1,), (contract,)), ((), ())), preferred_element_type=F32)
    above, level, below = (rows[:, b * 2 * CH : (b + 1) * 2 * CH] for b in range(3))
    return level + from_above(above) + from_below(below)


def store_turned(turned, delta, start):
    for b, value in enumerate((from_below(delta), delta, from_above(delta))):
        turned[b * 2 * CH : (b + 1) * 2 * CH, start : start + delta.shape[0]] = value.astype(BF16).T


def pair_sums(field, turned, p, c):
    rhs = jnp.concatenate([field.slab(p, k, field.halo - 1 + c, COLS) for k in range(4)], axis=1)
    return lax.dot_general(turned[:, p * POS : (p + 1) * POS], rhs, (((1,), (0,)), ((), ())), preferred_element_type=F32)


def begin_grads(field, turned, begun, p):
    for c in range(3):
        begun[c] = pair_sums(field, turned, p, c)


def weight_grads(field, turned, part, scale, begun=None):
    for c in range(3):
        if begun is None:
            rhs = jnp.concatenate(
                [jnp.concatenate([field.slab(p, k, field.halo - 1 + c, COLS) for k in range(4)], axis=1) for p in range(2)], axis=0)
            sums = lax.dot_general(turned[...], rhs, (((1,), (0,)), ((), ())), preferred_element_type=F32)
        else:
            sums = begun[c] + pair_sums(field, turned, 1, c)
        for b in range(3):
            for a in range(3):
                one = sums[2 * b * CH : (2 * b + 1) * CH, a * CH : (a + 1) * CH]
                two = sums[(2 * b + 1) * CH : (2 * b + 2) * CH, (a + 1) * CH : (a + 2) * CH]
                tap = (a * 3 + b) * 3 + c
                part[tap * CH : (tap + 1) * CH, :] = ((one + two) * scale).T.astype(BF16)


def swap(value):
    return jnp.swapaxes(value, 0, 1)


def spread(ring, source, stage, send, recv, own):
    chip, core = ring.s // 2, ring.s % 2
    for turn, flip in ((0, 1), (1, 0), (3, 0), (1, 1), (3, 1), (2, 0), (2, 1)):
        d = (chip + turn) % 4 * 2 + (core + flip) % 2
        cols = pl.ds(pl.multiple_of(d * COLS, COLS), COLS)
        remote(source.at[:, :, cols], stage.at[pl.ds(2 * ring.y_lo, 2), pl.ds(4 * ring.r, 4)], send, recv, Ring.at(ring.g, d)).start()

    cols = pl.ds(pl.multiple_of(ring.s * COLS, COLS), COLS)
    pltpu.make_async_copy(source.at[:, :, cols], stage.at[pl.ds(2 * ring.y_lo, 2), pl.ds(4 * ring.r, 4)], own).start()


def relay(ring, stage, flat, recv, own, ahead, there, send, landed):
    for turn in (0, 3, 1, 2):
        for core in range(2):
            s = (ring.s + 2 * turn) % GROUP // 2 * 2 + core
            half, quarter = Ring.parts(s)

            @pl.when(s == ring.s)
            def _():
                take(flat, 2 * 4 * COLS, own)

            @pl.when(s != ring.s)
            def _():
                take(flat, 2 * 4 * COLS, recv.at[s])

            @pl.when(there & (half == 1))
            def _():
                rows = pl.ds(4 * quarter, 4)
                remote(stage.at[pl.ds(2, 2), rows], ahead.at[:, rows], send, landed, Ring.at(ring.g + 1, ring.s)).start()


def give_back(ring, stage, result, send, recv, own, half):
    cols = pl.ds(pl.multiple_of(ring.s * COLS, COLS), COLS)
    pair = pl.ds(2 * half, 2)

    @pl.loop(0, 4)
    def _(i):
        quarter = (ring.r + i) % 4
        rows = pl.ds(4 * quarter, 4)
        here = (half == ring.y_lo) & (i == 0)

        @pl.when(here)
        def _():
            pltpu.make_async_copy(stage.at[pair, rows], result.at[:, :, cols], own).start()

        @pl.when(jnp.logical_not(here))
        def _():
            remote(stage.at[pair, rows], result.at[:, :, cols], send, recv, (ring.g * 2 + half, quarter)).start()


def await_blocks(flat, sem, own):
    take(flat, (GROUP - 1) * 2 * 4 * COLS, sem)
    take(flat, 2 * 4 * COLS, own)


def kernel(scale, clip_in, cotangent_in, first_kernel, second_kernel, critic_map, clip_grad, full_first, second_out,
           clip_a, act_a, second_a, first_a, first_w, first_wt, second_w, second_wt, clip, cotangent, stage, cot_f, slopes,
           turned, begun, part, other, slots, near, piece, tiles,
           red_send, red_recv, halo_send, halo_recv, block_send, block_recv, block_own, weight_sem, load_sem,
           ahead, clip_recv, ahead_sem, full_second):
    loads = [pltpu.make_async_copy(source, target, load_sem.at[i])
             for i, (source, target) in enumerate(((clip_in, clip), (cotangent_in, cotangent)))]
    for load in loads:
        load.start()
    me, ring = Place(), Ring()
    clips = Field(clip_a, ring, 2, 2, 1, False, halo_send.at[0], halo_recv.at[0])
    acts = Field(act_a, ring, 2, 1, 1, True, halo_send.at[1], halo_recv.at[1])
    seconds = Field(second_a, ring, 0, 1, -1, False, halo_send.at[2], halo_recv.at[2])
    firsts = Field(first_a, ring, 0, 1, -1, False, halo_send.at[3], halo_recv.at[3])
    fields = (clips, acts, seconds, firsts)
    first_sum, second_sum = (
        AllReduce(me, part.at[i], full, other.at[i], slots.at[i], near.at[i], piece.at[i], tiles.at[i],
                  red_send.at[i], red_recv.at[i])
        for i, full in enumerate((full_first, full_second)))

    for field in fields:
        field.clear()

    barrier = pltpu.get_barrier_semaphore()
    count = greet_reduce_peers(me, barrier)

    @pl.loop(1, GROUP)
    def _(o):
        pl.semaphore_signal(barrier, inc=1, device_id=Ring.at(ring.g, (ring.s + o) % GROUP), device_id_type=MESH)

    count = count + GROUP - 1
    for step in (-1, 1):
        for side in (-1, 0, 1):
            g, s = ring.g + step, ring.s + side
            there = (g >= 0) & (g < NG) & (s >= 0) & (s < GROUP)

            @pl.when(there)
            def _():
                pl.semaphore_signal(barrier, inc=1, device_id=Ring.at(g, s), device_id_type=MESH)

            count = count + jnp.where(there, 1, 0)
    build_weights(first_kernel, first_w, first_wt, weight_sem.at[0])
    for i in range(2):
        part[i, 27 * CH :, :] = jnp.zeros((CH, CH), BF16)
    loads[0].wait()
    pl.semaphore_wait(barrier, count)

    spread(ring, clip, stage.at[0], block_send.at[0], clip_recv.at[ring.s], block_own.at[0])
    build_weights(second_kernel, second_w, second_wt, weight_sem.at[1])

    relay(ring, stage.at[0], full_first, clip_recv, block_own.at[0], ahead, clips.has_target(), ahead_sem.at[0], ahead_sem.at[1])
    for f in range(FR):
        clip_a[2 + f, 2 : COLS + 2] = swap(stage[0, f])
    clips.edges(0)
    clips.edges(1)
    loads[1].wait()
    spread(ring, cotangent, stage.at[1], block_send.at[1], block_recv.at[1], block_own.at[1])
    await_weights(first_w, first_wt, weight_sem.at[0])
    await_weights(second_w, second_wt, weight_sem.at[1])
    clips.await_edges(0)
    clips.await_edges(1)

    def sigmoid_slope(z):
        sigma = jax.nn.sigmoid(z)
        return sigma, sigma * (1.0 + z * (1.0 - sigma))

    def first_layer(p):
        width = COLS // 2 + 1
        for half in range(2):
            start = half * width
            pre = convolve(clips, first_w, p, 0, start, width)
            sigma, slope = sigmoid_slope(pre)
            act = (pre * sigma).astype(BF16)
            for j in range(2):
                act_a[2 + 2 * p + j, start : start + width] = act[:, j * CH : (j + 1) * CH].reshape(width, ROWN, CH)
            skip = ROWN if half == 0 else 0
            slopes[p, half * POS // 2 : (half + 1) * POS // 2] = slope[skip : skip + POS // 2]
        pair, edge = pl.ds(2 + 2 * p, 2), jnp.zeros((2, ROWN, CH), BF16)

        @pl.when(ring.s == 0)
        def _():
            act_a[pair, 0] = edge

        @pl.when(ring.s == GROUP - 1)
        def _():
            act_a[pair, COLS + 1] = edge

    width = COLS // 2

    def second_layer(p):
        for start in (0, width):
            pre = convolve(acts, second_w, p, 0, start, width)
            sigma, slope = sigmoid_slope(pre)
            critic = pre * sigma
            delta = slope * jnp.concatenate(
                [cot_f[2 * p + j, start : start + width].reshape(width * ROWN, CH).astype(F32) for j in range(2)], axis=1)
            for j in range(2):
                half = slice(j * CH, (j + 1) * CH)
                stage[2, 2 * p + j, :, start : start + width] = swap(critic[:, half].astype(BF16).reshape(width, ROWN, CH))
                seconds.put(2 * p + j, start, delta[:, half])
            store_turned(turned, delta, p * POS + start * ROWN)

    def back_layer(p):
        for start in (0, width):
            rows = slice(start * ROWN, (start + width) * ROWN)
            delta = convolve(seconds, second_wt, p, 1, start, width) * slopes[p, rows]
            for j in range(2):
                firsts.put(2 * p + j, start, delta[:, j * CH : (j + 1) * CH])
            store_turned(turned, delta, p * POS + start * ROWN)

    def input_layer(p):
        for start in (0, width):
            back = convolve(firsts, first_wt, p, 1, start, width)
            for j in range(2):
                stage[0, 2 * p + j, :, start : start + width] = swap(
                    back[:, j * CH : (j + 1) * CH].astype(BF16).reshape(width, ROWN, CH))

    def give_critic(half):
        give_back(ring, stage.at[2], critic_map, block_send.at[2], block_recv.at[2], block_own.at[2], half)

    def give_grad(half):
        give_back(ring, stage.at[0], clip_grad, block_send.at[3], block_recv.at[3], block_own.at[3], half)

    first_layer(1)
    acts.frames()

    @pl.when(clips.has_source())
    def _():
        take(full_first, 4 * 2 * 4 * COLS, ahead_sem.at[1])
        for f in range(2):
            clip_a[f, 2 : COLS + 2] = swap(ahead[f])

    clips.edges(-1)
    clips.await_edges(-1)
    first_layer(0)
    await_blocks(full_first, block_recv.at[1], block_own.at[1])
    for f in range(FR):
        cot_f[f] = swap(stage[1, f])
    second_layer(1)
    seconds.edges(1)
    give_critic(1)
    acts.await_frames()
    second_layer(0)
    seconds.frames()
    seconds.edges(0)
    weight_grads(acts, turned, part.at[1], scale)
    second_sum.scatter_core()
    seconds.await_edges(0)
    seconds.await_edges(1)
    give_critic(0)
    back_layer(0)
    second_sum.scatter_far()
    firsts.edges(0)

    @pl.when(me.z != 0)
    def _():
        firsts.frames()

    begin_grads(clips, turned, begun, 0)
    seconds.await_frames()
    back_layer(1)
    firsts.edges(1)
    weight_grads(clips, turned, part.at[0], scale, begun)
    first_sum.scatter_core()
    firsts.await_edges(0)
    firsts.await_edges(1)
    first_sum.scatter_far()
    second_sum.scatter_near()
    take(full_first, (GROUP - 1) * 2 * 4 * COLS, block_send.at[0])

    @pl.when(clips.has_target())
    def _():
        take(full_first, 4 * 2 * 4 * COLS, ahead_sem.at[0])

    input_layer(0)
    second_sum.scatter_z()
    first_sum.scatter_near()

    @pl.when(me.z != NZ - 1)
    def _():
        firsts.await_frames()
        input_layer(1)

    give_grad(0)

    @pl.when(me.z != NZ - 1)
    def _():
        give_grad(1)

    second_sum.gather_z()
    first_sum.scatter_z()


    @pl.when(me.z == 0)
    def _():
        firsts.frames()

    second_sum.gather_near()
    first_sum.gather_z()
    second_sum.gather_far()
    first_sum.gather_near()

    @pl.when(me.z == NZ - 1)
    def _():
        firsts.await_frames()
        input_layer(1)
        give_grad(1)

    first_sum.gather_far()
    second_sum.gather_core()
    second_sum.finish()

    @pl.loop(0, 27 * CH // 192)
    def _(k):
        rows = rows_of(k * 192, 192)
        second_out[rows, :] = full_second[rows, :].astype(F32)

    for field in fields:
        field.finish()
    for i in range(1, 4):
        take(full_first, (GROUP - 1) * 2 * 4 * COLS, block_send.at[i])
    for i in range(2, 4):
        await_blocks(full_first, block_recv.at[i], block_own.at[i])
    first_sum.gather_core()
    first_sum.finish()


def write_out(critic_in, grad_in, first_in, second_in, critic, grad, first, second, wide, sem):
    half = 27 * CH // 2
    stores = []

    def store(source, target):
        stores.append(pltpu.make_async_copy(source, target, sem.at[len(stores)]))
        stores[-1].start()

    store(second_in, second)
    for h in range(2):
        @pl.loop(0, half // 192)
        def _(k):
            wide[h, rows_of(k * 192, 192), :] = first_in[rows_of(h * half + k * 192, 192), :].astype(F32)

        store(wide.at[h], first.at[pl.ds(h * half, half)])
    store(critic_in, critic)
    store(grad_in, grad)
    for one in stores:
        one.wait()


def on_device(clip, first_kernel, second_kernel, cotangent):
    cells = clip.shape[0] * lax.axis_size("frame") * clip.shape[1] * lax.axis_size("row") * clip.shape[2]
    scale = 1.0 / float(cells) ** 0.5
    vmem, anywhere = pl.BlockSpec(memory_space=pltpu.VMEM), pl.BlockSpec(memory_space=pl.ANY)
    total = jax.ShapeDtypeStruct((ROWS, CH), BF16)
    dma = pltpu.SemaphoreType.DMA
    flat = (2 * 4 * GROUP * COLS, CH)

    def field(halo):
        return pltpu.VMEM((FR + 2, COLS + 2 * halo, ROWN, CH), BF16)

    results = pl.pallas_call(
        functools.partial(kernel, scale),
        out_shape=(jax.ShapeDtypeStruct(clip.shape, BF16), jax.ShapeDtypeStruct(clip.shape, BF16), total,
                   jax.ShapeDtypeStruct((27 * CH, CH), F32)),
        in_specs=[pl.BlockSpec(memory_space=pltpu.HBM)] * 4,
        out_specs=(vmem, vmem, vmem, vmem),
        scratch_shapes=[
            field(2), field(1), field(1), field(1),
            pltpu.VMEM((12 * CH, 6 * CH), BF16), pltpu.VMEM((6 * CH, 12 * CH), BF16),
            pltpu.VMEM((12 * CH, 6 * CH), BF16), pltpu.VMEM((6 * CH, 12 * CH), BF16),
            pltpu.VMEM(clip.shape, BF16), pltpu.VMEM(clip.shape, BF16),
            pltpu.VMEM((3, FR, ROWN, COLS, CH), BF16),
            pltpu.VMEM((FR, COLS, ROWN, CH), BF16),
            pltpu.VMEM((2, POS, 2 * CH), F32),
            pltpu.VMEM((6 * CH, 2 * POS), BF16),
            pltpu.VMEM((3, 6 * CH, 4 * CH), F32),
            pltpu.VMEM((2, ROWS, CH), BF16),
            pltpu.VMEM((2, HALF, CH), BF16),
            pltpu.VMEM((2, HALF, CH), BF16),
            pltpu.VMEM((2, HALF // 4, CH), BF16),
            pltpu.VMEM((2, BLK, CH), BF16),
            pltpu.VMEM((2, NZ * TILE, CH), BF16),
            dma((2, 8)), dma((2, 8)), dma((4, 7)), dma((4, 7)), dma((4,)), dma((4,)), dma((4,)), dma((2, 2)), dma((2,)),
            pltpu.VMEM((2, ROWN, COLS, CH), BF16), dma((GROUP,)), dma((2,)),
            pltpu.VMEM((ROWS, CH), BF16),
        ],
        compiler_params=pltpu.CompilerParams(collective_id=0, has_side_effects=True, vmem_limit_bytes=38 << 20),
    )(*(pltpu.with_memory_space_constraint(one, pltpu.HBM) for one in (
        clip, cotangent, first_kernel.reshape(27, CH, CH), second_kernel.reshape(27, CH, CH))))
    critic_map, clip_grad, first, second = results

    whole = jax.ShapeDtypeStruct((27 * CH, CH), F32)
    critic_map, clip_grad, first, second = pl.pallas_call(
        write_out,
        out_shape=(jax.ShapeDtypeStruct(flat, BF16), jax.ShapeDtypeStruct(flat, BF16), whole, whole),
        in_specs=[vmem] * 4,
        out_specs=(anywhere,) * 4,
        scratch_shapes=[pltpu.VMEM((2, 27 * CH // 2, CH), F32), dma((5,))],
        compiler_params=pltpu.CompilerParams(vmem_limit_bytes=10 << 20),
    )(critic_map.reshape(flat), clip_grad.reshape(flat), first, second)
    taps = (3, 3, 3, CH, CH)
    return critic_map.reshape(clip.shape), clip_grad.reshape(clip.shape), first.reshape(taps), second.reshape(taps)


def solution(mesh):
    placed = (P("frame", "row", None, None), P(), P(), P("frame", "row", None, None))
    return jax.shard_map(
        on_device,
        mesh=mesh,
        in_specs=placed,
        out_specs=(P("frame", "row", None, None), P("frame", "row", None, None), P(), P()),
        check_vma=False,
    )
```
